128 devices in a mesh: node: 32 (over y, z, core), feat: 4 (over x).
Axes of the slice: x: 4, y: 4, z: 4, core: 2. Of those that a mesh axis runs over, the one named last changes fastest.
Arguments:
- memory: float32 [32768, 172], P('node')
- last_update: int32 [32768], P('node'), may hold values from 6000 to 9999
- ev_time: int32 [65536], P(('node', 'feat')), may hold values from 10000 to 11999
- nbr_gap: int32 [65536, 10], P(('node', 'feat')), may hold values from 1 to 1999
- slot_rows: int32 [128, 1536], P(('node', 'feat')), may hold values from -1 to 1023, as said below
- slot_ref: int32 [65536, 12], P(('node', 'feat')), may hold values from 0 to 1535, as said below
- edge_feat: bfloat16 [65536, 256], P('node', 'feat'), may hold values from -6 to 6
- frequency: float32 [100], replicated, may hold values from 0.001 to 0.1
- phase_shift: float32 [100], replicated, may hold values from -3.140625 to 3.140625
- w_query: bfloat16 [272, 272], replicated, may hold values from -0.375 to 0.375
- w_key: bfloat16 [272, 272], replicated, may hold values from -0.375 to 0.375
- w_value: bfloat16 [272, 272], replicated, may hold values from -0.375 to 0.375
- w_merge: bfloat16 [444, 172], replicated, may hold values from -0.25 to 0.25
- b_merge: float32 [172], replicated, may hold values from -3 to 3
- w_out: bfloat16 [172, 172], replicated, may hold values from -0.4375 to 0.4375
- b_out: float32 [172], replicated, may hold values from -3 to 3
- w_input: float32 [3, 700, 172], P(None, None, 'feat'), may hold values from -0.21875 to 0.21875
- w_hidden: float32 [3, 172, 172], P(None, None, 'feat'), may hold values from -0.4375 to 0.4375
- gru_bias: float32 [4, 172], P(None, 'feat'), may hold values from -3 to 3
Outputs:
- embedding: bfloat16 [65536, 172], P(('node', 'feat'))
- new_memory: float32 [32768, 172], P('node', 'feat')
The draws below stay inside these ranges and needn't reach their ends.
Inputs may be any that keep to these rules, and one draw needn't show every extreme that they name: `slot_rows`: row r lists the nodes read by events r * 512 to (r + 1) * 512 - 1: slot s asks owner s // 48 (an index along node) for one of its local rows, or holds -1. Within one owner's 48 slots the live ones come first and name distinct rows; every row has 1024 live slots. `slot_ref`: entries of event e name live slots of row e // 512 of slot_rows; every live slot is named by some event of its block.
All inputs are finite; a program needn't handle non-finite values.
Results may differ from the reference program's by a relative error of at most 0.01.
Values may be sent and summed in bfloat16 or wider, within the bound.
A program may use at most 128 MiB of HBM per device.

```python
import math
import jax
import jax.numpy as jnp
from jax import lax

MEM = 172
TIME = 100
MSGF = 256
EMB = 172
HEADS = 2
K = 10
EV_DEV = 512
NODE_DEV = 1024
ATT = 272
RAW = 700
CAP = 48
SLOTS = 1536
NODES = 32768
EVENTS = 65536
N_NODE = 32
N_FEAT = 4


def layout(key):
    device_total = N_NODE * N_FEAT
    quarter = EV_DEV // N_NODE
    key_hot, key_low, key_rows, key_first, key_extra, key_mix = jax.random.split(key, 6)
    hottest = jax.random.randint(key_hot, (), 0, N_NODE)
    lightest = (hottest + jax.random.randint(key_low, (device_total,), 1, N_NODE)) % N_NODE
    owners = jnp.arange(N_NODE, dtype=jnp.int32)
    loads = jnp.where(owners[None, :] == hottest, 3 * quarter, jnp.where(owners[None, :] == lightest[:, None], quarter, 2 * quarter))
    row_keys = jax.random.split(key_rows, device_total * N_NODE)
    drawn_rows = jax.vmap(lambda subkey: jax.random.permutation(subkey, NODE_DEV)[:CAP])(row_keys)
    drawn_rows = drawn_rows.reshape(device_total, N_NODE, CAP).astype(jnp.int32)
    filled = jnp.arange(CAP, dtype=jnp.int32)[None, None, :] < loads[:, :, None]
    slot_rows = jnp.where(filled, drawn_rows, -1).reshape(device_total, SLOTS).astype(jnp.int32)
    ranking = (1 - filled.reshape(device_total, SLOTS).astype(jnp.int32)) * SLOTS + jnp.arange(SLOTS, dtype=jnp.int32)[None, :]
    live_slots = jnp.argsort(ranking, axis=1)[:, :2 * EV_DEV].astype(jnp.int32)
    entry_total = EV_DEV * (K + 2)
    covering = jax.vmap(lambda subkey: jax.random.permutation(subkey, 2 * EV_DEV))(jax.random.split(key_first, device_total))
    further = jax.random.randint(key_extra, (device_total, entry_total - 2 * EV_DEV), 0, 2 * EV_DEV)
    picks = jnp.concatenate([covering.astype(jnp.int32), further.astype(jnp.int32)], 1)
    picks = jax.vmap(lambda subkey, entries: jax.random.permutation(subkey, entries))(jax.random.split(key_mix, device_total), picks)
    slot_ref = jnp.take_along_axis(live_slots, picks, axis=1).reshape(device_total * EV_DEV, K + 2).astype(jnp.int32)
    return (slot_rows, slot_ref)


def draw_slot_rows(key, part):
    return layout(jax.random.fold_in(key, 3))[0]


def draw_slot_ref(key, part):
    return layout(jax.random.fold_in(key, 3))[1]


def draw_memory(key, part):
    key = jax.random.fold_in(key, 11)
    key_base = jax.random.fold_in(key, 0)
    base_vals = jnp.clip(jax.random.normal(key_base, (NODES, MEM), jnp.float32), -6.0, 6.0)
    return base_vals


def set_ends(values, own_key, low, top_value):
    place = [jax.random.randint(jax.random.fold_in(own_key, axis), (), 0, length) for axis, length in enumerate(values.shape)]
    widest = values.shape.index(max(values.shape))
    beside = place[:widest] + [(place[widest] + 1) % values.shape[widest]] + place[widest + 1:]
    return values.at[tuple(place)].set(low).at[tuple(beside)].set(top_value)


def block_levels(rng, extent, cuts, least, high):
    loudness, own = 1.0, jax.random.fold_in(rng, 6)
    for axis_at, parts in cuts:
        draws = jnp.exp(jax.random.uniform(jax.random.fold_in(own, axis_at), (parts,), jnp.float32, least / len(cuts), high / len(cuts)))
        loudness = loudness * jnp.repeat(draws, extent[axis_at] // parts).reshape([-1 if axis == axis_at else 1 for axis in range(len(extent))])
    return loudness


def noise(key, dims, scale, bound, cuts=(), kind=jnp.bfloat16):
    drawn = jax.random.normal(key, dims, jnp.float32) * scale
    if len(cuts) > 0:
        drawn = block_levels(key, dims, cuts, -0.22, 0.18) * drawn
    return jnp.clip(drawn, min=-bound, max=bound).astype(kind)


def setup_inputs(seed: int = 0) -> dict:
    arg_keys = jax.random.split(jax.random.key(seed), 20)
    memory = draw_memory(jax.random.fold_in(arg_keys[19], 71), 0)
    last_update = set_ends(jax.random.randint(arg_keys[1], (NODES,), 6000, 10000), jax.random.fold_in(arg_keys[1], 1), 6000, 9999).astype(jnp.int32)
    ev_time = set_ends(jax.random.randint(arg_keys[2], (EVENTS,), 10000, 12000), jax.random.fold_in(arg_keys[2], 1), 10000, 11999).astype(jnp.int32)
    nbr_gap = set_ends(jax.random.randint(arg_keys[3], (EVENTS, K), 1, 2000), jax.random.fold_in(arg_keys[3], 1), 1, 1999).astype(jnp.int32)
    slot_rows = draw_slot_rows(jax.random.fold_in(arg_keys[19], 71), 0)
    slot_ref = draw_slot_ref(jax.random.fold_in(arg_keys[19], 71), 0)
    edge_feat = noise(arg_keys[6], (EVENTS, MSGF), 1.0, 6.0, ((0, 32), (1, 4)))
    frequency = jnp.clip(jnp.exp(jax.random.uniform(arg_keys[7], (TIME,), jnp.float32, math.log(0.001), math.log(0.1))), 0.001, 0.1)
    phase_shift = jnp.clip(jax.random.uniform(arg_keys[8], (TIME,), jnp.float32, -3.140625, 3.140625), -3.140625, 3.140625)
    w_query = noise(arg_keys[9], (ATT, ATT), ATT ** -0.5, 0.375)
    w_key = noise(arg_keys[10], (ATT, ATT), ATT ** -0.5, 0.375)
    w_value = noise(arg_keys[11], (ATT, ATT), ATT ** -0.5, 0.375)
    w_merge = noise(arg_keys[12], (ATT + MEM, EMB), (ATT + MEM) ** -0.5, 0.25)
    b_merge = noise(arg_keys[13], (EMB,), 0.5, 3.0, (), jnp.float32)
    w_out = noise(arg_keys[14], (EMB, EMB), EMB ** -0.5, 0.4375)
    b_out = noise(arg_keys[15], (EMB,), 0.5, 3.0, (), jnp.float32)
    w_input = noise(arg_keys[16], (3, RAW, MEM), RAW ** -0.5, 0.21875, ((2, 4),), jnp.float32)
    w_hidden = noise(arg_keys[17], (3, MEM, MEM), MEM ** -0.5, 0.4375, ((2, 4),), jnp.float32)
    gru_bias = noise(arg_keys[18], (4, MEM), 0.5, 3.0, ((1, 4),), jnp.float32)
    return dict(memory=memory, last_update=last_update, ev_time=ev_time, nbr_gap=nbr_gap, slot_rows=slot_rows, slot_ref=slot_ref, edge_feat=edge_feat, frequency=frequency, phase_shift=phase_shift, w_query=w_query, w_key=w_key, w_value=w_value, w_merge=w_merge, b_merge=b_merge, w_out=w_out, b_out=b_out, w_input=w_input, w_hidden=w_hidden, gru_bias=gru_bias)


precise = lax.Precision.HIGHEST

def time_code(gap_vals, frequency, phase_shift):
    return jnp.cos(gap_vals[..., None] * frequency + phase_shift)

def embed_events(source, neighbors, gap_vals, frequency, phase_shift, w_query, w_key, w_value, w_merge, b_merge, w_out, b_out):
    event_count = source.shape[0]
    nbr_count = neighbors.shape[1]
    att_width = w_query.shape[0]
    head_size = att_width // HEADS
    still_code = jnp.broadcast_to(jnp.cos(phase_shift), (event_count, phase_shift.shape[0]))
    query_in = jnp.concatenate([source, still_code], 1).astype(jnp.bfloat16)
    key_in = jnp.concatenate([neighbors, time_code(gap_vals, frequency, phase_shift)], 2).astype(jnp.bfloat16)
    key_in = key_in.reshape(event_count * nbr_count, att_width)
    queries = jnp.dot(query_in, w_query, preferred_element_type=jnp.float32).reshape(event_count, HEADS, head_size)
    key_vecs = jnp.dot(key_in, w_key, preferred_element_type=jnp.float32).reshape(event_count, nbr_count, HEADS, head_size)
    values = jnp.dot(key_in, w_value, preferred_element_type=jnp.float32).reshape(event_count, nbr_count, HEADS, head_size)
    scores = jnp.einsum('ehd,ekhd->ehk', queries, key_vecs, precision=precise) / math.sqrt(head_size)
    weights = jax.nn.softmax(scores, axis=2)
    attended = jnp.einsum('ehk,ekhd->ehd', weights, values, precision=precise).reshape(event_count, att_width)
    merged = jnp.concatenate([attended, source], 1).astype(jnp.bfloat16)
    hidden = jax.nn.relu(jnp.dot(merged, w_merge, preferred_element_type=jnp.float32) + b_merge).astype(jnp.bfloat16)
    return (jnp.dot(hidden, w_out, preferred_element_type=jnp.float32) + b_out).astype(jnp.bfloat16)

def build_messages(source, target, stamp_src, stamp_dst, ev_time, edge_rows, frequency, phase_shift):
    code_src = time_code((ev_time - stamp_src).astype(jnp.float32), frequency, phase_shift)
    code_dst = time_code((ev_time - stamp_dst).astype(jnp.float32), frequency, phase_shift)
    wide_edges = edge_rows.astype(jnp.float32)
    to_source = jnp.concatenate([source, target, code_src, wide_edges], 1)
    to_target = jnp.concatenate([target, source, code_dst, wide_edges], 1)
    return jnp.concatenate([to_source, to_target], 0)

def gru_update(inputs, previous, own_cols, w_hidden, gru_bias):
    recurrent = jnp.einsum('rn,gnm->grm', previous, w_hidden, precision=precise)
    reset_gate = jax.nn.sigmoid(inputs[0] + recurrent[0] + gru_bias[0])
    update_gate = jax.nn.sigmoid(inputs[1] + recurrent[1] + gru_bias[1])
    candidate = jnp.tanh(inputs[2] + gru_bias[2] + reset_gate * (recurrent[2] + gru_bias[3]))
    return (1.0 - update_gate) * candidate + update_gate * own_cols

def reference(memory, last_update, ev_time, nbr_gap, slot_rows, slot_ref, edge_feat, frequency, phase_shift, w_query, w_key, w_value, w_merge, b_merge, w_out, b_out, w_input, w_hidden, gru_bias):
    block_total = EVENTS // EV_DEV
    owner_of = (slot_ref // CAP).astype(jnp.int32)
    block_of = (jnp.arange(EVENTS, dtype=jnp.int32) // EV_DEV).astype(jnp.int32)
    local_rows = slot_rows[block_of[:, None], slot_ref]
    node_ids = (owner_of * NODE_DEV + local_rows).astype(jnp.int32)

    def scan_block(state_pair, block_inputs):
        totals, hit_counts = state_pair
        block_ids, block_times, block_gaps, edge_rows = block_inputs
        fetched = memory[block_ids]
        stamps = last_update[block_ids[:, :2]]
        embedded = embed_events(fetched[:, 0], fetched[:, 2:], block_gaps.astype(jnp.float32), frequency, phase_shift, w_query, w_key, w_value, w_merge, b_merge, w_out, b_out)
        message_rows = build_messages(fetched[:, 0], fetched[:, 1], stamps[:, 0], stamps[:, 1], block_times, edge_rows, frequency, phase_shift)
        endpoints = jnp.concatenate([block_ids[:, 0], block_ids[:, 1]])
        totals = totals.at[endpoints].add(message_rows)
        hit_counts = hit_counts.at[endpoints].add(jnp.ones(endpoints.shape, jnp.float32))
        return ((totals, hit_counts), embedded)
    initial = (jnp.zeros((NODES, RAW), jnp.float32), jnp.zeros((NODES,), jnp.float32))
    scanned = (node_ids.reshape(block_total, EV_DEV, K + 2), ev_time.reshape(block_total, EV_DEV), nbr_gap.reshape(block_total, EV_DEV, K), edge_feat.reshape(block_total, EV_DEV, MSGF))
    (totals, hit_counts), embedded = lax.scan(scan_block, initial, scanned)
    averaged = totals / jnp.maximum(hit_counts, 1.0)[:, None]
    inputs = jnp.einsum('rn,gnm->grm', averaged, w_input, precision=precise)
    renewed = gru_update(inputs, memory, memory, w_hidden, gru_bias)
    new_memory = jnp.where((hit_counts > 0.0)[:, None], renewed, memory)
    return (embedded.reshape(EVENTS, EMB), new_memory)
```

```python
import functools
import math

import jax
import jax.numpy as jnp
from jax import lax
from jax.experimental import pallas as pl
from jax.experimental.pallas import tpu as pltpu
from jax.sharding import PartitionSpec as P

F32, BF16, I32 = jnp.float32, jnp.bfloat16, jnp.int32
MESH = pl.DeviceIdType.MESH
COS = (
    0.9999999998851011,
    -0.49999999850736465,
    0.041666663483369594,
    -0.0013888863001969808,
    2.4800551963260593e-05,
    -2.7534774132807624e-07,
    2.060335926598073e-09,
    -9.721760760713551e-12,
)
TURN_HI = 6.28125
TURN_LO = 2.0 * math.pi - TURN_HI

MEM, TIME, ATT, EMB, UNITS = 172, 100, 272, 172, 43
CAP, K, EV, ROWS, SLOTS = 48, 10, 512, 1024, 1536
HEAD = ATT // 2
GROUPS, PEERS = 4, 32


def cosine(x):
    turns = jnp.floor(x * (0.5 / math.pi) + 0.5)
    r = (x - turns * TURN_HI) - turns * TURN_LO
    u = r * r
    total = jnp.full_like(u, COS[-1])
    for c in COS[-2::-1]:
        total = total * u + c
    return total


def mm(a, b):
    return jnp.dot(a, b, preferred_element_type=F32)


def mm_nt(a, b):
    return lax.dot_general(a, b, (((1,), (1,)), ((), ())), preferred_element_type=F32)


def iota(shape, dim):
    return lax.broadcasted_iota(I32, shape, dim)


def one_hot(mask):
    return jnp.where(mask, 1.0, 0.0).astype(BF16)


def kernel(
    memory,
    last_update,
    ev_time,
    nbr_gap,
    slot_rows,
    slot_ref,
    edge_feat,
    frequency,
    phase_shift,
    w_query,
    w_key,
    w_value,
    w_merge,
    b_merge,
    w_out,
    b_out,
    w_input,
    w_hidden,
    gru_bias,
    embedding,
    new_memory,
    req_send,
    req_recv,
    row_send,
    fetched,
    edge_recv,
    w_mine,
    wx_mine,
    w_all,
    wx_all,
    main_send,
    main_recv,
    ext_send,
    ext_recv,
    vec,
    memb,
    tail,
    small,
    times,
    wkv,
    wq,
    wm,
    zed,
    own,
    req_lanes,
    end_cols,
    hits,
    src,
    msg,
    ext_tmp,
    query,
    hot,
    near,
    kv,
    att,
    acc,
    send_sem,
    recv_req,
    recv_rows,
    recv_x,
    recv_main,
    recv_ext,
):
    n = lax.axis_index("node")
    f = lax.axis_index("feat")
    y, z, c = n // 8, (n // 2) % 4, n % 2

    def peer(dy, j, dx):
        to = ((y + dy) % 4) * 8 + ((z + j // 2) % 4) * 2 + (c + j % 2) % 2
        return to, (f + dx) % 4

    def send(src_ref, dst_ref, s_sem, r_sem, to):
        pltpu.make_async_remote_copy(
            src_ref=src_ref,
            dst_ref=dst_ref,
            send_sem=s_sem,
            recv_sem=r_sem,
            device_id=to,
            device_id_type=MESH,
        ).start()

    def wait_bytes(ref, sem):
        pltpu.make_async_copy(ref, ref, sem).wait()

    barrier = pltpu.get_barrier_semaphore()

    def greet(i, carry):
        to = peer(i // 32, i % 8, (i // 8) % 4)
        pl.semaphore_signal(barrier, inc=1, device_id=to, device_id_type=MESH)
        return carry

    lax.fori_loop(1, 128, greet, 0)

    req_send[...] = jnp.full(req_send.shape, -1, I32)
    for o in range(32):
        req_send[o, :, 0:CAP] = slot_rows[:, o * CAP : (o + 1) * CAP]
    req_recv[0] = req_send[n]
    edge_recv[f] = edge_feat[pl.ds(pl.multiple_of(f * EV, EV), EV), :]

    pl.semaphore_wait(barrier, 127)

    def ask(i, carry):
        dy, dx, j = i // 32, (i // 8) % 4, i % 8
        to = peer(dy, j, dx)
        send(req_send.at[to[0]], req_recv.at[i], send_sem.at[0], recv_req.at[1], to)
        return carry

    for dy in range(4):
        for j in range(8):
            if dy == 0 and j == 0:
                continue
            to = peer(dy, j, 0)
            send(
                req_send.at[to[0]],
                req_recv.at[dy * 32 + j],
                send_sem.at[0],
                recv_req.at[2 + dy],
                to,
            )
    for dy in range(4):
        lax.fori_loop(dy * 32 + 8, dy * 32 + 32, ask, 0)

    for dx in range(1, 4):
        to = peer(0, 0, dx)
        send(
            edge_feat.at[pl.ds(pl.multiple_of(to[1] * EV, EV), EV), :],
            edge_recv.at[f],
            send_sem.at[1],
            recv_x.at[0],
            to,
        )

    small[...] = jnp.zeros(small.shape, F32)
    small[0:8, :] = last_update[...].astype(F32)
    stamp_cols = small[...].T
    tail[:, 0:44] = memory[:, 128:MEM]
    lane = iota((128, 128), 1)
    memb[:, 0:128] = memory[:, 0:128].astype(BF16)
    for b in range(8):
        stamp = stamp_cols[:, b : b + 1]
        high = jnp.floor(stamp * (1.0 / 128.0))
        low = stamp - high * 128.0
        part = tail[b * 128 : (b + 1) * 128, :]
        part = jnp.where(
            lane < 44, part, jnp.where(lane == 44, high, jnp.where(lane == 45, low, 0.0))
        )
        memb[b * 128 : (b + 1) * 128, 128:256] = part.astype(BF16)

    r640 = iota((640, 700), 0)
    c640 = iota((640, 700), 1)
    picked = (
        ((r640 < MEM) & (c640 == r640 + MEM))
        | ((r640 >= 256) & (r640 < 256 + TIME) & (c640 == r640 - 256 + 2 * MEM))
        | ((r640 >= 384) & (c640 == r640 - 384 + 2 * MEM + TIME))
    )
    place = one_hot(picked)
    rows43 = iota((UNITS, 128), 0)
    cols43 = iota((UNITS, 128), 1)
    wide = mm(w_input[0].astype(BF16), one_hot(cols43 == rows43))
    wide += mm(w_input[1].astype(BF16), one_hot(cols43 == rows43 + UNITS))
    wide += mm(w_input[2].astype(BF16), one_hot(cols43 == rows43 + 2 * UNITS))
    w_mine[...] = mm(place, wide.astype(BF16)).astype(BF16)
    last = mm_nt(one_hot(iota((8, UNITS), 1) == UNITS - 1), w_input[2].astype(BF16))
    wx_mine[...] = mm_nt(last.astype(BF16), place)[0:1, :]
    w_all[0] = w_mine[...]
    wx_all[0] = wx_mine[...]
    for dx in range(1, 4):
        to = peer(0, 0, 4 - dx)
        send(w_mine, w_all.at[dx], send_sem.at[2], recv_x.at[1], to)
        send(wx_mine, wx_all.at[dx], send_sem.at[3], recv_x.at[2], to)

    for dy in range(4):
        first = 1 if dy == 0 else 0
        wait_bytes(req_recv.at[dy * 32 + first : dy * 32 + 8], recv_req.at[2 + dy])
    for dy in range(4):
        small[8 * dy : 8 * dy + 8, :] = req_recv[dy * 32 : dy * 32 + 8].reshape(8, 128).astype(F32)
    asked = small[...].T.astype(I32)
    row_lane = iota((CAP, ROWS), 1)
    for dy in range(4):
        mask = jnp.concatenate(
            [
                one_hot(asked[0:CAP, 8 * dy + j : 8 * dy + j + 1] == row_lane)
                for j in range(8)
            ],
            axis=0,
        )
        rows = mm(mask, memb[...]).astype(BF16)
        for j in range(8):
            piece = rows[j * CAP : (j + 1) * CAP, :]
            if dy == 0 and j == 0:
                fetched[n] = piece
            else:
                row_send[dy * 8 + j] = piece
                to_n = ((y - dy + 4) % 4) * 8 + ((z - j // 2 + 4) % 4) * 2 + (c + j % 2) % 2
                send(
                    row_send.at[dy * 8 + j],
                    fetched.at[n],
                    send_sem.at[4],
                    recv_rows,
                    (to_n, f),
                )

    vec[...] = jnp.zeros(vec.shape, F32)
    vec[0:1, 0:TIME] = frequency[...]
    vec[1:2, 0:TIME] = phase_shift[...]
    vec[2:3, 0:EMB] = b_merge[...]
    vec[3:4, 0:EMB] = b_out[...]
    vec[4:8, 0:UNITS] = gru_bias[...]
    freq = vec[0:1, 0:128]
    phase = vec[1:2, 0:128]

    for k in range(K):
        times[k] = cosine(nbr_gap[:, k : k + 1].astype(F32) * freq + phase).astype(BF16)

    r272 = iota((384, ATT), 0)
    c272 = iota((384, ATT), 1)
    place = one_hot(
        ((c272 < MEM) & (r272 == c272)) | ((c272 >= MEM) & (r272 == c272 + (256 - MEM)))
    )
    wkv[...] = jnp.zeros(wkv.shape, BF16)
    wkv[:, 0:ATT] = mm(place, w_key[...]).astype(BF16)
    wkv[:, 384 : 384 + ATT] = mm(place, w_value[...]).astype(BF16)
    wq[...] = jnp.zeros(wq.shape, BF16)
    wq[:, 0:ATT] = mm(place, w_query[...]).astype(BF16)
    r444 = iota((640, ATT + MEM), 0)
    c444 = iota((640, ATT + MEM), 1)
    place = one_hot(
        ((c444 < ATT) & (r444 == c444)) | ((c444 >= ATT) & (r444 == c444 + (384 - ATT)))
    )
    wm[...] = mm(place, w_merge[...]).astype(BF16)

    tail[...] = jnp.zeros(tail.shape, F32)
    tail[0:EV, 0 : K + 2] = slot_ref[...].astype(F32)
    cols = tail[0:EV, :].T.astype(I32)
    end_cols[:, 0:EV] = cols[0:1, :]
    end_cols[:, EV : 2 * EV] = cols[1:2, :]

    wait_bytes(fetched.at[0:31], recv_rows)
    table = fetched.reshape(SLOTS, 256)

    slot_lane = iota((256, SLOTS), 1)
    count = jnp.zeros((1, SLOTS), F32)
    for b in range(2):
        picks = slot_ref[b * 256 : (b + 1) * 256, :]
        for e in range(2):
            mask = jnp.where(picks[:, e : e + 1] == slot_lane, 1.0, 0.0)
            count += jnp.sum(mask, axis=0, keepdims=True)
            src[e, b * 256 : (b + 1) * 256, :] = mm(mask.astype(BF16), table[...])
    hits[...] = count

    small[...] = jnp.zeros(small.shape, F32)
    small[0:4, :] = ev_time[...].astype(F32)
    ev_cols = small[...].T
    lane = iota((EV, 128), 1)
    wait_bytes(edge_recv.at[0:3], recv_x.at[0])
    for half in range(2):
        pair = jnp.concatenate(
            [edge_recv[2 * half].astype(F32), edge_recv[2 * half + 1].astype(F32)], axis=1
        ).astype(BF16)
        for e in range(2):
            msg[e * EV : (e + 1) * EV, 384 + half * 128 : 512 + half * 128] = pair
    for e in range(2):
        msg[e * EV : (e + 1) * EV, 0:256] = src[1 - e].astype(BF16)
        for b in range(4):
            stamp = (
                src[e, b * 128 : (b + 1) * 128, MEM : MEM + 1] * 128.0
                + src[e, b * 128 : (b + 1) * 128, MEM + 1 : MEM + 2]
            )
            gap = ev_cols[:, b : b + 1] - stamp
            msg[e * EV + b * 128 : e * EV + (b + 1) * 128, 256:384] = cosine(
                gap * freq + phase
            ).astype(BF16)

    wait_bytes(w_all.at[0:3], recv_x.at[1])
    wait_bytes(wx_all.at[0:3], recv_x.at[2])
    ext_send[...] = jnp.zeros(ext_send.shape, F32)

    def give(step, carry):
        dy = (step + 1) % 4
        base = ((y + dy) % 4) * 384
        mask = one_hot(iota((384, 2 * EV), 0) + base == end_cols[...])
        sums = mm(mask, msg[...]).astype(BF16)
        for pair in range(2):
            w_pair = jnp.concatenate([w_all[2 * pair], w_all[2 * pair + 1]], axis=1)
            out = mm(sums, w_pair).astype(BF16)
            for i in range(2):
                main_send[dy, 2 * pair + i] = out[:, i * 128 : (i + 1) * 128].reshape(8, CAP, 128)
        rows4 = jnp.concatenate(
            [wx_all[dx] for dx in range(4)] + [jnp.zeros((4, 640), F32)], axis=0
        )
        ext_tmp[0:8, :] = mm_nt(rows4.astype(BF16), sums)
        ext_tmp[8:9, :] = hits[:, pl.ds(pl.multiple_of(base, 128), 384)]
        for j in range(8):
            count_row = ext_tmp[8:9, j * CAP : (j + 1) * CAP]
            for dx in range(4):
                ext_send[dy, dx, j, :, 0:CAP] = ext_tmp[dx : dx + 1, j * CAP : (j + 1) * CAP]
                ext_send[dy, dx, j, :, 64 : 64 + CAP] = count_row

        def post(i, inner):
            dx, j = i % 4, i // 4
            to = peer(dy, j, dx)
            at = to[0] % 8
            send(
                main_send.at[dy, dx, at],
                main_recv.at[dy, dx * 8 + j],
                send_sem.at[5],
                recv_main.at[dy],
                to,
            )
            send(
                ext_send.at[dy, dx, at],
                ext_recv.at[dy, dx * 8 + j],
                send_sem.at[6],
                recv_ext.at[dy],
                to,
            )
            return inner

        lax.fori_loop(jnp.where(dy == 0, 1, 0), 32, post, 0)
        return carry

    lax.fori_loop(0, 4, give, 0)
    main_recv[0, 0] = main_send[0, 0, n % 8]
    ext_recv[0, 0] = ext_send[0, 0, n % 8]

    still = jnp.broadcast_to(cosine(phase), (EV, 128)).astype(BF16)
    query[...] = (
        mm(src[0].astype(BF16), wq[0:256, :]) + mm(still, wq[256:384, :])
    ) * (1.0 / math.sqrt(HEAD))
    lane_q = iota((16, 384), 1)
    first_head = lane_q < HEAD
    slot_lane = iota((128, SLOTS), 1)

    def attend(b, carry):
        at = pl.multiple_of(b * 128, 128)
        picks = slot_ref[pl.ds(at, 128), :]
        for k in range(K):
            hot[k * 128 : (k + 1) * 128, :] = one_hot(picks[:, 2 + k : 3 + k] == slot_lane)
        near[...] = mm(hot[...], table[...]).astype(BF16)
        code = times[:, pl.ds(at, 128), :].reshape(K * 128, 128)
        kv[...] = (mm(near[...], wkv[0:256, :]) + mm(code, wkv[256:384, :])).reshape(K, 128, 768)

        def group(g, inner):
            r = pl.multiple_of(g * 16, 16)
            q = query[pl.ds(at + r, 16), :]
            s0, s1 = [], []
            for k in range(K):
                t = q * kv[k, pl.ds(r, 16), 0:384]
                s0.append(jnp.sum(jnp.where(first_head, t, 0.0), axis=1, keepdims=True))
                s1.append(jnp.sum(jnp.where(first_head, 0.0, t), axis=1, keepdims=True))
            m0 = functools.reduce(jnp.maximum, s0)
            m1 = functools.reduce(jnp.maximum, s1)
            p0 = [jnp.exp(s - m0) for s in s0]
            p1 = [jnp.exp(s - m1) for s in s1]
            total = jnp.zeros((16, 384), F32)
            for k in range(K):
                w = jnp.where(first_head, p0[k], p1[k])
                total += w * kv[k, pl.ds(r, 16), 384:768]
            norm = jnp.where(first_head, sum(p0), sum(p1))
            att[pl.ds(at + r, 16), :] = (total / norm).astype(BF16)
            return inner

        lax.fori_loop(0, 8, group, 0)
        return carry

    lax.fori_loop(0, 4, attend, 0)
    hidden = mm(att[...], wm[0:384, :]) + mm(src[0].astype(BF16), wm[384:640, :])
    hidden = jnp.maximum(hidden + vec[2:3, 0:EMB], 0.0).astype(BF16)
    embedding[...] = (mm(hidden, w_out[...]) + vec[3:4, 0:EMB]).astype(BF16)

    rows172 = iota((UNITS, 128), 0)
    cols172 = iota((UNITS, 128), 1)
    widen = one_hot(rows172 == cols172)
    pad = one_hot(iota((256, MEM), 0) == iota((256, MEM), 1))
    gates = (
        w_input[0, 0:MEM, :] + w_hidden[0],
        w_input[1, 0:MEM, :] + w_hidden[1],
        w_input[2, 0:MEM, :],
        w_hidden[2],
    )
    for g, w in enumerate(gates):
        w_wide = mm(w.astype(BF16), widen).astype(BF16)
        zed[g] = mm(memb[...], mm(pad, w_wide).astype(BF16))
    own[...] = jnp.dot(
        memory[...],
        jnp.where(
            (iota((MEM, 128), 0) == iota((MEM, 128), 1) + f * UNITS) & (iota((MEM, 128), 1) < UNITS),
            1.0,
            0.0,
        ),
        preferred_element_type=F32,
        precision=lax.Precision.HIGHEST,
    )

    wait_bytes(req_recv.at[0:96], recv_req.at[1])
    for i in range(128):
        dy, j = i // 32, i % 32
        req_lanes[dy, :, j * CAP : (j + 1) * CAP] = req_recv[i, :, 0:CAP]

    acc[...] = jnp.zeros(acc.shape, F32)
    lane48 = iota((CAP, 128), 1)
    for dy in (1, 2, 3, 0):
        first = 1 if dy == 0 else 0
        wait_bytes(main_recv.at[dy, first:32], recv_main.at[dy])
        wait_bytes(ext_recv.at[dy, first:32], recv_ext.at[dy])
        small[...] = jnp.zeros(small.shape, F32)
        small[0:32, :] = ext_recv[dy].reshape(32, 128)
        ext_t = small[...].T
        count = ext_t[64 : 64 + CAP, :]
        high = jnp.floor(count * (1.0 / 128.0))
        low = count - high * 128.0
        both = jnp.where(
            lane48 < 32,
            ext_t[0:CAP, :],
            jnp.where(
                lane48 < 64,
                pltpu.roll(low, 32, axis=1),
                jnp.where(lane48 < 96, pltpu.roll(high, 64, axis=1), 0.0),
            ),
        )
        side = jnp.concatenate(
            [jnp.where(lane48 % 32 == i, both, 0.0).astype(BF16) for i in range(32)], axis=0
        )
        right = jnp.concatenate([main_recv[dy].reshape(SLOTS, 128), side], axis=1)
        for b in range(4):
            mask = one_hot(iota((256, SLOTS), 0) + b * 256 == req_lanes[dy])
            acc[b * 256 : (b + 1) * 256, :] += mm(mask, right)

    lane = iota((256, 128), 1)
    for b in range(4):
        at = slice(b * 256, (b + 1) * 256)
        main = acc[at, 0:128]
        extra = acc[at, 128:256]
        last_unit = jnp.sum(jnp.where(lane < 32, extra, 0.0), axis=1, keepdims=True)
        heard = jnp.sum(
            jnp.where(
                (lane >= 32) & (lane < 64),
                extra,
                jnp.where((lane >= 64) & (lane < 96), extra * 128.0, 0.0),
            ),
            axis=1,
            keepdims=True,
        )
        share = 1.0 / jnp.maximum(heard, 1.0)
        i1 = pltpu.roll(main, 128 - UNITS, axis=1)
        i2 = jnp.where(lane == UNITS - 1, last_unit, pltpu.roll(main, 128 - 2 * UNITS, axis=1))
        b0, b1, b2, b3 = (vec[4 + g : 5 + g, 0:128] for g in range(4))
        reset = jax.nn.sigmoid(main * share + zed[0, at, :] + b0)
        update = jax.nn.sigmoid(i1 * share + zed[1, at, :] + b1)
        cand = jnp.tanh(i2 * share + zed[2, at, :] + b2 + reset * (zed[3, at, :] + b3))
        mine = own[at, :]
        fresh = (1.0 - update) * cand + update * mine
        new_memory[at, :] = jnp.where(heard > 0.0, fresh, mine)[:, 0:UNITS]

    wait_bytes(req_recv.at[0:127], send_sem.at[0])
    wait_bytes(edge_recv.at[0:3], send_sem.at[1])
    wait_bytes(w_all.at[0:3], send_sem.at[2])
    wait_bytes(wx_all.at[0:3], send_sem.at[3])
    wait_bytes(row_send.at[0:31], send_sem.at[4])
    wait_bytes(main_recv.at[0:3], send_sem.at[5])
    wait_bytes(main_recv.at[3, 0:31], send_sem.at[5])
    wait_bytes(ext_recv.at[0:3], send_sem.at[6])
    wait_bytes(ext_recv.at[3, 0:31], send_sem.at[6])


def step(
    memory,
    last_update,
    ev_time,
    nbr_gap,
    slot_rows,
    slot_ref,
    edge_feat,
    frequency,
    phase_shift,
    w_query,
    w_key,
    w_value,
    w_merge,
    b_merge,
    w_out,
    b_out,
    w_input,
    w_hidden,
    gru_bias,
):
    args = (
        memory,
        last_update.reshape(8, 128),
        ev_time.reshape(4, 128),
        nbr_gap,
        slot_rows,
        slot_ref,
        edge_feat,
        frequency.reshape(1, TIME),
        phase_shift.reshape(1, TIME),
        w_query,
        w_key,
        w_value,
        w_merge,
        b_merge.reshape(1, EMB),
        w_out,
        b_out.reshape(1, EMB),
        w_input,
        w_hidden,
        gru_bias,
    )
    vmem = pl.BlockSpec(memory_space=pltpu.VMEM)
    V, D = pltpu.VMEM, pltpu.SemaphoreType.DMA
    return pl.pallas_call(
        kernel,
        out_shape=(
            jax.ShapeDtypeStruct((EV, EMB), BF16),
            jax.ShapeDtypeStruct((ROWS, UNITS), F32),
        ),
        in_specs=[vmem] * len(args),
        out_specs=(vmem, vmem),
        scratch_shapes=[
            V((32, 1, 128), I32),
            V((128, 1, 128), I32),
            V((32, CAP, 256), BF16),
            V((32, CAP, 256), BF16),
            V((4, EV, 64), BF16),
            V((640, 128), BF16),
            V((1, 640), F32),
            V((4, 640, 128), BF16),
            V((4, 1, 640), F32),
            V((4, 4, 8, CAP, 128), BF16),
            V((4, 32, CAP, 128), BF16),
            V((4, 4, 8, 1, 128), F32),
            V((4, 32, 1, 128), F32),
            V((8, 256), F32),
            V((ROWS, 256), BF16),
            V((ROWS, 128), F32),
            V((128, 128), F32),
            V((K, EV, 128), BF16),
            V((384, 768), BF16),
            V((384, 384), BF16),
            V((640, EMB), BF16),
            V((4, ROWS, 128), F32),
            V((ROWS, 128), F32),
            V((4, 1, SLOTS), I32),
            V((1, 2 * EV), I32),
            V((1, SLOTS), F32),
            V((2, EV, 256), F32),
            V((2 * EV, 640), BF16),
            V((16, 384), F32),
            V((EV, 384), F32),
            V((K * 128, SLOTS), BF16),
            V((K * 128, 256), BF16),
            V((K, 128, 768), F32),
            V((EV, 384), BF16),
            V((ROWS, 256), F32),
            D((7,)),
            D((6,)),
            D,
            D((3,)),
            D((4,)),
            D((4,)),
        ],
        compiler_params=pltpu.CompilerParams(
            collective_id=0, has_side_effects=True, vmem_limit_bytes=60 * 1024 * 1024
        ),
    )(*args)


def solution(mesh):
    return jax.shard_map(
        step,
        mesh=mesh,
        in_specs=(
            P("node", None),
            P("node"),
            P(("node", "feat")),
            P(("node", "feat"), None),
            P(("node", "feat"), None),
            P(("node", "feat"), None),
            P("node", "feat"),
            P(),
            P(),
            P(),
            P(),
            P(),
            P(),
            P(),
            P(),
            P(),
            P(None, None, "feat"),
            P(None, None, "feat"),
            P(None, "feat"),
        ),
        out_specs=(P(("node", "feat"), None), P("node", "feat")),
        check_vma=False,
    )
```

```python
import functools
import math

import jax
import jax.numpy as jnp
from jax import lax
from jax.experimental import pallas as pl
from jax.experimental.pallas import tpu as pltpu
from jax.sharding import PartitionSpec as P

F32, BF16, I32 = jnp.float32, jnp.bfloat16, jnp.int32
MESH = pl.DeviceIdType.MESH
COS = (
    0.9999999998851011,
    -0.49999999850736465,
    0.041666663483369594,
    -0.0013888863001969808,
    2.4800551963260593e-05,
    -2.7534774132807624e-07,
    2.060335926598073e-09,
    -9.721760760713551e-12,
)
TURN_HI = 6.28125
TURN_LO = 2.0 * math.pi - TURN_HI

MEM, TIME, ATT, EMB, UNITS = 172, 100, 272, 172, 43
CAP, K, EV, ROWS, SLOTS = 48, 10, 512, 1024, 1536
HEAD = ATT // 2
GROUPS, PEERS = 4, 32


def cosine(x):
    turns = jnp.floor(x * (0.5 / math.pi) + 0.5)
    r = (x - turns * TURN_HI) - turns * TURN_LO
    u = r * r
    total = jnp.full_like(u, COS[-1])
    for c in COS[-2::-1]:
        total = total * u + c
    return total


def mm(a, b):
    return jnp.dot(a, b, preferred_element_type=F32)


def mm_nt(a, b):
    return lax.dot_general(a, b, (((1,), (1,)), ((), ())), preferred_element_type=F32)


def iota(shape, dim):
    return lax.broadcasted_iota(I32, shape, dim)


def one_hot(mask):
    return jnp.where(mask, 1.0, 0.0).astype(BF16)


def kernel(
    memory,
    last_update,
    ev_time,
    nbr_gap,
    slot_rows,
    slot_ref,
    edge_feat,
    frequency,
    phase_shift,
    w_query,
    w_key,
    w_value,
    w_merge,
    b_merge,
    w_out,
    b_out,
    w_input,
    w_hidden,
    gru_bias,
    embedding,
    new_memory,
    req_send,
    req_recv,
    row_send,
    fetched,
    edge_recv,
    w_mine,
    wx_mine,
    w_all,
    wx_all,
    main_send,
    main_recv,
    ext_send,
    ext_recv,
    vec,
    mem_t,
    memb,
    wide_t,
    cols,
    small,
    times,
    wkv,
    wq,
    wm,
    w_ext,
    zed,
    own,
    end_cols,
    hits,
    ends,
    src,
    msg,
    ext_tmp,
    query,
    hot,
    near,
    kv,
    att,
    claims,
    side,
    acc,
    send_sem,
    recv_req,
    recv_rows,
    recv_x,
    recv_main,
    recv_ext,
):
    n = lax.axis_index("node")
    f = lax.axis_index("feat")
    y, z, c = n // 8, (n // 2) % 4, n % 2
    at_y = [((y + d) % 4) * 8 for d in range(4)]
    at_z = [((z + d) % 4) * 2 for d in range(4)]
    at_c = [(c + d) % 2 for d in range(2)]
    at_f = [(f + d) % 4 for d in range(4)]
    in_y = [at_z[j // 2] + at_c[j % 2] for j in range(8)]

    def peer(dy, j, dx):
        return at_y[dy] + in_y[j], at_f[dx]

    def send(src_ref, dst_ref, s_sem, r_sem, to):
        pltpu.make_async_remote_copy(
            src_ref=src_ref,
            dst_ref=dst_ref,
            send_sem=s_sem,
            recv_sem=r_sem,
            device_id=to,
            device_id_type=MESH,
        ).start()

    def wait_bytes(ref, sem):
        pltpu.make_async_copy(ref, ref, sem).wait()

    everyone = [(dy, dx, j) for dy in range(4) for dx in range(4) for j in range(8)][1:]

    for dx in range(4):
        w_all[dx, 176:256, :] = jnp.zeros((80, 128), BF16)
        w_all[dx, 368:384, :] = jnp.zeros((16, 128), BF16)

    barrier = pltpu.get_barrier_semaphore()
    for dy, dx, j in everyone:
        pl.semaphore_signal(
            barrier, inc=1, device_id=peer(dy, j, dx), device_id_type=MESH
        )

    req_send[...] = jnp.full(req_send.shape, -1, I32)
    for o in range(32):
        req_send[o, :, 0:CAP] = slot_rows[:, o * CAP : (o + 1) * CAP]
    req_recv[0] = req_send[n]
    edge_recv[f] = edge_feat[:, pl.ds(pl.multiple_of(f * EV, EV), EV)]

    mem_t[0:MEM, :] = memory[...]
    stamp = last_update[...].astype(F32)
    high = jnp.floor(stamp * (1.0 / 128.0))
    mem_t[MEM : MEM + 1, :] = high
    mem_t[MEM + 1 : MEM + 2, :] = stamp - high * 128.0
    mem_t[MEM + 2 : 256, :] = jnp.zeros((256 - MEM - 2, ROWS), F32)
    for b in range(4):
        memb[b * 256 : (b + 1) * 256, :] = mem_t[:, b * 256 : (b + 1) * 256].T.astype(BF16)

    pl.semaphore_wait(barrier, 127)

    for dy, dx, j in everyone:
        if dx == 0:
            to = peer(dy, j, 0)
            send(
                req_send.at[to[0]],
                req_recv.at[dy * 32 + j],
                send_sem.at[0],
                recv_req.at[2 + dy],
                to,
            )
    for dx in range(1, 4):
        to = peer(0, 0, dx)
        send(
            edge_feat.at[:, pl.ds(pl.multiple_of(to[1] * EV, EV), EV)],
            edge_recv.at[f],
            send_sem.at[1],
            recv_x.at[0],
            to,
        )

    r640 = iota((640, 700), 0)
    c640 = iota((640, 700), 1)
    place = one_hot(
        ((r640 < MEM) & (c640 == r640 + MEM))
        | ((r640 >= 256) & (r640 < 256 + TIME) & (c640 == r640 - 256 + 2 * MEM))
        | ((r640 >= 384) & (c640 == r640 - 384 + 2 * MEM + TIME))
    )
    rows43 = iota((128, UNITS), 0)
    cols43 = iota((128, UNITS), 1)
    wide = mm(one_hot(rows43 == cols43), w_input[0].astype(BF16))
    wide += mm(one_hot(rows43 == cols43 + UNITS), w_input[1].astype(BF16))
    wide += mm(one_hot(rows43 == cols43 + 2 * UNITS), w_input[2].astype(BF16))
    w_mine[...] = mm_nt(place, wide.astype(BF16)).astype(BF16)
    last = mm(one_hot(iota((8, UNITS), 1) == UNITS - 1), w_input[2].astype(BF16))
    wx_mine[...] = mm_nt(last.astype(BF16), place)[0:1, :]
    for dx in range(1, 4):
        to = peer(0, 0, 4 - dx)
        for rows in (slice(0, 176), slice(256, 368), slice(384, 640)):
            send(w_mine.at[rows], w_all.at[dx, rows], send_sem.at[2], recv_x.at[1], to)
        send(wx_mine, wx_all.at[dx], send_sem.at[3], recv_x.at[2], to)
    w_all[0] = w_mine[...]
    wx_all[0] = wx_mine[...]

    for dy in range(4):
        first = 1 if dy == 0 else 0
        wait_bytes(req_recv.at[dy * 32 + first : dy * 32 + 8], recv_req.at[2 + dy])
    small[...] = jnp.zeros(small.shape, F32)
    for dy in range(4):
        small[8 * dy : 8 * dy + 8, :] = req_recv[dy * 32 : dy * 32 + 8].reshape(8, 128).astype(F32)
    asked = small[...].T.astype(I32)
    row_lane = iota((CAP, ROWS), 1)
    for dy in (2, 1, 3, 0):
        mask = jnp.concatenate(
            [
                one_hot(asked[0:CAP, 8 * dy + j : 8 * dy + j + 1] == row_lane)
                for j in range(8)
            ],
            axis=0,
        )
        rows = mm(mask, memb[...]).astype(BF16)
        for j in range(8):
            piece = rows[j * CAP : (j + 1) * CAP, :]
            if dy == 0 and j == 0:
                fetched[n] = piece
            else:
                row_send[dy * 8 + j] = piece
                back = (4 - j // 2) % 4 * 2 + j % 2
                send(
                    row_send.at[dy * 8 + j],
                    fetched.at[n],
                    send_sem.at[4],
                    recv_rows,
                    peer((4 - dy) % 4, back, 0),
                )

    for dy, dx, j in everyone:
        if dx != 0:
            to = peer(dy, j, dx)
            send(
                req_send.at[to[0]],
                req_recv.at[dy * 32 + dx * 8 + j],
                send_sem.at[0],
                recv_req.at[1],
                to,
            )

    vec[...] = jnp.zeros(vec.shape, F32)
    vec[0:1, 0:TIME] = frequency[...]
    vec[1:2, 0:TIME] = phase_shift[...]
    vec[2:3, 0:EMB] = b_merge[...]
    vec[3:4, 0:EMB] = b_out[...]
    vec[4:8, 0:UNITS] = gru_bias[...]
    freq = vec[0:1, 0:128]
    phase = vec[1:2, 0:128]

    wide_t[...] = jnp.zeros(wide_t.shape, F32)
    wide_t[0 : K + 2, :] = slot_ref[...].astype(F32)
    wide_t[16 : 16 + K, :] = nbr_gap[...].astype(F32)
    wide_t[32:33, :] = ev_time[...].astype(F32)
    cols[...] = wide_t[...].T
    end_cols[:, 0:EV] = slot_ref[0:1, :]
    end_cols[:, EV : 2 * EV] = slot_ref[1:2, :]

    for k in range(K):
        times[k] = cosine(cols[:, 16 + k : 17 + k] * freq + phase).astype(BF16)

    slot_lane = iota((128, SLOTS), 1)

    def mark(b, count):
        picks = cols[pl.ds(pl.multiple_of(b * 128, 128), 128), :].astype(I32)
        for k in range(K):
            hot[b, k * 128 : (k + 1) * 128, :] = one_hot(picks[:, 2 + k : 3 + k] == slot_lane)
        for e in range(2):
            mask = jnp.where(picks[:, e : e + 1] == slot_lane, 1.0, 0.0)
            count += jnp.sum(mask, axis=0, keepdims=True)
            ends[e, pl.ds(pl.multiple_of(b * 128, 128), 128), :] = mask.astype(BF16)
        return count

    hits[...] = lax.fori_loop(0, 4, mark, jnp.zeros((1, SLOTS), F32))

    r272 = iota((384, ATT), 0)
    c272 = iota((384, ATT), 1)
    place = one_hot(
        ((c272 < MEM) & (r272 == c272)) | ((c272 >= MEM) & (r272 == c272 + (256 - MEM)))
    )
    wkv[...] = jnp.zeros(wkv.shape, BF16)
    wkv[:, 0:ATT] = mm(place, w_key[...]).astype(BF16)
    wkv[:, 384 : 384 + ATT] = mm(place, w_value[...]).astype(BF16)
    wq[...] = jnp.zeros(wq.shape, BF16)
    wq[:, 0:ATT] = mm(place, w_query[...]).astype(BF16)
    r444 = iota((640, ATT + MEM), 0)
    c444 = iota((640, ATT + MEM), 1)
    place = one_hot(
        ((c444 < ATT) & (r444 == c444)) | ((c444 >= ATT) & (r444 == c444 + (384 - ATT)))
    )
    wm[...] = mm_nt(place, w_merge[...]).astype(BF16)

    widen = one_hot(iota((CAP, UNITS), 0) == iota((CAP, UNITS), 1))
    mem_b = memory[...].astype(BF16)
    gates = (
        w_input[0, :, 0:MEM] + w_hidden[0],
        w_input[1, :, 0:MEM] + w_hidden[1],
        w_input[2, :, 0:MEM],
        w_hidden[2],
    )
    for g, w in enumerate(gates):
        zed[g] = mm(mm(widen, w.astype(BF16)).astype(BF16), mem_b)
    own[...] = jnp.dot(
        jnp.where(
            (iota((CAP, MEM), 1) == iota((CAP, MEM), 0) + f * UNITS)
            & (iota((CAP, MEM), 0) < UNITS),
            1.0,
            0.0,
        ),
        memory[...],
        preferred_element_type=F32,
        precision=lax.Precision.HIGHEST,
    )

    wait_bytes(edge_recv.at[0:3], recv_x.at[0])
    edges = edge_recv[...].reshape(256, EV).astype(F32).T.astype(BF16)
    for e in range(2):
        msg[e * EV : (e + 1) * EV, 384:640] = edges
    ext_send[...] = jnp.zeros(ext_send.shape, F32)

    wait_bytes(fetched.at[0:31], recv_rows)
    table = fetched.reshape(SLOTS, 256)

    for e in range(2):
        src[e] = mm(ends[e], table[...])
    for e in range(2):
        msg[e * EV : (e + 1) * EV, 0:256] = src[1 - e].astype(BF16)
        stamp = src[e, :, MEM : MEM + 1] * 128.0 + src[e, :, MEM + 1 : MEM + 2]
        gap = cols[:, 32:33] - stamp
        msg[e * EV : (e + 1) * EV, 256:384] = cosine(gap * freq + phase).astype(BF16)

    wait_bytes(w_all.at[0:3, 0:544], recv_x.at[1])
    wait_bytes(wx_all.at[0:3], recv_x.at[2])
    rows4 = jnp.concatenate([wx_all[dx] for dx in range(4)] + [jnp.zeros((4, 640), F32)], axis=0)
    w_ext[...] = rows4.astype(BF16)

    for dy in (2, 1, 3, 0):
        base = at_y[dy] * CAP
        mask = one_hot(iota((384, 2 * EV), 0) + base == end_cols[...])
        sums = mm(mask, msg[...]).astype(BF16)
        for pair in range(2):
            w_pair = jnp.concatenate([w_all[2 * pair], w_all[2 * pair + 1]], axis=1)
            out = mm(sums, w_pair).astype(BF16)
            for i in range(2):
                main_send[dy, 2 * pair + i] = out[:, i * 128 : (i + 1) * 128].reshape(8, CAP, 128)
        ext_tmp[0:8, :] = mm_nt(w_ext[...], sums)
        ext_tmp[8:9, :] = hits[:, pl.ds(pl.multiple_of(base, 128), 384)]
        for j in range(8):
            count_row = ext_tmp[8:9, j * CAP : (j + 1) * CAP]
            for dx in range(4):
                ext_send[dy, dx, j, :, 0:CAP] = ext_tmp[dx : dx + 1, j * CAP : (j + 1) * CAP]
                ext_send[dy, dx, j, :, 64 : 64 + CAP] = count_row
        for j in range(8):
            for dx in range(4):
                if dy == 0 and dx == 0 and j == 0:
                    continue
                to = peer(dy, j, dx)
                send(
                    main_send.at[dy, dx, in_y[j]],
                    main_recv.at[dy, dx * 8 + j],
                    send_sem.at[5],
                    recv_main.at[dy],
                    to,
                )
                send(
                    ext_send.at[dy, dx, in_y[j]],
                    ext_recv.at[dy, dx * 8 + j],
                    send_sem.at[6],
                    recv_ext.at[dy],
                    to,
                )
    main_recv[0, 0] = main_send[0, 0, in_y[0]]
    ext_recv[0, 0] = ext_send[0, 0, in_y[0]]

    still = jnp.broadcast_to(cosine(phase), (EV, 128)).astype(BF16)
    query[...] = (
        mm(src[0].astype(BF16), wq[0:256, :]) + mm(still, wq[256:384, :])
    ) * (1.0 / math.sqrt(HEAD))
    lane_q = iota((16, 384), 1)
    first_head = lane_q < HEAD

    def attend(b, carry):
        at = pl.multiple_of(b * 128, 128)
        near[...] = mm(hot[b], table[...]).astype(BF16)
        code = times[:, pl.ds(at, 128), :].reshape(K * 128, 128)
        kv[...] = (mm(near[...], wkv[0:256, :]) + mm(code, wkv[256:384, :])).reshape(K, 128, 768)

        def group(g, inner):
            r = pl.multiple_of(g * 16, 16)
            q = query[pl.ds(at + r, 16), :]
            s0, s1 = [], []
            for k in range(K):
                t = q * kv[k, pl.ds(r, 16), 0:384]
                s0.append(jnp.sum(jnp.where(first_head, t, 0.0), axis=1, keepdims=True))
                s1.append(jnp.sum(jnp.where(first_head, 0.0, t), axis=1, keepdims=True))
            m0 = functools.reduce(jnp.maximum, s0)
            m1 = functools.reduce(jnp.maximum, s1)
            p0 = [jnp.exp(s - m0) for s in s0]
            p1 = [jnp.exp(s - m1) for s in s1]
            total = jnp.zeros((16, 384), F32)
            for k in range(K):
                w = jnp.where(first_head, p0[k], p1[k])
                total += w * kv[k, pl.ds(r, 16), 384:768]
            norm = jnp.where(first_head, sum(p0), sum(p1))
            att[pl.ds(at + r, 16), :] = (total / norm).astype(BF16)
            return inner

        lax.fori_loop(0, 8, group, 0)
        return carry

    lax.fori_loop(0, 4, attend, 0)
    hidden = mm(att[...], wm[0:384, :]) + mm(src[0].astype(BF16), wm[384:640, :])
    hidden = jnp.maximum(hidden + vec[2:3, 0:EMB], 0.0).astype(BF16)
    embedding[...] = (mm(hidden, w_out[...]) + vec[3:4, 0:EMB]).T.astype(BF16)

    wait_bytes(req_recv.at[0:96], recv_req.at[1])
    asked = req_recv[...].reshape(128, 128).astype(F32).T.astype(I32)
    for dy in (2, 1, 3, 0):
        for i in range(32):
            at = dy * 32 + i
            claims[i * CAP : (i + 1) * CAP, :] = one_hot(asked[0:CAP, at : at + 1] == row_lane)
        first = 1 if dy == 0 else 0
        wait_bytes(main_recv.at[dy, first:32], recv_main.at[dy])
        wait_bytes(ext_recv.at[dy, first:32], recv_ext.at[dy])
        for i in range(32):
            side[0:1, i * CAP : (i + 1) * CAP] = ext_recv[dy, i, :, 0:CAP]
            side[1:2, i * CAP : (i + 1) * CAP] = ext_recv[dy, i, :, 64 : 64 + CAP]
        count = side[1:2, :]
        high = jnp.floor(count * (1.0 / 128.0))
        row = iota((16, SLOTS), 0)
        rest = jnp.where(
            row == 0,
            side[0:1, :],
            jnp.where(row == 1, count - high * 128.0, jnp.where(row == 2, high, 0.0)),
        )
        left = jnp.concatenate(
            [main_recv[dy].reshape(SLOTS, 128).T, rest.astype(BF16)], axis=0
        )
        total = mm(left, claims[...])
        if dy == 2:
            acc[...] = total
        else:
            acc[...] += total

    small[...] = jnp.zeros(small.shape, F32)
    small[0:4, :] = vec[4:8, 0:128]
    bias = small[...].T
    b0, b1, b2, b3 = (bias[0:UNITS, g : g + 1] for g in range(4))
    heard = acc[129:130, :] + acc[130:131, :] * 128.0
    share = 1.0 / jnp.maximum(heard, 1.0)
    reset = jax.nn.sigmoid(acc[0:UNITS, :] * share + zed[0, 0:UNITS, :] + b0)
    update = jax.nn.sigmoid(acc[UNITS : 2 * UNITS, :] * share + zed[1, 0:UNITS, :] + b1)
    cand = jnp.tanh(
        acc[2 * UNITS : 3 * UNITS, :] * share
        + zed[2, 0:UNITS, :]
        + b2
        + reset * (zed[3, 0:UNITS, :] + b3)
    )
    mine = own[0:UNITS, :]
    fresh = (1.0 - update) * cand + update * mine
    new_memory[...] = jnp.where(heard > 0.0, fresh, mine)

    wait_bytes(req_recv.at[0:127], send_sem.at[0])
    wait_bytes(edge_recv.at[0:3], send_sem.at[1])
    wait_bytes(w_all.at[0:3, 0:544], send_sem.at[2])
    wait_bytes(wx_all.at[0:3], send_sem.at[3])
    wait_bytes(row_send.at[0:31], send_sem.at[4])
    wait_bytes(main_recv.at[0:3], send_sem.at[5])
    wait_bytes(main_recv.at[3, 0:31], send_sem.at[5])
    wait_bytes(ext_recv.at[0:3], send_sem.at[6])
    wait_bytes(ext_recv.at[3, 0:31], send_sem.at[6])


def step(
    memory,
    last_update,
    ev_time,
    nbr_gap,
    slot_rows,
    slot_ref,
    edge_feat,
    frequency,
    phase_shift,
    w_query,
    w_key,
    w_value,
    w_merge,
    b_merge,
    w_out,
    b_out,
    w_input,
    w_hidden,
    gru_bias,
):
    args = (
        memory.T,
        last_update.reshape(1, ROWS),
        ev_time.reshape(1, EV),
        nbr_gap.T,
        slot_rows,
        slot_ref.T,
        edge_feat.T,
        frequency.reshape(1, TIME),
        phase_shift.reshape(1, TIME),
        w_query,
        w_key,
        w_value,
        w_merge.T,
        b_merge.reshape(1, EMB),
        w_out,
        b_out.reshape(1, EMB),
        jnp.swapaxes(w_input, 1, 2),
        jnp.swapaxes(w_hidden, 1, 2),
        gru_bias,
    )
    vmem = pl.BlockSpec(memory_space=pltpu.VMEM)
    V, D = pltpu.VMEM, pltpu.SemaphoreType.DMA
    embedding, new_memory = pl.pallas_call(
        kernel,
        out_shape=(
            jax.ShapeDtypeStruct((EMB, EV), BF16),
            jax.ShapeDtypeStruct((UNITS, ROWS), F32),
        ),
        in_specs=[vmem] * len(args),
        out_specs=(vmem, vmem),
        scratch_shapes=[
            V((32, 1, 128), I32),
            V((128, 1, 128), I32),
            V((32, CAP, 256), BF16),
            V((32, CAP, 256), BF16),
            V((4, 64, EV), BF16),
            V((640, 128), BF16),
            V((1, 640), F32),
            V((4, 640, 128), BF16),
            V((4, 1, 640), F32),
            V((4, 4, 8, CAP, 128), BF16),
            V((4, 32, CAP, 128), BF16),
            V((4, 4, 8, 1, 128), F32),
            V((4, 32, 1, 128), F32),
            V((8, 256), F32),
            V((256, ROWS), F32),
            V((ROWS, 256), BF16),
            V((128, EV), F32),
            V((EV, 128), F32),
            V((128, 128), F32),
            V((K, EV, 128), BF16),
            V((384, 768), BF16),
            V((384, 384), BF16),
            V((640, EMB), BF16),
            V((8, 640), BF16),
            V((4, CAP, ROWS), F32),
            V((CAP, ROWS), F32),
            V((1, 2 * EV), I32),
            V((1, SLOTS), F32),
            V((2, EV, SLOTS), BF16),
            V((2, EV, 256), F32),
            V((2 * EV, 640), BF16),
            V((16, 384), F32),
            V((EV, 384), F32),
            V((4, K * 128, SLOTS), BF16),
            V((K * 128, 256), BF16),
            V((K, 128, 768), F32),
            V((EV, 384), BF16),
            V((SLOTS, ROWS), BF16),
            V((8, SLOTS), F32),
            V((144, ROWS), F32),
            D((7,)),
            D((6,)),
            D,
            D((3,)),
            D((4,)),
            D((4,)),
        ],
        compiler_params=pltpu.CompilerParams(
            collective_id=0, has_side_effects=True, vmem_limit_bytes=60 * 1024 * 1024
        ),
    )(*args)
    return embedding.T, new_memory.T


def solution(mesh):
    return jax.shard_map(
        step,
        mesh=mesh,
        in_specs=(
            P("node", None),
            P("node"),
            P(("node", "feat")),
            P(("node", "feat"), None),
            P(("node", "feat"), None),
            P(("node", "feat"), None),
            P("node", "feat"),
            P(),
            P(),
            P(),
            P(),
            P(),
            P(),
            P(),
            P(),
            P(),
            P(None, None, "feat"),
            P(None, None, "feat"),
            P(None, "feat"),
        ),
        out_specs=(P(("node", "feat"), None), P("node", "feat")),
        check_vma=False,
    )
```

```python
import functools
import math

import jax
import jax.numpy as jnp
from jax import lax
from jax.experimental import pallas as pl
from jax.experimental.pallas import tpu as pltpu
from jax.sharding import PartitionSpec as P

F32, BF16, I32 = jnp.float32, jnp.bfloat16, jnp.int32
MESH = pl.DeviceIdType.MESH
COS = (
    0.9999999998851011,
    -0.49999999850736465,
    0.041666663483369594,
    -0.0013888863001969808,
    2.4800551963260593e-05,
    -2.7534774132807624e-07,
    2.060335926598073e-09,
    -9.721760760713551e-12,
)
TURN_HI = 6.28125
TURN_LO = 2.0 * math.pi - TURN_HI

MEM, TIME, ATT, EMB, UNITS = 172, 100, 272, 172, 43
CAP, K, EV, ROWS, SLOTS = 48, 10, 512, 1024, 1536
HEAD = ATT // 2

HOME = (0, 0, 0, 0)


def backward(way):
    return tuple(3 if d == 2 else 0 for d in way[:3]) + (0,)


RELAYED = {
    way: backward(way)
    for way in [
        (dy, dz, dx, dc) for dy in range(4) for dz in range(4) for dx in range(4) for dc in range(2)
    ]
    if way[:3].count(2) >= 2 or way[:3] in ((2, 0, 0), (0, 2, 0), (0, 0, 2))
}


def cosine(x):
    turns = jnp.floor(x * (0.5 / math.pi) + 0.5)
    r = (x - turns * TURN_HI) - turns * TURN_LO
    u = r * r
    total = jnp.full_like(u, COS[-1])
    for c in COS[-2::-1]:
        total = total * u + c
    return total


def mm(a, b):
    return jnp.dot(a, b, preferred_element_type=F32)


def mm_nt(a, b):
    return lax.dot_general(a, b, (((1,), (1,)), ((), ())), preferred_element_type=F32)


def iota(shape, dim):
    return lax.broadcasted_iota(I32, shape, dim)


def one_hot(mask):
    return jnp.where(mask, 1.0, 0.0).astype(BF16)


def kernel(*refs):
    given, refs = refs[:19], refs[19:]
    loaded, refs = refs[-19:], refs[:-19]
    (
        embedding,
        new_memory,
        req_send,
        req_recv,
        row_send,
        fetched,
        edge_recv,
        w_mine,
        wx_mine,
        w_all,
        wx_all,
        main_send,
        main_recv,
        ext_send,
        ext_recv,
        relay_rows,
        relay_main,
        relay_ext,
        vec,
        mem_t,
        memb,
        wide_t,
        cols,
        small,
        times,
        wkv,
        wq,
        wm,
        w_ext,
        zed,
        own,
        end_cols,
        hits,
        ends,
        src,
        msg,
        ext_tmp,
        query,
        hot,
        near,
        qk,
        claims,
        asked_by,
        mix,
        side,
        acc,
        send_sem,
        recv_req,
        recv_rows,
        recv_x,
        recv_main,
        recv_ext,
        recv_relay,
        in_sem,
    ) = refs
    (
        memory,
        last_update,
        ev_time,
        nbr_gap,
        slot_rows,
        slot_ref,
        edge_feat,
        frequency,
        phase_shift,
        w_query,
        w_key,
        w_value,
        w_merge,
        b_merge,
        w_out,
        b_out,
        w_input,
        w_hidden,
        gru_bias,
    ) = loaded
    loads = [
        pltpu.make_async_copy(a, b, in_sem.at[i]) for i, (a, b) in enumerate(zip(given, loaded))
    ]
    n = lax.axis_index("node")
    f = lax.axis_index("feat")
    y, z, c = n // 8, (n // 2) % 4, n % 2
    at_y = [((y + d) % 4) * 8 for d in range(4)]
    at_z = [((z + d) % 4) * 2 for d in range(4)]
    at_c = [(c + d) % 2 for d in range(2)]
    at_f = [(f + d) % 4 for d in range(4)]
    in_y = [at_z[j // 2] + at_c[j % 2] for j in range(8)]

    def peer(dy, j, dx):
        return at_y[dy] + in_y[j], at_f[dx]

    def send(src_ref, dst_ref, s_sem, r_sem, to):
        pltpu.make_async_remote_copy(
            src_ref=src_ref,
            dst_ref=dst_ref,
            send_sem=s_sem,
            recv_sem=r_sem,
            device_id=to,
            device_id_type=MESH,
        ).start()

    def wait_bytes(ref, sem):
        pltpu.make_async_copy(ref, ref, sem).wait()

    def less(a, b):
        return (a[0] - b[0]) % 4, (a[1] - b[1]) % 4, (a[2] - b[2]) % 4, (a[3] - b[3]) % 2

    def there(d):
        return peer(d[0], d[1] * 2 + d[3], d[2])

    everyone = [(dy, dx, j) for dy in range(4) for dx in range(4) for j in range(8)][1:]

    for dx in range(4):
        w_all[dx, 176:256, :] = jnp.zeros((80, 128), BF16)
        w_all[dx, 368:384, :] = jnp.zeros((16, 128), BF16)

    barrier = pltpu.get_barrier_semaphore()
    near_by = [(dy, dx, j) for dy, dx, j in everyone if dx == 0 or (dy == 0 and j == 0)]
    for dy, dx, j in near_by:
        pl.semaphore_signal(
            barrier, inc=1, device_id=peer(dy, j, dx), device_id_type=MESH
        )
    for first in (4, 0, 1, 6):
        loads[first].start()
    for i in range(19):
        if i not in (4, 0, 1, 6):
            loads[i].start()

    req_send[...] = jnp.full(req_send.shape, -1, I32)
    loads[4].wait()
    for o in range(32):
        req_send[o, :, 0:CAP] = slot_rows[:, o * CAP : (o + 1) * CAP]
    req_recv[0] = req_send[n]
    loads[6].wait()
    edge_recv[f] = edge_feat[:, pl.ds(pl.multiple_of(f * EV, EV), EV)]

    loads[0].wait()
    loads[1].wait()
    mem_t[0:MEM, :] = memory[...]
    stamp = last_update[...].astype(F32)
    high = jnp.floor(stamp * (1.0 / 128.0))
    mem_t[MEM : MEM + 1, :] = high
    mem_t[MEM + 1 : MEM + 2, :] = stamp - high * 128.0
    mem_t[MEM + 2 : 256, :] = jnp.zeros((256 - MEM - 2, ROWS), F32)
    for b in range(4):
        memb[b * 256 : (b + 1) * 256, :] = mem_t[:, b * 256 : (b + 1) * 256].T.astype(BF16)

    pl.semaphore_wait(barrier, len(near_by))

    for dy, dx, j in everyone:
        if dx == 0:
            to = peer(dy, j, 0)
            send(
                req_send.at[to[0]],
                req_recv.at[dy * 32 + j],
                send_sem.at[0],
                recv_req.at[2 + dy],
                to,
            )
    for dx in range(1, 4):
        to = peer(0, 0, dx)
        send(
            edge_feat.at[:, pl.ds(pl.multiple_of(to[1] * EV, EV), EV)],
            edge_recv.at[f],
            send_sem.at[1],
            recv_x.at[0],
            to,
        )

    loads[16].wait()
    r640 = iota((640, 700), 0)
    c640 = iota((640, 700), 1)
    place = one_hot(
        ((r640 < MEM) & (c640 == r640 + MEM))
        | ((r640 >= 256) & (r640 < 256 + TIME) & (c640 == r640 - 256 + 2 * MEM))
        | ((r640 >= 384) & (c640 == r640 - 384 + 2 * MEM + TIME))
    )
    rows43 = iota((128, UNITS), 0)
    cols43 = iota((128, UNITS), 1)
    wide = mm(one_hot(rows43 == cols43), w_input[0].astype(BF16))
    wide += mm(one_hot(rows43 == cols43 + UNITS), w_input[1].astype(BF16))
    wide += mm(one_hot(rows43 == cols43 + 2 * UNITS), w_input[2].astype(BF16))
    w_mine[...] = mm_nt(place, wide.astype(BF16)).astype(BF16)
    last = mm(one_hot(iota((8, UNITS), 1) == UNITS - 1), w_input[2].astype(BF16))
    wx_mine[...] = mm_nt(last.astype(BF16), place)[0:1, :]
    for dx in range(1, 4):
        to = peer(0, 0, 4 - dx)
        for rows in (slice(0, 176), slice(256, 368), slice(384, 640)):
            send(w_mine.at[rows], w_all.at[dx, rows], send_sem.at[2], recv_x.at[1], to)
        send(wx_mine, wx_all.at[dx], send_sem.at[3], recv_x.at[2], to)
    w_all[0] = w_mine[...]
    wx_all[0] = wx_mine[...]

    for dy in range(4):
        first = 1 if dy == 0 else 0
        wait_bytes(req_recv.at[dy * 32 + first : dy * 32 + 8], recv_req.at[2 + dy])
    small[...] = jnp.zeros(small.shape, F32)
    for dy in range(4):
        small[8 * dy : 8 * dy + 8, :] = req_recv[dy * 32 : dy * 32 + 8].reshape(8, 128).astype(F32)
    asked = small[...].T.astype(I32)
    row_lane = iota((CAP, ROWS), 1)
    row_relays = []
    for dy in (2, 0, 1, 3):
        mask = jnp.concatenate(
            [
                one_hot(asked[0:CAP, 8 * dy + j : 8 * dy + j + 1] == row_lane)
                for j in range(8)
            ],
            axis=0,
        )
        rows = mm(mask, memb[...]).astype(BF16)
        for j in range(8):
            if dy == 0 and j == 0:
                fetched[n] = rows[0:CAP, :]
            else:
                row_send[dy * 8 + j] = rows[j * CAP : (j + 1) * CAP, :]
        for j in (4, 5, 2, 3, 6, 7, 1, 0):
            if dy == 0 and j == 0:
                continue
            way = less(HOME, (dy, j // 2, 0, j % 2))
            step = RELAYED.get(way)
            if step is None:
                dst, sem, to = fetched.at[n], recv_rows, there(way)
            else:
                dst, sem, to = relay_rows.at[len(row_relays)], recv_relay.at[0], there(step)
                row_relays.append((way, step))
            send(row_send.at[dy * 8 + j], dst, send_sem.at[4], sem, to)

    def pass_rows():
        wait_bytes(relay_rows, recv_relay.at[0])
        for at, (way, step) in enumerate(row_relays):
            origin = there(less(HOME, step))[0]
            send(
                relay_rows.at[at],
                fetched.at[origin],
                send_sem.at[4],
                recv_rows,
                there(less(way, step)),
            )

    wait_bytes(edge_recv.at[0:3], recv_x.at[0])
    for dy, dx, j in everyone:
        if dx != 0:
            to = peer(dy, j, dx)
            send(
                req_send.at[to[0]],
                req_recv.at[dy * 32 + dx * 8 + j],
                send_sem.at[0],
                recv_req.at[1],
                to,
            )

    for i in (2, 3, 5, 7, 8, 9, 10, 11, 12, 13, 14, 15, 17, 18):
        loads[i].wait()
    vec[...] = jnp.zeros(vec.shape, F32)
    vec[0:1, 0:TIME] = frequency[...]
    vec[1:2, 0:TIME] = phase_shift[...]
    vec[2:3, 0:EMB] = b_merge[...]
    vec[3:4, 0:EMB] = b_out[...]
    vec[4:8, 0:UNITS] = gru_bias[...]
    freq = vec[0:1, 0:128]
    phase = vec[1:2, 0:128]

    pass_rows()

    wide_t[...] = jnp.zeros(wide_t.shape, F32)
    wide_t[0 : K + 2, :] = slot_ref[...].astype(F32)
    wide_t[16 : 16 + K, :] = nbr_gap[...].astype(F32)
    wide_t[32:33, :] = ev_time[...].astype(F32)
    cols[...] = wide_t[...].T
    end_cols[:, 0:EV] = slot_ref[0:1, :]
    end_cols[:, EV : 2 * EV] = slot_ref[1:2, :]

    for k in range(K):
        times[k] = cosine(cols[:, 16 + k : 17 + k] * freq + phase).astype(BF16).astype(F32)

    slot_lane = iota((128, SLOTS), 1)

    def mark(b, count):
        picks = cols[pl.ds(pl.multiple_of(b * 128, 128), 128), :].astype(I32)
        for k in range(K):
            hot[b, k * 128 : (k + 1) * 128, :] = one_hot(picks[:, 2 + k : 3 + k] == slot_lane)
        for e in range(2):
            mask = jnp.where(picks[:, e : e + 1] == slot_lane, 1.0, 0.0)
            count += jnp.sum(mask, axis=0, keepdims=True)
            ends[e, pl.ds(pl.multiple_of(b * 128, 128), 128), :] = mask.astype(BF16)
        return count

    hits[...] = lax.fori_loop(0, 4, mark, jnp.zeros((1, SLOTS), F32))

    r272 = iota((384, ATT), 0)
    c272 = iota((384, ATT), 1)
    place = one_hot(
        ((c272 < MEM) & (r272 == c272)) | ((c272 >= MEM) & (r272 == c272 + (256 - MEM)))
    )
    wkv[...] = jnp.zeros(wkv.shape, BF16)
    wkv[:, 0:ATT] = mm(place, w_key[...]).astype(BF16)
    wkv[:, 384 : 384 + ATT] = mm(place, w_value[...]).astype(BF16)
    wq[...] = jnp.zeros(wq.shape, BF16)
    wq[:, 0:ATT] = mm(place, w_query[...]).astype(BF16)
    r444 = iota((640, ATT + MEM), 0)
    c444 = iota((640, ATT + MEM), 1)
    place = one_hot(
        ((c444 < ATT) & (r444 == c444)) | ((c444 >= ATT) & (r444 == c444 + (384 - ATT)))
    )
    wm[...] = mm_nt(place, w_merge[...]).astype(BF16)

    widen = one_hot(iota((CAP, UNITS), 0) == iota((CAP, UNITS), 1))
    mem_b = memory[...].astype(BF16)
    gates = (
        w_input[0, :, 0:MEM] + w_hidden[0],
        w_input[1, :, 0:MEM] + w_hidden[1],
        w_input[2, :, 0:MEM],
        w_hidden[2],
    )
    for g, w in enumerate(gates):
        zed[g] = mm(mm(widen, w.astype(BF16)).astype(BF16), mem_b)
    own[...] = jnp.dot(
        jnp.where(
            (iota((CAP, MEM), 1) == iota((CAP, MEM), 0) + f * UNITS)
            & (iota((CAP, MEM), 0) < UNITS),
            1.0,
            0.0,
        ),
        memory[...],
        preferred_element_type=F32,
        precision=lax.Precision.HIGHEST,
    )

    edges = edge_recv[...].reshape(256, EV).astype(F32).T.astype(BF16)
    for e in range(2):
        msg[e * EV : (e + 1) * EV, 384:640] = edges
    ext_send[...] = jnp.zeros(ext_send.shape, F32)

    wait_bytes(fetched.at[0:31], recv_rows)
    table = fetched.reshape(SLOTS, 256)

    for e in range(2):
        src[e] = mm(ends[e], table[...])
    for e in range(2):
        msg[e * EV : (e + 1) * EV, 0:256] = src[1 - e].astype(BF16)
        stamp = src[e, :, MEM : MEM + 1] * 128.0 + src[e, :, MEM + 1 : MEM + 2]
        gap = cols[:, 32:33] - stamp
        msg[e * EV : (e + 1) * EV, 256:384] = cosine(gap * freq + phase).astype(BF16)

    wait_bytes(w_all.at[0:3, 0:544], recv_x.at[1])
    wait_bytes(wx_all.at[0:3], recv_x.at[2])
    rows4 = jnp.concatenate([wx_all[dx] for dx in range(4)] + [jnp.zeros((4, 640), F32)], axis=0)
    w_ext[...] = rows4.astype(BF16)

    relays = [[], []]
    for dy in (2, 0, 1, 3):
        base = at_y[dy] * CAP
        mask = one_hot(iota((384, 2 * EV), 0) + base == end_cols[...])
        sums = mm(mask, msg[...]).astype(BF16)
        for pair in range(2):
            w_pair = jnp.concatenate([w_all[2 * pair], w_all[2 * pair + 1]], axis=1)
            out = mm(sums, w_pair).astype(BF16)
            for i in range(2):
                main_send[dy, 2 * pair + i] = out[:, i * 128 : (i + 1) * 128].reshape(8, CAP, 128)
        ext_tmp[0:8, :] = mm_nt(w_ext[...], sums)
        ext_tmp[8:9, :] = hits[:, pl.ds(pl.multiple_of(base, 128), 384)]
        for j in range(8):
            count_row = ext_tmp[8:9, j * CAP : (j + 1) * CAP]
            for dx in range(4):
                ext_send[dy, dx, j, :, 0:CAP] = ext_tmp[dx : dx + 1, j * CAP : (j + 1) * CAP]
                ext_send[dy, dx, j, :, 64 : 64 + CAP] = count_row
        batch = 0 if dy == 2 else 1
        ways = [(dy, j // 2, dx, j % 2) for j in range(8) for dx in range(4)]
        ways = sorted(ways, key=lambda way: way not in RELAYED)
        for way in ways:
            if way == HOME:
                continue
            dx, j = way[2], way[1] * 2 + way[3]
            step = RELAYED.get(way)
            if step is None:
                to = there(way)
                to_main, to_ext = main_recv.at[dy, dx * 8 + j], ext_recv.at[dy, dx * 8 + j]
                main_sem, ext_sem = recv_main.at[dy], recv_ext.at[dy]
            else:
                to = there(step)
                at = 16 * batch + len(relays[batch])
                to_main, to_ext = relay_main.at[at], relay_ext.at[at]
                main_sem, ext_sem = recv_relay.at[1 + 2 * batch], recv_relay.at[2 + 2 * batch]
                relays[batch].append((at, way, step))
            send(main_send.at[dy, dx, in_y[j]], to_main, send_sem.at[5], main_sem, to)
            send(ext_send.at[dy, dx, in_y[j]], to_ext, send_sem.at[6], ext_sem, to)

    def pass_sums(batch):
        first, end = (0, 16) if batch == 0 else (16, 26)
        wait_bytes(relay_main.at[first:end], recv_relay.at[1 + 2 * batch])
        wait_bytes(relay_ext.at[first:end], recv_relay.at[2 + 2 * batch])
        for at, way, step in relays[batch]:
            to = there(less(way, step))
            dy, dx, j = way[0], way[2], way[1] * 2 + way[3]
            send(
                relay_main.at[at],
                main_recv.at[dy, dx * 8 + j],
                send_sem.at[5],
                recv_main.at[dy],
                to,
            )
            send(
                relay_ext.at[at],
                ext_recv.at[dy, dx * 8 + j],
                send_sem.at[6],
                recv_ext.at[dy],
                to,
            )

    main_recv[0, 0] = main_send[0, 0, in_y[0]]
    ext_recv[0, 0] = ext_send[0, 0, in_y[0]]

    still = jnp.broadcast_to(cosine(phase), (EV, 128)).astype(BF16)
    query[...] = (
        mm(src[0].astype(BF16), wq[0:256, :]) + mm(still, wq[256:384, :])
    ) * (1.0 / math.sqrt(HEAD))
    head_of = iota((EV, 384), 1) < HEAD
    for h in range(2):
        part = query[...]
        part = jnp.where(head_of, part, 0.0) if h == 0 else jnp.where(head_of, 0.0, part)
        coarse = part.astype(BF16)
        fine = (part - coarse.astype(F32)).astype(BF16)
        qk[h] = mm_nt(coarse, wkv[:, 0:384]) + mm_nt(fine, wkv[:, 0:384])
    pass_sums(0)

    wait_bytes(req_recv.at[0:96], recv_req.at[1])
    for dy in range(4):
        small[...] = jnp.zeros(small.shape, F32)
        small[0:32, :] = req_recv[dy * 32 : dy * 32 + 32].reshape(32, 128).astype(F32)
        asked_by[dy] = small[...].T

    def attend(b, carry):
        at = pl.multiple_of(b * 128, 128)
        near[...] = mm(hot[b], table[...]).reshape(K, 128, 256)

        def group(g, inner):
            r = pl.multiple_of(g * 16, 16)
            rows = pl.ds(at + r, 16)
            q0, q1 = qk[0, rows, :], qk[1, rows, :]
            s0, s1 = [], []
            for k in range(K):
                x, t = near[k, pl.ds(r, 16), :], times[k, rows, :]
                u0 = x * q0[:, 0:256]
                u1 = x * q1[:, 0:256]
                u0 = u0[:, 0:128] + u0[:, 128:256] + t * q0[:, 256:384]
                u1 = u1[:, 0:128] + u1[:, 128:256] + t * q1[:, 256:384]
                s0.append(jnp.sum(u0, axis=1, keepdims=True))
                s1.append(jnp.sum(u1, axis=1, keepdims=True))
            m0 = functools.reduce(jnp.maximum, s0)
            m1 = functools.reduce(jnp.maximum, s1)
            p0 = [jnp.exp(s - m0) for s in s0]
            p1 = [jnp.exp(s - m1) for s in s1]
            n0 = 1.0 / sum(p0)
            n1 = 1.0 / sum(p1)
            a0 = a1 = jnp.zeros((16, 256), F32)
            c0 = c1 = jnp.zeros((16, 128), F32)
            for k in range(K):
                x, t = near[k, pl.ds(r, 16), :], times[k, rows, :]
                a0 += p0[k] * x
                a1 += p1[k] * x
                c0 += p0[k] * t
                c1 += p1[k] * t
            mix[0, rows, 0:256] = a0 * n0
            mix[1, rows, 0:256] = a1 * n1
            mix[0, rows, 256:384] = c0 * n0
            mix[1, rows, 256:384] = c1 * n1
            return inner

        lax.fori_loop(0, 8, group, 0)
        for i in range(32):
            claims[b, i * CAP : (i + 1) * CAP, :] = one_hot(
                asked_by[b, 0:CAP, i : i + 1].astype(I32) == row_lane
            )

        @pl.when(b == 1)
        def _():
            pass_sums(1)

        return carry

    lax.fori_loop(0, 4, attend, 0)
    halves = []
    for h in range(2):
        part = mix[h]
        coarse = part.astype(BF16)
        fine = (part - coarse.astype(F32)).astype(BF16)
        halves.append(mm(coarse, wkv[:, 384:768]) + mm(fine, wkv[:, 384:768]))
    attended = jnp.where(head_of, halves[0], halves[1]).astype(BF16)
    hidden = mm(attended, wm[0:384, :]) + mm(src[0].astype(BF16), wm[384:640, :])
    hidden = jnp.maximum(hidden + vec[2:3, 0:EMB], 0.0).astype(BF16)
    embedding[...] = (mm(hidden, w_out[...]) + vec[3:4, 0:EMB]).T.astype(BF16)

    for dy in (2, 0, 1, 3):
        first = 1 if dy == 0 else 0
        wait_bytes(main_recv.at[dy, first:32], recv_main.at[dy])
        wait_bytes(ext_recv.at[dy, first:32], recv_ext.at[dy])
        for i in range(32):
            side[0:1, i * CAP : (i + 1) * CAP] = ext_recv[dy, i, :, 0:CAP]
            side[1:2, i * CAP : (i + 1) * CAP] = ext_recv[dy, i, :, 64 : 64 + CAP]
        count = side[1:2, :]
        high = jnp.floor(count * (1.0 / 128.0))
        row = iota((16, SLOTS), 0)
        rest = jnp.where(
            row == 0,
            side[0:1, :],
            jnp.where(row == 1, count - high * 128.0, jnp.where(row == 2, high, 0.0)),
        )
        left = jnp.concatenate(
            [main_recv[dy].reshape(SLOTS, 128).T, rest.astype(BF16)], axis=0
        )
        total = mm(left, claims[dy])
        if dy == 2:
            acc[...] = total
        else:
            acc[...] += total

    small[...] = jnp.zeros(small.shape, F32)
    small[0:4, :] = vec[4:8, 0:128]
    bias = small[...].T
    b0, b1, b2, b3 = (bias[0:UNITS, g : g + 1] for g in range(4))
    heard = acc[129:130, :] + acc[130:131, :] * 128.0
    share = 1.0 / jnp.maximum(heard, 1.0)
    reset = jax.nn.sigmoid(acc[0:UNITS, :] * share + zed[0, 0:UNITS, :] + b0)
    update = jax.nn.sigmoid(acc[UNITS : 2 * UNITS, :] * share + zed[1, 0:UNITS, :] + b1)
    cand = jnp.tanh(
        acc[2 * UNITS : 3 * UNITS, :] * share
        + zed[2, 0:UNITS, :]
        + b2
        + reset * (zed[3, 0:UNITS, :] + b3)
    )
    mine = own[0:UNITS, :]
    fresh = (1.0 - update) * cand + update * mine
    new_memory[...] = jnp.where(heard > 0.0, fresh, mine)

    wait_bytes(req_recv.at[0:127], send_sem.at[0])
    wait_bytes(edge_recv.at[0:3], send_sem.at[1])
    wait_bytes(w_all.at[0:3, 0:544], send_sem.at[2])
    wait_bytes(wx_all.at[0:3], send_sem.at[3])
    wait_bytes(row_send.at[0:31], send_sem.at[4])
    wait_bytes(relay_rows, send_sem.at[4])
    wait_bytes(main_recv.at[0:3], send_sem.at[5])
    wait_bytes(main_recv.at[3, 0:31], send_sem.at[5])
    wait_bytes(relay_main, send_sem.at[5])
    wait_bytes(ext_recv.at[0:3], send_sem.at[6])
    wait_bytes(ext_recv.at[3, 0:31], send_sem.at[6])
    wait_bytes(relay_ext, send_sem.at[6])


def step(
    memory,
    last_update,
    ev_time,
    nbr_gap,
    slot_rows,
    slot_ref,
    edge_feat,
    frequency,
    phase_shift,
    w_query,
    w_key,
    w_value,
    w_merge,
    b_merge,
    w_out,
    b_out,
    w_input,
    w_hidden,
    gru_bias,
):
    args = (
        memory.T,
        last_update.reshape(1, ROWS),
        ev_time.reshape(1, EV),
        nbr_gap.T,
        slot_rows,
        slot_ref.T,
        edge_feat.T,
        frequency.reshape(1, TIME),
        phase_shift.reshape(1, TIME),
        w_query,
        w_key,
        w_value,
        w_merge.T,
        b_merge.reshape(1, EMB),
        w_out,
        b_out.reshape(1, EMB),
        jnp.swapaxes(w_input, 1, 2),
        jnp.swapaxes(w_hidden, 1, 2),
        gru_bias,
    )
    vmem = pl.BlockSpec(memory_space=pltpu.VMEM)
    V, D = pltpu.VMEM, pltpu.SemaphoreType.DMA
    embedding, new_memory = pl.pallas_call(
        kernel,
        out_shape=(
            jax.ShapeDtypeStruct((EMB, EV), BF16),
            jax.ShapeDtypeStruct((UNITS, ROWS), F32),
        ),
        in_specs=[pl.BlockSpec(memory_space=pl.ANY)] * len(args),
        out_specs=(vmem, vmem),
        scratch_shapes=[
            V((32, 1, 128), I32),
            V((128, 1, 128), I32),
            V((32, CAP, 256), BF16),
            V((32, CAP, 256), BF16),
            V((4, 64, EV), BF16),
            V((640, 128), BF16),
            V((1, 640), F32),
            V((4, 640, 128), BF16),
            V((4, 1, 640), F32),
            V((4, 4, 8, CAP, 128), BF16),
            V((4, 32, CAP, 128), BF16),
            V((4, 4, 8, 1, 128), F32),
            V((4, 32, 1, 128), F32),
            V((6, CAP, 256), BF16),
            V((26, CAP, 128), BF16),
            V((26, 1, 128), F32),
            V((8, 256), F32),
            V((256, ROWS), F32),
            V((ROWS, 256), BF16),
            V((128, EV), F32),
            V((EV, 128), F32),
            V((128, 128), F32),
            V((K, EV, 128), F32),
            V((384, 768), BF16),
            V((384, 384), BF16),
            V((640, EMB), BF16),
            V((8, 640), BF16),
            V((4, CAP, ROWS), F32),
            V((CAP, ROWS), F32),
            V((1, 2 * EV), I32),
            V((1, SLOTS), F32),
            V((2, EV, SLOTS), BF16),
            V((2, EV, 256), F32),
            V((2 * EV, 640), BF16),
            V((16, 384), F32),
            V((EV, 384), F32),
            V((4, K * 128, SLOTS), BF16),
            V((K, 128, 256), F32),
            V((2, EV, 384), F32),
            V((4, SLOTS, ROWS), BF16),
            V((4, 128, 128), F32),
            V((2, EV, 384), F32),
            V((8, SLOTS), F32),
            V((144, ROWS), F32),
            D((7,)),
            D((6,)),
            D,
            D((3,)),
            D((4,)),
            D((4,)),
            D((5,)),
            D((19,)),
        ]
        + [V(a.shape, a.dtype) for a in args],
        compiler_params=pltpu.CompilerParams(
            collective_id=0, has_side_effects=True, vmem_limit_bytes=60 * 1024 * 1024
        ),
    )(*args)
    return embedding.T, new_memory.T


def solution(mesh):
    return jax.shard_map(
        step,
        mesh=mesh,
        in_specs=(
            P("node", None),
            P("node"),
            P(("node", "feat")),
            P(("node", "feat"), None),
            P(("node", "feat"), None),
            P(("node", "feat"), None),
            P("node", "feat"),
            P(),
            P(),
            P(),
            P(),
            P(),
            P(),
            P(),
            P(),
            P(),
            P(None, None, "feat"),
            P(None, None, "feat"),
            P(None, "feat"),
        ),
        out_specs=(P(("node", "feat"), None), P("node", "feat")),
        check_vma=False,
    )
```

```python
import functools
import math

import jax
import jax.numpy as jnp
from jax import lax
from jax.experimental import pallas as pl
from jax.experimental.pallas import tpu as pltpu
from jax.sharding import PartitionSpec as P

F32, BF16, I32 = jnp.float32, jnp.bfloat16, jnp.int32
MESH = pl.DeviceIdType.MESH
COS = (
    0.9999999998851011,
    -0.49999999850736465,
    0.041666663483369594,
    -0.0013888863001969808,
    2.4800551963260593e-05,
    -2.7534774132807624e-07,
    2.060335926598073e-09,
    -9.721760760713551e-12,
)
TURN_HI = 6.28125
TURN_LO = 2.0 * math.pi - TURN_HI

MEM, TIME, ATT, EMB, UNITS = 172, 100, 272, 172, 43
CAP, K, EV, ROWS, SLOTS = 48, 10, 512, 1024, 1536
HEAD = ATT // 2


def cosine(x):
    turns = jnp.floor(x * (0.5 / math.pi) + 0.5)
    r = (x - turns * TURN_HI) - turns * TURN_LO
    u = r * r
    total = jnp.full_like(u, COS[-1])
    for c in COS[-2::-1]:
        total = total * u + c
    return total


def mm(a, b):
    return jnp.dot(a, b, preferred_element_type=F32)


def mm_nt(a, b):
    return lax.dot_general(a, b, (((1,), (1,)), ((), ())), preferred_element_type=F32)


def iota(shape, dim):
    return lax.broadcasted_iota(I32, shape, dim)


def one_hot(mask):
    return jnp.where(mask, 1.0, 0.0).astype(BF16)


def kernel(*refs):
    given, refs = refs[:19], refs[19:]
    loaded, refs = refs[-19:], refs[:-19]
    (
        embedding,
        new_memory,
        req_send,
        req_recv,
        row_send,
        fetched,
        edge_recv,
        w_mine,
        wx_mine,
        w_all,
        wx_all,
        main_send,
        main_recv,
        ext_send,
        ext_recv,
        vec,
        mem_t,
        memb,
        wide_t,
        cols,
        small,
        times,
        wkv,
        wq,
        wm,
        w_ext,
        zed,
        own,
        end_cols,
        hits,
        ends,
        src,
        msg,
        ext_tmp,
        query,
        hot,
        near,
        qk,
        claims,
        asked_by,
        mix,
        side,
        acc,
        send_sem,
        recv_req,
        recv_rows,
        recv_x,
        recv_main,
        recv_ext,
        in_sem,
    ) = refs
    (
        memory,
        last_update,
        ev_time,
        nbr_gap,
        slot_rows,
        slot_ref,
        edge_feat,
        frequency,
        phase_shift,
        w_query,
        w_key,
        w_value,
        w_merge,
        b_merge,
        w_out,
        b_out,
        w_input,
        w_hidden,
        gru_bias,
    ) = loaded
    loads = [
        pltpu.make_async_copy(a, b, in_sem.at[i]) for i, (a, b) in enumerate(zip(given, loaded))
    ]
    n = lax.axis_index("node")
    f = lax.axis_index("feat")
    y, z, c = n // 8, (n // 2) % 4, n % 2
    at_y = [((y + d) % 4) * 8 for d in range(4)]
    at_z = [((z + d) % 4) * 2 for d in range(4)]
    at_c = [(c + d) % 2 for d in range(2)]
    at_f = [(f + d) % 4 for d in range(4)]
    in_y = [at_z[j // 2] + at_c[j % 2] for j in range(8)]

    def peer(dy, j, dx):
        return at_y[dy] + in_y[j], at_f[dx]

    def send(src_ref, dst_ref, s_sem, r_sem, to):
        pltpu.make_async_remote_copy(
            src_ref=src_ref,
            dst_ref=dst_ref,
            send_sem=s_sem,
            recv_sem=r_sem,
            device_id=to,
            device_id_type=MESH,
        ).start()

    def wait_bytes(ref, sem):
        pltpu.make_async_copy(ref, ref, sem).wait()

    everyone = [(dy, dx, j) for dy in range(4) for dx in range(4) for j in range(8)][1:]

    for dx in range(4):
        w_all[dx, 176:256, :] = jnp.zeros((80, 128), BF16)
        w_all[dx, 368:384, :] = jnp.zeros((16, 128), BF16)

    barrier = pltpu.get_barrier_semaphore()
    near_by = [(dy, dx, j) for dy, dx, j in everyone if dx == 0 or (dy == 0 and j == 0)]
    for dy, dx, j in near_by:
        pl.semaphore_signal(
            barrier, inc=1, device_id=peer(dy, j, dx), device_id_type=MESH
        )
    for first in (4, 0, 1, 6):
        loads[first].start()
    for i in range(19):
        if i not in (4, 0, 1, 6):
            loads[i].start()

    req_send[...] = jnp.full(req_send.shape, -1, I32)
    loads[4].wait()
    for o in range(32):
        req_send[o, :, 0:CAP] = slot_rows[:, o * CAP : (o + 1) * CAP]
    req_recv[0] = req_send[n]
    loads[6].wait()
    edge_recv[f] = edge_feat[:, pl.ds(pl.multiple_of(f * EV, EV), EV)]

    loads[0].wait()
    loads[1].wait()
    mem_t[0:MEM, :] = memory[...]
    stamp = last_update[...].astype(F32)
    high = jnp.floor(stamp * (1.0 / 128.0))
    mem_t[MEM : MEM + 1, :] = high
    mem_t[MEM + 1 : MEM + 2, :] = stamp - high * 128.0
    mem_t[MEM + 2 : 256, :] = jnp.zeros((256 - MEM - 2, ROWS), F32)
    for b in range(4):
        memb[b * 256 : (b + 1) * 256, :] = mem_t[:, b * 256 : (b + 1) * 256].T.astype(BF16)

    pl.semaphore_wait(barrier, len(near_by))

    for dy, dx, j in everyone:
        if dx == 0:
            to = peer(dy, j, 0)
            send(
                req_send.at[to[0]],
                req_recv.at[dy * 32 + j],
                send_sem.at[0],
                recv_req.at[2 + dy],
                to,
            )
    for dx in range(1, 4):
        to = peer(0, 0, dx)
        send(
            edge_feat.at[:, pl.ds(pl.multiple_of(to[1] * EV, EV), EV)],
            edge_recv.at[f],
            send_sem.at[1],
            recv_x.at[0],
            to,
        )

    loads[16].wait()
    r640 = iota((640, 700), 0)
    c640 = iota((640, 700), 1)
    place = one_hot(
        ((r640 < MEM) & (c640 == r640 + MEM))
        | ((r640 >= 256) & (r640 < 256 + TIME) & (c640 == r640 - 256 + 2 * MEM))
        | ((r640 >= 384) & (c640 == r640 - 384 + 2 * MEM + TIME))
    )
    rows43 = iota((128, UNITS), 0)
    cols43 = iota((128, UNITS), 1)
    wide = mm(one_hot(rows43 == cols43), w_input[0].astype(BF16))
    wide += mm(one_hot(rows43 == cols43 + UNITS), w_input[1].astype(BF16))
    wide += mm(one_hot(rows43 == cols43 + 2 * UNITS), w_input[2].astype(BF16))
    w_mine[...] = mm_nt(place, wide.astype(BF16)).astype(BF16)
    last = mm(one_hot(iota((8, UNITS), 1) == UNITS - 1), w_input[2].astype(BF16))
    wx_mine[...] = mm_nt(last.astype(BF16), place)[0:1, :]
    for dx in range(1, 4):
        to = peer(0, 0, 4 - dx)
        for rows in (slice(0, 176), slice(256, 368), slice(384, 640)):
            send(w_mine.at[rows], w_all.at[dx, rows], send_sem.at[2], recv_x.at[1], to)
        send(wx_mine, wx_all.at[dx], send_sem.at[3], recv_x.at[2], to)
    w_all[0] = w_mine[...]
    wx_all[0] = wx_mine[...]

    for i in (2, 3, 5, 7, 8, 9, 10, 11, 12, 13, 14, 15, 17, 18):
        loads[i].wait()
    vec[...] = jnp.zeros(vec.shape, F32)
    vec[0:1, 0:TIME] = frequency[...]
    vec[1:2, 0:TIME] = phase_shift[...]
    vec[2:3, 0:EMB] = b_merge[...]
    vec[3:4, 0:EMB] = b_out[...]
    vec[4:8, 0:UNITS] = gru_bias[...]
    freq = vec[0:1, 0:128]
    phase = vec[1:2, 0:128]

    wide_t[...] = jnp.zeros(wide_t.shape, F32)
    wide_t[0 : K + 2, :] = slot_ref[...].astype(F32)
    wide_t[16 : 16 + K, :] = nbr_gap[...].astype(F32)
    wide_t[32:33, :] = ev_time[...].astype(F32)
    cols[...] = wide_t[...].T
    end_cols[:, 0:EV] = slot_ref[0:1, :]
    end_cols[:, EV : 2 * EV] = slot_ref[1:2, :]

    for k in range(K):
        times[k] = cosine(cols[:, 16 + k : 17 + k] * freq + phase).astype(BF16).astype(F32)

    for dy in range(4):
        first = 1 if dy == 0 else 0
        wait_bytes(req_recv.at[dy * 32 + first : dy * 32 + 8], recv_req.at[2 + dy])
    small[...] = jnp.zeros(small.shape, F32)
    for dy in range(4):
        small[8 * dy : 8 * dy + 8, :] = req_recv[dy * 32 : dy * 32 + 8].reshape(8, 128).astype(F32)
    asked = small[...].T.astype(I32)
    row_lane = iota((CAP, ROWS), 1)
    for dy in (2, 1, 3, 0):
        mask = jnp.concatenate(
            [
                one_hot(asked[0:CAP, 8 * dy + j : 8 * dy + j + 1] == row_lane)
                for j in range(8)
            ],
            axis=0,
        )
        rows = mm(mask, memb[...]).astype(BF16)
        for j in range(8):
            if dy == 0 and j == 0:
                fetched[n] = rows[0:CAP, :]
            else:
                row_send[dy * 8 + j] = rows[j * CAP : (j + 1) * CAP, :]
        for j in (4, 5, 2, 3, 6, 7, 1, 0):
            if dy == 0 and j == 0:
                continue
            back = (4 - j // 2) % 4 * 2 + j % 2
            send(
                row_send.at[dy * 8 + j],
                fetched.at[n],
                send_sem.at[4],
                recv_rows.at[dy],
                peer((4 - dy) % 4, back, 0),
            )

    wait_bytes(edge_recv.at[0:3], recv_x.at[0])
    for dy, dx, j in everyone:
        if dx != 0:
            to = peer(dy, j, dx)
            send(
                req_send.at[to[0]],
                req_recv.at[dy * 32 + dx * 8 + j],
                send_sem.at[0],
                recv_req.at[1],
                to,
            )

    slot_lane = iota((128, SLOTS), 1)

    def mark(b, count):
        picks = cols[pl.ds(pl.multiple_of(b * 128, 128), 128), :].astype(I32)
        for k in range(K):
            hot[b, k * 128 : (k + 1) * 128, :] = one_hot(picks[:, 2 + k : 3 + k] == slot_lane)
        for e in range(2):
            mask = jnp.where(picks[:, e : e + 1] == slot_lane, 1.0, 0.0)
            count += jnp.sum(mask, axis=0, keepdims=True)
            ends[e, pl.ds(pl.multiple_of(b * 128, 128), 128), :] = mask.astype(BF16)
        return count

    hits[...] = lax.fori_loop(0, 4, mark, jnp.zeros((1, SLOTS), F32))

    r272 = iota((384, ATT), 0)
    c272 = iota((384, ATT), 1)
    place = one_hot(
        ((c272 < MEM) & (r272 == c272)) | ((c272 >= MEM) & (r272 == c272 + (256 - MEM)))
    )
    wkv[...] = jnp.zeros(wkv.shape, BF16)
    wkv[:, 0:ATT] = mm(place, w_key[...]).astype(BF16)
    wkv[:, 384 : 384 + ATT] = mm(place, w_value[...]).astype(BF16)
    wq[...] = jnp.zeros(wq.shape, BF16)
    wq[:, 0:ATT] = mm(place, w_query[...]).astype(BF16)
    r444 = iota((640, ATT + MEM), 0)
    c444 = iota((640, ATT + MEM), 1)
    place = one_hot(
        ((c444 < ATT) & (r444 == c444)) | ((c444 >= ATT) & (r444 == c444 + (384 - ATT)))
    )
    wm[...] = mm_nt(place, w_merge[...]).astype(BF16)

    widen = one_hot(iota((CAP, UNITS), 0) == iota((CAP, UNITS), 1))
    mem_b = memory[...].astype(BF16)
    gates = (
        w_input[0, :, 0:MEM] + w_hidden[0],
        w_input[1, :, 0:MEM] + w_hidden[1],
        w_input[2, :, 0:MEM],
        w_hidden[2],
    )
    for g, w in enumerate(gates):
        zed[g] = mm(mm(widen, w.astype(BF16)).astype(BF16), mem_b)
    own[...] = jnp.dot(
        jnp.where(
            (iota((CAP, MEM), 1) == iota((CAP, MEM), 0) + f * UNITS)
            & (iota((CAP, MEM), 0) < UNITS),
            1.0,
            0.0,
        ),
        memory[...],
        preferred_element_type=F32,
        precision=lax.Precision.HIGHEST,
    )

    edges = edge_recv[...].reshape(256, EV).astype(F32).T.astype(BF16)
    for e in range(2):
        msg[e * EV : (e + 1) * EV, 384:640] = edges
    ext_send[...] = jnp.zeros(ext_send.shape, F32)

    def half_of(table_of, lanes_of, half):
        return (
            jnp.concatenate([table_of(dy) for dy in half], axis=0),
            lambda ref: jnp.concatenate([lanes_of(ref, dy) for dy in half], axis=1),
        )

    def owners(dy):
        return fetched[pl.ds(at_y[dy], 8)].reshape(384, 256)

    def marks(view, dy):
        return view[:, pl.ds(pl.multiple_of(at_y[dy] * CAP, 128), 384)]

    for dy in (1, 2):
        wait_bytes(fetched.at[0:8], recv_rows.at[dy])
    table, lanes = half_of(owners, marks, (1, 2))
    for e in range(2):
        src[e] = mm(lanes(ends.at[e]), table)

    def first_half(b, carry):
        table, lanes = half_of(owners, marks, (1, 2))
        near[b] = mm(lanes(hot.at[b]), table).reshape(K, 128, 256)
        return carry

    lax.fori_loop(0, 4, first_half, 0)

    wait_bytes(fetched.at[0:8], recv_rows.at[3])
    wait_bytes(fetched.at[0:7], recv_rows.at[0])
    table, lanes = half_of(owners, marks, (3, 0))
    for e in range(2):
        src[e] += mm(lanes(ends.at[e]), table)
    for e in range(2):
        msg[e * EV : (e + 1) * EV, 0:256] = src[1 - e].astype(BF16)
        stamp = src[e, :, MEM : MEM + 1] * 128.0 + src[e, :, MEM + 1 : MEM + 2]
        gap = cols[:, 32:33] - stamp
        msg[e * EV : (e + 1) * EV, 256:384] = cosine(gap * freq + phase).astype(BF16)

    wait_bytes(w_all.at[0:3, 0:544], recv_x.at[1])
    wait_bytes(wx_all.at[0:3], recv_x.at[2])
    rows4 = jnp.concatenate([wx_all[dx] for dx in range(4)] + [jnp.zeros((4, 640), F32)], axis=0)
    w_ext[...] = rows4.astype(BF16)

    for dy in (2, 1, 3, 0):
        base = at_y[dy] * CAP
        mask = one_hot(iota((384, 2 * EV), 0) + base == end_cols[...])
        sums = mm(mask, msg[...]).astype(BF16)
        for pair in range(2):
            w_pair = jnp.concatenate([w_all[2 * pair], w_all[2 * pair + 1]], axis=1)
            out = mm(sums, w_pair).astype(BF16)
            for i in range(2):
                main_send[dy, 2 * pair + i] = out[:, i * 128 : (i + 1) * 128].reshape(8, CAP, 128)
        ext_tmp[0:8, :] = mm_nt(w_ext[...], sums)
        ext_tmp[8:9, :] = hits[:, pl.ds(pl.multiple_of(base, 128), 384)]
        for j in range(8):
            count_row = ext_tmp[8:9, j * CAP : (j + 1) * CAP]
            for dx in range(4):
                ext_send[dy, dx, j, :, 0:CAP] = ext_tmp[dx : dx + 1, j * CAP : (j + 1) * CAP]
                ext_send[dy, dx, j, :, 64 : 64 + CAP] = count_row
        for j in range(8):
            for dx in range(4):
                if dy == 0 and dx == 0 and j == 0:
                    continue
                to = peer(dy, j, dx)
                send(
                    main_send.at[dy, dx, in_y[j]],
                    main_recv.at[dy, dx * 8 + j],
                    send_sem.at[5],
                    recv_main.at[dy],
                    to,
                )
                send(
                    ext_send.at[dy, dx, in_y[j]],
                    ext_recv.at[dy, dx * 8 + j],
                    send_sem.at[6],
                    recv_ext.at[dy],
                    to,
                )
    main_recv[0, 0] = main_send[0, 0, in_y[0]]
    ext_recv[0, 0] = ext_send[0, 0, in_y[0]]

    still = jnp.broadcast_to(cosine(phase), (EV, 128)).astype(BF16)
    query[...] = (
        mm(src[0].astype(BF16), wq[0:256, :]) + mm(still, wq[256:384, :])
    ) * (1.0 / math.sqrt(HEAD))
    head_of = iota((EV, 384), 1) < HEAD
    for h in range(2):
        part = query[...]
        part = jnp.where(head_of, part, 0.0) if h == 0 else jnp.where(head_of, 0.0, part)
        coarse = part.astype(BF16)
        fine = (part - coarse.astype(F32)).astype(BF16)
        qk[h] = mm_nt(coarse, wkv[:, 0:384]) + mm_nt(fine, wkv[:, 0:384])

    wait_bytes(req_recv.at[0:96], recv_req.at[1])
    for dy in range(4):
        small[...] = jnp.zeros(small.shape, F32)
        small[0:32, :] = req_recv[dy * 32 : dy * 32 + 32].reshape(32, 128).astype(F32)
        asked_by[dy] = small[...].T

    def attend(b, carry):
        at = pl.multiple_of(b * 128, 128)
        table, lanes = half_of(owners, marks, (3, 0))
        near[b] += mm(lanes(hot.at[b]), table).reshape(K, 128, 256)

        def group(g, inner):
            r = pl.multiple_of(g * 16, 16)
            rows = pl.ds(at + r, 16)
            q0, q1 = qk[0, rows, :], qk[1, rows, :]
            s0, s1 = [], []
            for k in range(K):
                x, t = near[b, k, pl.ds(r, 16), :], times[k, rows, :]
                u0 = x * q0[:, 0:256]
                u1 = x * q1[:, 0:256]
                u0 = u0[:, 0:128] + u0[:, 128:256] + t * q0[:, 256:384]
                u1 = u1[:, 0:128] + u1[:, 128:256] + t * q1[:, 256:384]
                s0.append(jnp.sum(u0, axis=1, keepdims=True))
                s1.append(jnp.sum(u1, axis=1, keepdims=True))
            m0 = functools.reduce(jnp.maximum, s0)
            m1 = functools.reduce(jnp.maximum, s1)
            p0 = [jnp.exp(s - m0) for s in s0]
            p1 = [jnp.exp(s - m1) for s in s1]
            n0 = 1.0 / sum(p0)
            n1 = 1.0 / sum(p1)
            a0 = a1 = jnp.zeros((16, 256), F32)
            c0 = c1 = jnp.zeros((16, 128), F32)
            for k in range(K):
                x, t = near[b, k, pl.ds(r, 16), :], times[k, rows, :]
                a0 += p0[k] * x
                a1 += p1[k] * x
                c0 += p0[k] * t
                c1 += p1[k] * t
            mix[0, rows, 0:256] = a0 * n0
            mix[1, rows, 0:256] = a1 * n1
            mix[0, rows, 256:384] = c0 * n0
            mix[1, rows, 256:384] = c1 * n1
            return inner

        lax.fori_loop(0, 8, group, 0, unroll=2)
        for i in range(32):
            claims[b, i * CAP : (i + 1) * CAP, :] = one_hot(
                asked_by[b, 0:CAP, i : i + 1].astype(I32) == row_lane
            )

        return carry

    lax.fori_loop(0, 4, attend, 0)
    halves = []
    for h in range(2):
        part = mix[h]
        coarse = part.astype(BF16)
        fine = (part - coarse.astype(F32)).astype(BF16)
        halves.append(mm(coarse, wkv[:, 384:768]) + mm(fine, wkv[:, 384:768]))
    attended = jnp.where(head_of, halves[0], halves[1]).astype(BF16)
    hidden = mm(attended, wm[0:384, :]) + mm(src[0].astype(BF16), wm[384:640, :])
    hidden = jnp.maximum(hidden + vec[2:3, 0:EMB], 0.0).astype(BF16)
    embedding[...] = (mm(hidden, w_out[...]) + vec[3:4, 0:EMB]).T.astype(BF16)

    for dy in (2, 1, 3, 0):
        first = 1 if dy == 0 else 0
        wait_bytes(main_recv.at[dy, first:32], recv_main.at[dy])
        wait_bytes(ext_recv.at[dy, first:32], recv_ext.at[dy])
        for i in range(32):
            side[0:1, i * CAP : (i + 1) * CAP] = ext_recv[dy, i, :, 0:CAP]
            side[1:2, i * CAP : (i + 1) * CAP] = ext_recv[dy, i, :, 64 : 64 + CAP]
        count = side[1:2, :]
        high = jnp.floor(count * (1.0 / 128.0))
        row = iota((16, SLOTS), 0)
        rest = jnp.where(
            row == 0,
            side[0:1, :],
            jnp.where(row == 1, count - high * 128.0, jnp.where(row == 2, high, 0.0)),
        )
        left = jnp.concatenate(
            [main_recv[dy].reshape(SLOTS, 128).T, rest.astype(BF16)], axis=0
        )
        total = mm(left, claims[dy])
        if dy == 2:
            acc[...] = total
        else:
            acc[...] += total

    small[...] = jnp.zeros(small.shape, F32)
    small[0:4, :] = vec[4:8, 0:128]
    bias = small[...].T
    b0, b1, b2, b3 = (bias[0:UNITS, g : g + 1] for g in range(4))
    heard = acc[129:130, :] + acc[130:131, :] * 128.0
    share = 1.0 / jnp.maximum(heard, 1.0)
    reset = jax.nn.sigmoid(acc[0:UNITS, :] * share + zed[0, 0:UNITS, :] + b0)
    update = jax.nn.sigmoid(acc[UNITS : 2 * UNITS, :] * share + zed[1, 0:UNITS, :] + b1)
    cand = jnp.tanh(
        acc[2 * UNITS : 3 * UNITS, :] * share
        + zed[2, 0:UNITS, :]
        + b2
        + reset * (zed[3, 0:UNITS, :] + b3)
    )
    mine = own[0:UNITS, :]
    fresh = (1.0 - update) * cand + update * mine
    new_memory[...] = jnp.where(heard > 0.0, fresh, mine)

    wait_bytes(req_recv.at[0:127], send_sem.at[0])
    wait_bytes(edge_recv.at[0:3], send_sem.at[1])
    wait_bytes(w_all.at[0:3, 0:544], send_sem.at[2])
    wait_bytes(wx_all.at[0:3], send_sem.at[3])
    wait_bytes(row_send.at[0:31], send_sem.at[4])
    wait_bytes(main_recv.at[0:3], send_sem.at[5])
    wait_bytes(main_recv.at[3, 0:31], send_sem.at[5])
    wait_bytes(ext_recv.at[0:3], send_sem.at[6])
    wait_bytes(ext_recv.at[3, 0:31], send_sem.at[6])


def step(
    memory,
    last_update,
    ev_time,
    nbr_gap,
    slot_rows,
    slot_ref,
    edge_feat,
    frequency,
    phase_shift,
    w_query,
    w_key,
    w_value,
    w_merge,
    b_merge,
    w_out,
    b_out,
    w_input,
    w_hidden,
    gru_bias,
):
    args = (
        memory.T,
        last_update.reshape(1, ROWS),
        ev_time.reshape(1, EV),
        nbr_gap.T,
        slot_rows,
        slot_ref.T,
        edge_feat.T,
        frequency.reshape(1, TIME),
        phase_shift.reshape(1, TIME),
        w_query,
        w_key,
        w_value,
        w_merge.T,
        b_merge.reshape(1, EMB),
        w_out,
        b_out.reshape(1, EMB),
        jnp.swapaxes(w_input, 1, 2),
        jnp.swapaxes(w_hidden, 1, 2),
        gru_bias,
    )
    vmem = pl.BlockSpec(memory_space=pltpu.VMEM)
    V, D = pltpu.VMEM, pltpu.SemaphoreType.DMA
    embedding, new_memory = pl.pallas_call(
        kernel,
        out_shape=(
            jax.ShapeDtypeStruct((EMB, EV), BF16),
            jax.ShapeDtypeStruct((UNITS, ROWS), F32),
        ),
        in_specs=[pl.BlockSpec(memory_space=pl.ANY)] * len(args),
        out_specs=(vmem, vmem),
        scratch_shapes=[
            V((32, 1, 128), I32),
            V((128, 1, 128), I32),
            V((32, CAP, 256), BF16),
            V((32, CAP, 256), BF16),
            V((4, 64, EV), BF16),
            V((640, 128), BF16),
            V((1, 640), F32),
            V((4, 640, 128), BF16),
            V((4, 1, 640), F32),
            V((4, 4, 8, CAP, 128), BF16),
            V((4, 32, CAP, 128), BF16),
            V((4, 4, 8, 1, 128), F32),
            V((4, 32, 1, 128), F32),
            V((8, 256), F32),
            V((256, ROWS), F32),
            V((ROWS, 256), BF16),
            V((128, EV), F32),
            V((EV, 128), F32),
            V((128, 128), F32),
            V((K, EV, 128), F32),
            V((384, 768), BF16),
            V((384, 384), BF16),
            V((640, EMB), BF16),
            V((8, 640), BF16),
            V((4, CAP, ROWS), F32),
            V((CAP, ROWS), F32),
            V((1, 2 * EV), I32),
            V((1, SLOTS), F32),
            V((2, EV, SLOTS), BF16),
            V((2, EV, 256), F32),
            V((2 * EV, 640), BF16),
            V((16, 384), F32),
            V((EV, 384), F32),
            V((4, K * 128, SLOTS), BF16),
            V((4, K, 128, 256), F32),
            V((2, EV, 384), F32),
            V((4, SLOTS, ROWS), BF16),
            V((4, 128, 128), F32),
            V((2, EV, 384), F32),
            V((8, SLOTS), F32),
            V((144, ROWS), F32),
            D((7,)),
            D((6,)),
            D((4,)),
            D((3,)),
            D((4,)),
            D((4,)),
            D((19,)),
        ]
        + [V(a.shape, a.dtype) for a in args],
        compiler_params=pltpu.CompilerParams(
            collective_id=0, has_side_effects=True, vmem_limit_bytes=60 * 1024 * 1024
        ),
    )(*args)
    return embedding.T, new_memory.T


def solution(mesh):
    return jax.shard_map(
        step,
        mesh=mesh,
        in_specs=(
            P("node", None),
            P("node"),
            P(("node", "feat")),
            P(("node", "feat"), None),
            P(("node", "feat"), None),
            P(("node", "feat"), None),
            P("node", "feat"),
            P(),
            P(),
            P(),
            P(),
            P(),
            P(),
            P(),
            P(),
            P(),
            P(None, None, "feat"),
            P(None, None, "feat"),
            P(None, "feat"),
        ),
        out_specs=(P(("node", "feat"), None), P("node", "feat")),
        check_vma=False,
    )
```

```python
import functools
import math

import jax
import jax.numpy as jnp
from jax import lax
from jax.experimental import pallas as pl
from jax.experimental.pallas import tpu as pltpu
from jax.sharding import PartitionSpec as P

F32, BF16, I32 = jnp.float32, jnp.bfloat16, jnp.int32
MESH = pl.DeviceIdType.MESH
COS = (
    0.9999999998851011,
    -0.49999999850736465,
    0.041666663483369594,
    -0.0013888863001969808,
    2.4800551963260593e-05,
    -2.7534774132807624e-07,
    2.060335926598073e-09,
    -9.721760760713551e-12,
)
TURN_HI = 6.28125
TURN_LO = 2.0 * math.pi - TURN_HI

MEM, TIME, ATT, EMB, UNITS = 172, 100, 272, 172, 43
CAP, K, EV, ROWS, SLOTS = 48, 10, 512, 1024, 1536
HEAD = ATT // 2


def cosine(x):
    turns = jnp.floor(x * (0.5 / math.pi) + 0.5)
    r = (x - turns * TURN_HI) - turns * TURN_LO
    u = r * r
    total = jnp.full_like(u, COS[-1])
    for c in COS[-2::-1]:
        total = total * u + c
    return total


def mm(a, b):
    return jnp.dot(a, b, preferred_element_type=F32)


def mm_nt(a, b):
    return lax.dot_general(a, b, (((1,), (1,)), ((), ())), preferred_element_type=F32)


def iota(shape, dim):
    return lax.broadcasted_iota(I32, shape, dim)


def one_hot(mask):
    return jnp.where(mask, 1.0, 0.0).astype(BF16)


def kernel(*refs):
    given, refs = refs[:19], refs[19:]
    loaded, refs = refs[-19:], refs[:-19]
    (
        embedding,
        new_memory,
        req_send,
        req_recv,
        row_send,
        fetched,
        edge_recv,
        w_mine,
        wx_mine,
        w_all,
        wx_all,
        main_send,
        main_recv,
        ext_send,
        ext_recv,
        vec,
        mem_t,
        memb,
        wide_t,
        cols,
        small,
        times,
        wkv,
        wq,
        wm,
        w_ext,
        zed,
        own,
        end_cols,
        ends,
        src,
        msg,
        ext_tmp,
        query,
        hot,
        near,
        qk,
        claims,
        asked_by,
        mix,
        side,
        acc,
        send_sem,
        recv_req,
        recv_rows,
        recv_x,
        recv_main,
        recv_ext,
        in_sem,
    ) = refs
    (
        memory,
        last_update,
        ev_time,
        nbr_gap,
        slot_rows,
        slot_ref,
        edge_feat,
        frequency,
        phase_shift,
        w_query,
        w_key,
        w_value,
        w_merge,
        b_merge,
        w_out,
        b_out,
        w_input,
        w_hidden,
        gru_bias,
    ) = loaded
    loads = [
        pltpu.make_async_copy(a, b, in_sem.at[i]) for i, (a, b) in enumerate(zip(given, loaded))
    ]
    n = lax.axis_index("node")
    f = lax.axis_index("feat")
    y, z, c = n // 8, (n // 2) % 4, n % 2
    at_y = [((y + d) % 4) * 8 for d in range(4)]
    at_z = [((z + d) % 4) * 2 for d in range(4)]
    at_c = [(c + d) % 2 for d in range(2)]
    at_f = [(f + d) % 4 for d in range(4)]
    def peer(t, i, dx):
        return at_y[i // 2] + at_z[(t - i // 2) % 4] + at_c[i % 2], at_f[dx]

    def send(src_ref, dst_ref, s_sem, r_sem, to):
        pltpu.make_async_remote_copy(
            src_ref=src_ref,
            dst_ref=dst_ref,
            send_sem=s_sem,
            recv_sem=r_sem,
            device_id=to,
            device_id_type=MESH,
        ).start()

    def wait_bytes(ref, sem):
        pltpu.make_async_copy(ref, ref, sem).wait()

    everyone = [(t, dx, i) for t in range(4) for dx in range(4) for i in range(8)][1:]

    for dx in range(4):
        w_all[dx, 176:256, :] = jnp.zeros((80, 128), BF16)
        w_all[dx, 368:384, :] = jnp.zeros((16, 128), BF16)

    barrier = pltpu.get_barrier_semaphore()
    near_by = [(t, dx, i) for t, dx, i in everyone if dx == 0 or (t == 0 and i == 0)]
    for t, dx, i in near_by:
        pl.semaphore_signal(
            barrier, inc=1, device_id=peer(t, i, dx), device_id_type=MESH
        )
    for first in (4, 0, 1, 6):
        loads[first].start()
    for i in range(19):
        if i not in (4, 0, 1, 6):
            loads[i].start()

    req_send[...] = jnp.full(req_send.shape, -1, I32)
    loads[4].wait()
    for o in range(32):
        req_send[o, :, 0:CAP] = slot_rows[:, o * CAP : (o + 1) * CAP]
    req_recv[0] = req_send[n]
    loads[6].wait()
    edge_recv[f] = edge_feat[:, pl.ds(pl.multiple_of(f * EV, EV), EV)]

    loads[0].wait()
    loads[1].wait()
    mem_t[0:MEM, :] = memory[...]
    stamp = last_update[...].astype(F32)
    high = jnp.floor(stamp * (1.0 / 128.0))
    mem_t[MEM : MEM + 1, :] = high
    mem_t[MEM + 1 : MEM + 2, :] = stamp - high * 128.0
    mem_t[MEM + 2 : 256, :] = jnp.zeros((256 - MEM - 2, ROWS), F32)
    for b in range(4):
        memb[b * 256 : (b + 1) * 256, :] = mem_t[:, b * 256 : (b + 1) * 256].T.astype(BF16)

    pl.semaphore_wait(barrier, len(near_by))

    for t, dx, i in everyone:
        if dx == 0:
            to = peer(t, i, 0)
            send(
                req_send.at[to[0]],
                req_recv.at[t * 32 + i],
                send_sem.at[0],
                recv_req.at[2 + t],
                to,
            )
    for dx in range(1, 4):
        to = peer(0, 0, dx)
        send(
            edge_feat.at[:, pl.ds(pl.multiple_of(to[1] * EV, EV), EV)],
            edge_recv.at[f],
            send_sem.at[1],
            recv_x.at[0],
            to,
        )

    loads[16].wait()
    r640 = iota((640, 700), 0)
    c640 = iota((640, 700), 1)
    place = one_hot(
        ((r640 < MEM) & (c640 == r640 + MEM))
        | ((r640 >= 256) & (r640 < 256 + TIME) & (c640 == r640 - 256 + 2 * MEM))
        | ((r640 >= 384) & (c640 == r640 - 384 + 2 * MEM + TIME))
    )
    rows43 = iota((128, UNITS), 0)
    cols43 = iota((128, UNITS), 1)
    wide = mm(one_hot(rows43 == cols43), w_input[0].astype(BF16))
    wide += mm(one_hot(rows43 == cols43 + UNITS), w_input[1].astype(BF16))
    wide += mm(one_hot(rows43 == cols43 + 2 * UNITS), w_input[2].astype(BF16))
    w_mine[...] = mm_nt(place, wide.astype(BF16)).astype(BF16)
    last = mm(one_hot(iota((8, UNITS), 1) == UNITS - 1), w_input[2].astype(BF16))
    wx_mine[...] = mm_nt(last.astype(BF16), place)[0:1, :]
    for dx in range(1, 4):
        to = peer(0, 0, 4 - dx)
        for rows in (slice(0, 176), slice(256, 368), slice(384, 640)):
            send(w_mine.at[rows], w_all.at[dx, rows], send_sem.at[2], recv_x.at[1], to)
        send(wx_mine, wx_all.at[dx], send_sem.at[3], recv_x.at[2], to)
    w_all[0] = w_mine[...]
    wx_all[0] = wx_mine[...]

    for i in (2, 3, 5, 7, 8, 9, 10, 11, 12, 13, 14, 15, 17, 18):
        loads[i].wait()
    vec[...] = jnp.zeros(vec.shape, F32)
    vec[0:1, 0:TIME] = frequency[...]
    vec[1:2, 0:TIME] = phase_shift[...]
    vec[2:3, 0:EMB] = b_merge[...]
    vec[3:4, 0:EMB] = b_out[...]
    vec[4:8, 0:UNITS] = gru_bias[...]
    freq = vec[0:1, 0:128]
    phase = vec[1:2, 0:128]

    wide_t[...] = jnp.zeros(wide_t.shape, F32)
    wide_t[0 : K + 2, :] = slot_ref[...].astype(F32)
    wide_t[16 : 16 + K, :] = nbr_gap[...].astype(F32)
    wide_t[32:33, :] = ev_time[...].astype(F32)
    cols[...] = wide_t[...].T
    end_cols[:, 0:EV] = slot_ref[0:1, :]
    end_cols[:, EV : 2 * EV] = slot_ref[1:2, :]

    for k in range(K):
        times[k] = cosine(cols[:, 16 + k : 17 + k] * freq + phase).astype(BF16).astype(F32)

    for t in range(4):
        first = 1 if t == 0 else 0
        wait_bytes(req_recv.at[t * 32 + first : t * 32 + 8], recv_req.at[2 + t])
    small[...] = jnp.zeros(small.shape, F32)
    for t in range(4):
        small[8 * t : 8 * t + 8, :] = req_recv[t * 32 : t * 32 + 8].reshape(8, 128).astype(F32)
    asked = small[...].T.astype(I32)
    row_lane = iota((CAP, ROWS), 1)
    for t in (2, 1, 3, 0):
        mask = jnp.concatenate(
            [
                one_hot(asked[0:CAP, 8 * t + i : 8 * t + i + 1] == row_lane)
                for i in range(8)
            ],
            axis=0,
        )
        rows = mm(mask, memb[...]).astype(BF16)
        for i in range(8):
            if t == 0 and i == 0:
                fetched[n] = rows[0:CAP, :]
            else:
                row_send[t * 8 + i] = rows[i * CAP : (i + 1) * CAP, :]
        for i in (4, 2, 6, 0, 5, 3, 7, 1):
            if t == 0 and i == 0:
                continue
            send(
                row_send.at[t * 8 + i],
                fetched.at[n],
                send_sem.at[4],
                recv_rows,
                peer((4 - t) % 4, (4 - i // 2) % 4 * 2 + i % 2, 0),
            )

    wait_bytes(edge_recv.at[0:3], recv_x.at[0])
    for t, dx, i in everyone:
        if dx != 0:
            to = peer(t, i, dx)
            send(
                req_send.at[to[0]],
                req_recv.at[t * 32 + dx * 8 + i],
                send_sem.at[0],
                recv_req.at[1],
                to,
            )

    slot_lane = iota((128, SLOTS), 1)

    def mark(b, carry):
        rows = pl.ds(pl.multiple_of(b * 128, 128), 128)
        picks = cols[rows, :].astype(I32)
        for k in range(K):
            hot[b, k * 128 : (k + 1) * 128, :] = one_hot(picks[:, 2 + k : 3 + k] == slot_lane)
        for e in range(2):
            ends[e, rows, :] = one_hot(picks[:, e : e + 1] == slot_lane)
        return carry

    lax.fori_loop(0, 4, mark, 0)

    r272 = iota((384, ATT), 0)
    c272 = iota((384, ATT), 1)
    place = one_hot(
        ((c272 < MEM) & (r272 == c272)) | ((c272 >= MEM) & (r272 == c272 + (256 - MEM)))
    )
    wkv[...] = jnp.zeros(wkv.shape, BF16)
    wkv[:, 0:ATT] = mm(place, w_key[...]).astype(BF16)
    wkv[:, 384 : 384 + ATT] = mm(place, w_value[...]).astype(BF16)
    wq[...] = jnp.zeros(wq.shape, BF16)
    wq[:, 0:ATT] = mm(place, w_query[...]).astype(BF16)
    r444 = iota((640, ATT + MEM), 0)
    c444 = iota((640, ATT + MEM), 1)
    place = one_hot(
        ((c444 < ATT) & (r444 == c444)) | ((c444 >= ATT) & (r444 == c444 + (384 - ATT)))
    )
    wm[...] = mm_nt(place, w_merge[...]).astype(BF16)

    widen = one_hot(iota((CAP, UNITS), 0) == iota((CAP, UNITS), 1))
    mem_b = memory[...].astype(BF16)
    gates = (
        w_input[0, :, 0:MEM] + w_hidden[0],
        w_input[1, :, 0:MEM] + w_hidden[1],
        w_input[2, :, 0:MEM],
        w_hidden[2],
    )
    for g, w in enumerate(gates):
        zed[g] = mm(mm(widen, w.astype(BF16)).astype(BF16), mem_b)
    own[...] = jnp.dot(
        jnp.where(
            (iota((CAP, MEM), 1) == iota((CAP, MEM), 0) + f * UNITS)
            & (iota((CAP, MEM), 0) < UNITS),
            1.0,
            0.0,
        ),
        memory[...],
        preferred_element_type=F32,
        precision=lax.Precision.HIGHEST,
    )

    edges = edge_recv[...].reshape(256, EV).astype(F32).T.astype(BF16)
    for e in range(2):
        msg[e * EV : (e + 1) * EV, 384:640] = edges
    ext_send[...] = jnp.zeros(ext_send.shape, F32)

    wait_bytes(req_recv.at[0:96], recv_req.at[1])
    for t in range(4):
        small[...] = jnp.zeros(small.shape, F32)
        small[0:32, :] = req_recv[t * 32 : t * 32 + 32].reshape(32, 128).astype(F32)
        asked_by[t] = small[...].T

    def claim(t, carry):
        for i in range(32):
            claims[t, i * CAP : (i + 1) * CAP, :] = one_hot(
                asked_by[t, 0:CAP, i : i + 1].astype(I32) == row_lane
            )
        return carry

    lax.fori_loop(0, 4, claim, 0)

    wait_bytes(fetched.at[0:31], recv_rows)
    table = fetched.reshape(SLOTS, 256)
    for e in range(2):
        src[e] = mm(ends[e], table[...])
    lane = iota((EV, 256), 1)
    counted = (lane == MEM + 2) | (lane == MEM + 3)
    for e in range(2):
        msg[e * EV : (e + 1) * EV, 0:256] = jnp.where(counted, 1.0, src[1 - e]).astype(BF16)
        stamp = src[e, :, MEM : MEM + 1] * 128.0 + src[e, :, MEM + 1 : MEM + 2]
        gap = cols[:, 32:33] - stamp
        msg[e * EV : (e + 1) * EV, 256:384] = cosine(gap * freq + phase).astype(BF16)

    wait_bytes(w_all.at[0:3, 0:544], recv_x.at[1])
    wait_bytes(wx_all.at[0:3], recv_x.at[2])
    rows4 = jnp.concatenate([wx_all[dx] for dx in range(4)] + [jnp.zeros((4, 640), F32)], axis=0)
    row = iota((8, 640), 0)
    counts = (row >= 4) & (row < 6) & (iota((8, 640), 1) == row + (MEM + 2 - 4))
    w_ext[...] = jnp.where(counts, 1.0, rows4).astype(BF16)

    lane = iota((384, 256), 1)
    for t in (2, 1, 3, 0):
        mask = jnp.concatenate(
            [
                one_hot(
                    iota((2 * CAP, 2 * EV), 0) + (at_y[dy] + at_z[(t - dy) % 4]) * CAP
                    == end_cols[...]
                )
                for dy in range(4)
            ],
            axis=0,
        )
        total = mm(mask, msg[...])
        first = total[:, 0:256]
        high = jnp.floor(first * (1.0 / 128.0))
        first = jnp.where(
            lane == MEM + 2, first - high * 128.0, jnp.where(lane == MEM + 3, high, first)
        )
        sums = jnp.concatenate([first, total[:, 256:640]], axis=1).astype(BF16)
        for pair in range(2):
            w_pair = jnp.concatenate([w_all[2 * pair], w_all[2 * pair + 1]], axis=1)
            out = mm(sums, w_pair).astype(BF16)
            for i in range(2):
                main_send[t, 2 * pair + i] = out[:, i * 128 : (i + 1) * 128].reshape(8, CAP, 128)
        ext_tmp[0:8, :] = mm_nt(w_ext[...], sums)
        ext_tmp[8:9, :] = ext_tmp[4:5, :] + ext_tmp[5:6, :] * 128.0
        for j in range(8):
            count_row = ext_tmp[8:9, j * CAP : (j + 1) * CAP]
            for dx in range(4):
                ext_send[t, dx, j, :, 0:CAP] = ext_tmp[dx : dx + 1, j * CAP : (j + 1) * CAP]
                ext_send[t, dx, j, :, 64 : 64 + CAP] = count_row
        for i in (4, 2, 6, 0, 5, 3, 7, 1):
            for dx in (2, 1, 3, 0):
                if t == 0 and dx == 0 and i == 0:
                    continue
                to = peer(t, i, dx)
                at = i // 2 * 2 + at_c[i % 2]
                send(
                    main_send.at[t, dx, at],
                    main_recv.at[t, dx * 8 + i],
                    send_sem.at[5],
                    recv_main.at[t],
                    to,
                )
                send(
                    ext_send.at[t, dx, at],
                    ext_recv.at[t, dx * 8 + i],
                    send_sem.at[6],
                    recv_ext.at[t],
                    to,
                )
    main_recv[0, 0] = main_send[0, 0, at_c[0]]
    ext_recv[0, 0] = ext_send[0, 0, at_c[0]]

    still = jnp.broadcast_to(cosine(phase), (EV, 128)).astype(BF16)
    query[...] = (
        mm(src[0].astype(BF16), wq[0:256, :]) + mm(still, wq[256:384, :])
    ) * (1.0 / math.sqrt(HEAD))
    head_of = iota((EV, 384), 1) < HEAD
    for h in range(2):
        part = query[...]
        part = jnp.where(head_of, part, 0.0) if h == 0 else jnp.where(head_of, 0.0, part)
        coarse = part.astype(BF16)
        fine = (part - coarse.astype(F32)).astype(BF16)
        qk[h] = mm_nt(coarse, wkv[:, 0:384]) + mm_nt(fine, wkv[:, 0:384])

    def attend(b, carry):
        at = pl.multiple_of(b * 128, 128)
        near[...] = mm(hot[b], table[...]).reshape(K, 128, 256)

        def group(g, inner):
            r = pl.multiple_of(g * 16, 16)
            rows = pl.ds(at + r, 16)
            q0, q1 = qk[0, rows, :], qk[1, rows, :]
            s0, s1 = [], []
            for k in range(K):
                x, t = near[k, pl.ds(r, 16), :], times[k, rows, :]
                u0 = x * q0[:, 0:256]
                u1 = x * q1[:, 0:256]
                u0 = u0[:, 0:128] + u0[:, 128:256] + t * q0[:, 256:384]
                u1 = u1[:, 0:128] + u1[:, 128:256] + t * q1[:, 256:384]
                s0.append(jnp.sum(u0, axis=1, keepdims=True))
                s1.append(jnp.sum(u1, axis=1, keepdims=True))
            m0 = functools.reduce(jnp.maximum, s0)
            m1 = functools.reduce(jnp.maximum, s1)
            p0 = [jnp.exp(s - m0) for s in s0]
            p1 = [jnp.exp(s - m1) for s in s1]
            n0 = 1.0 / sum(p0)
            n1 = 1.0 / sum(p1)
            a0 = a1 = jnp.zeros((16, 256), F32)
            c0 = c1 = jnp.zeros((16, 128), F32)
            for k in range(K):
                x, t = near[k, pl.ds(r, 16), :], times[k, rows, :]
                a0 += p0[k] * x
                a1 += p1[k] * x
                c0 += p0[k] * t
                c1 += p1[k] * t
            mix[0, rows, 0:256] = a0 * n0
            mix[1, rows, 0:256] = a1 * n1
            mix[0, rows, 256:384] = c0 * n0
            mix[1, rows, 256:384] = c1 * n1
            return inner

        lax.fori_loop(0, 8, group, 0, unroll=2)
        return carry

    lax.fori_loop(0, 4, attend, 0)
    halves = []
    for h in range(2):
        part = mix[h]
        coarse = part.astype(BF16)
        fine = (part - coarse.astype(F32)).astype(BF16)
        halves.append(mm(coarse, wkv[:, 384:768]) + mm(fine, wkv[:, 384:768]))
    attended = jnp.where(head_of, halves[0], halves[1]).astype(BF16)
    hidden = mm(attended, wm[0:384, :]) + mm(src[0].astype(BF16), wm[384:640, :])
    hidden = jnp.maximum(hidden + vec[2:3, 0:EMB], 0.0).astype(BF16)
    embedding[...] = (mm(hidden, w_out[...]) + vec[3:4, 0:EMB]).T.astype(BF16)

    for t in (2, 1, 3, 0):
        first = 1 if t == 0 else 0
        wait_bytes(main_recv.at[t, first:32], recv_main.at[t])
        wait_bytes(ext_recv.at[t, first:32], recv_ext.at[t])
        for i in range(32):
            side[0:1, i * CAP : (i + 1) * CAP] = ext_recv[t, i, :, 0:CAP]
            side[1:2, i * CAP : (i + 1) * CAP] = ext_recv[t, i, :, 64 : 64 + CAP]
        count = side[1:2, :]
        high = jnp.floor(count * (1.0 / 128.0))
        row = iota((16, SLOTS), 0)
        rest = jnp.where(
            row == 0,
            side[0:1, :],
            jnp.where(row == 1, count - high * 128.0, jnp.where(row == 2, high, 0.0)),
        )
        left = jnp.concatenate(
            [main_recv[t].reshape(SLOTS, 128).T, rest.astype(BF16)], axis=0
        )
        total = mm(left, claims[t])
        if t == 2:
            acc[...] = total
        else:
            acc[...] += total

    small[...] = jnp.zeros(small.shape, F32)
    small[0:4, :] = vec[4:8, 0:128]
    bias = small[...].T
    b0, b1, b2, b3 = (bias[0:UNITS, g : g + 1] for g in range(4))
    heard = acc[129:130, :] + acc[130:131, :] * 128.0
    share = 1.0 / jnp.maximum(heard, 1.0)
    reset = jax.nn.sigmoid(acc[0:UNITS, :] * share + zed[0, 0:UNITS, :] + b0)
    update = jax.nn.sigmoid(acc[UNITS : 2 * UNITS, :] * share + zed[1, 0:UNITS, :] + b1)
    cand = jnp.tanh(
        acc[2 * UNITS : 3 * UNITS, :] * share
        + zed[2, 0:UNITS, :]
        + b2
        + reset * (zed[3, 0:UNITS, :] + b3)
    )
    mine = own[0:UNITS, :]
    fresh = (1.0 - update) * cand + update * mine
    new_memory[...] = jnp.where(heard > 0.0, fresh, mine)

    wait_bytes(req_recv.at[0:127], send_sem.at[0])
    wait_bytes(edge_recv.at[0:3], send_sem.at[1])
    wait_bytes(w_all.at[0:3, 0:544], send_sem.at[2])
    wait_bytes(wx_all.at[0:3], send_sem.at[3])
    wait_bytes(row_send.at[0:31], send_sem.at[4])
    wait_bytes(main_recv.at[0:3], send_sem.at[5])
    wait_bytes(main_recv.at[3, 0:31], send_sem.at[5])
    wait_bytes(ext_recv.at[0:3], send_sem.at[6])
    wait_bytes(ext_recv.at[3, 0:31], send_sem.at[6])


def step(
    memory,
    last_update,
    ev_time,
    nbr_gap,
    slot_rows,
    slot_ref,
    edge_feat,
    frequency,
    phase_shift,
    w_query,
    w_key,
    w_value,
    w_merge,
    b_merge,
    w_out,
    b_out,
    w_input,
    w_hidden,
    gru_bias,
):
    args = (
        memory.T,
        last_update.reshape(1, ROWS),
        ev_time.reshape(1, EV),
        nbr_gap.T,
        slot_rows,
        slot_ref.T,
        edge_feat.T,
        frequency.reshape(1, TIME),
        phase_shift.reshape(1, TIME),
        w_query,
        w_key,
        w_value,
        w_merge.T,
        b_merge.reshape(1, EMB),
        w_out,
        b_out.reshape(1, EMB),
        jnp.swapaxes(w_input, 1, 2),
        jnp.swapaxes(w_hidden, 1, 2),
        gru_bias,
    )
    vmem = pl.BlockSpec(memory_space=pltpu.VMEM)
    V, D = pltpu.VMEM, pltpu.SemaphoreType.DMA
    embedding, new_memory = pl.pallas_call(
        kernel,
        out_shape=(
            jax.ShapeDtypeStruct((EMB, EV), BF16),
            jax.ShapeDtypeStruct((UNITS, ROWS), F32),
        ),
        in_specs=[pl.BlockSpec(memory_space=pl.ANY)] * len(args),
        out_specs=(vmem, vmem),
        scratch_shapes=[
            V((32, 1, 128), I32),
            V((128, 1, 128), I32),
            V((32, CAP, 256), BF16),
            V((32, CAP, 256), BF16),
            V((4, 64, EV), BF16),
            V((640, 128), BF16),
            V((1, 640), F32),
            V((4, 640, 128), BF16),
            V((4, 1, 640), F32),
            V((4, 4, 8, CAP, 128), BF16),
            V((4, 32, CAP, 128), BF16),
            V((4, 4, 8, 1, 128), F32),
            V((4, 32, 1, 128), F32),
            V((8, 256), F32),
            V((256, ROWS), F32),
            V((ROWS, 256), BF16),
            V((128, EV), F32),
            V((EV, 128), F32),
            V((128, 128), F32),
            V((K, EV, 128), F32),
            V((384, 768), BF16),
            V((384, 384), BF16),
            V((640, EMB), BF16),
            V((8, 640), BF16),
            V((4, CAP, ROWS), F32),
            V((CAP, ROWS), F32),
            V((1, 2 * EV), I32),
            V((2, EV, SLOTS), BF16),
            V((2, EV, 256), F32),
            V((2 * EV, 640), BF16),
            V((16, 384), F32),
            V((EV, 384), F32),
            V((4, K * 128, SLOTS), BF16),
            V((K, 128, 256), F32),
            V((2, EV, 384), F32),
            V((4, SLOTS, ROWS), BF16),
            V((4, 128, 128), F32),
            V((2, EV, 384), F32),
            V((8, SLOTS), F32),
            V((144, ROWS), F32),
            D((7,)),
            D((6,)),
            D,
            D((3,)),
            D((4,)),
            D((4,)),
            D((19,)),
        ]
        + [V(a.shape, a.dtype) for a in args],
        compiler_params=pltpu.CompilerParams(
            collective_id=0, has_side_effects=True, vmem_limit_bytes=60 * 1024 * 1024
        ),
    )(*args)
    return embedding.T, new_memory.T


def solution(mesh):
    return jax.shard_map(
        step,
        mesh=mesh,
        in_specs=(
            P("node", None),
            P("node"),
            P(("node", "feat")),
            P(("node", "feat"), None),
            P(("node", "feat"), None),
            P(("node", "feat"), None),
            P("node", "feat"),
            P(),
            P(),
            P(),
            P(),
            P(),
            P(),
            P(),
            P(),
            P(),
            P(None, None, "feat"),
            P(None, None, "feat"),
            P(None, "feat"),
        ),
        out_specs=(P(("node", "feat"), None), P("node", "feat")),
        check_vma=False,
    )
```

```python
import functools
import math

import jax
import jax.numpy as jnp
from jax import lax
from jax.experimental import pallas as pl
from jax.experimental.pallas import tpu as pltpu
from jax.sharding import PartitionSpec as P

F32, BF16, I32 = jnp.float32, jnp.bfloat16, jnp.int32
MESH = pl.DeviceIdType.MESH
COS = (
    0.9999999998851011,
    -0.49999999850736465,
    0.041666663483369594,
    -0.0013888863001969808,
    2.4800551963260593e-05,
    -2.7534774132807624e-07,
    2.060335926598073e-09,
    -9.721760760713551e-12,
)
TURN_HI = 6.28125
TURN_LO = 2.0 * math.pi - TURN_HI

MEM, TIME, ATT, EMB, UNITS = 172, 100, 272, 172, 43
CAP, K, EV, ROWS, SLOTS = 48, 10, 512, 1024, 1536
HEAD = ATT // 2


def cosine(x):
    turns = jnp.floor(x * (0.5 / math.pi) + 0.5)
    r = (x - turns * TURN_HI) - turns * TURN_LO
    u = r * r
    total = jnp.full_like(u, COS[-1])
    for c in COS[-2::-1]:
        total = total * u + c
    return total


def mm(a, b):
    return jnp.dot(a, b, preferred_element_type=F32)


def mm_nt(a, b):
    return lax.dot_general(a, b, (((1,), (1,)), ((), ())), preferred_element_type=F32)


def iota(shape, dim):
    return lax.broadcasted_iota(I32, shape, dim)


def one_hot(mask):
    return jnp.where(mask, 1.0, 0.0).astype(BF16)


def kernel(*refs):
    given, refs = refs[:19], refs[19:]
    loaded, refs = refs[-19:], refs[:-19]
    (
        embedding,
        new_memory,
        req_send,
        req_recv,
        row_send,
        fetched,
        edge_recv,
        w_mine,
        wx_mine,
        w_all,
        wx_all,
        main_send,
        main_recv,
        ext_send,
        ext_recv,
        vec,
        mem_t,
        memb,
        wide_t,
        cols,
        small,
        times,
        wkv,
        wq,
        wm,
        w_ext,
        zed,
        own,
        end_cols,
        ends,
        src,
        msg,
        ext_tmp,
        query,
        hot,
        near,
        qk,
        claims,
        asked_by,
        mix,
        side,
        acc,
        send_sem,
        recv_req,
        recv_rows,
        recv_x,
        recv_main,
        recv_ext,
        in_sem,
    ) = refs
    (
        memory,
        last_update,
        ev_time,
        nbr_gap,
        slot_rows,
        slot_ref,
        edge_feat,
        frequency,
        phase_shift,
        w_query,
        w_key,
        w_value,
        w_merge,
        b_merge,
        w_out,
        b_out,
        w_input,
        w_hidden,
        gru_bias,
    ) = loaded
    loads = [
        pltpu.make_async_copy(a, b, in_sem.at[i]) for i, (a, b) in enumerate(zip(given, loaded))
    ]
    n = lax.axis_index("node")
    f = lax.axis_index("feat")
    y, z, c = n // 8, (n // 2) % 4, n % 2
    at_y = [((y + d) % 4) * 8 for d in range(4)]
    at_z = [((z + d) % 4) * 2 for d in range(4)]
    at_c = [(c + d) % 2 for d in range(2)]
    at_f = [(f + d) % 4 for d in range(4)]
    def peer(t, i, dx):
        return at_y[i // 2] + at_z[(t - i // 2) % 4] + at_c[i % 2], at_f[dx]

    def send(src_ref, dst_ref, s_sem, r_sem, to):
        pltpu.make_async_remote_copy(
            src_ref=src_ref,
            dst_ref=dst_ref,
            send_sem=s_sem,
            recv_sem=r_sem,
            device_id=to,
            device_id_type=MESH,
        ).start()

    def wait_bytes(ref, sem):
        pltpu.make_async_copy(ref, ref, sem).wait()

    everyone = [(t, dx, i) for t in range(4) for dx in range(4) for i in range(8)][1:]

    for dx in range(4):
        w_all[dx, 176:256, :] = jnp.zeros((80, 128), BF16)
        w_all[dx, 368:384, :] = jnp.zeros((16, 128), BF16)

    barrier = pltpu.get_barrier_semaphore()
    near_by = [(t, dx, i) for t, dx, i in everyone if dx == 0 or (t == 0 and i == 0)]
    for t, dx, i in near_by:
        pl.semaphore_signal(
            barrier, inc=1, device_id=peer(t, i, dx), device_id_type=MESH
        )
    for first in (4, 0, 1, 6):
        loads[first].start()
    for i in range(19):
        if i not in (4, 0, 1, 6):
            loads[i].start()

    req_send[...] = jnp.full(req_send.shape, -1, I32)
    loads[4].wait()
    for o in range(32):
        req_send[o, :, 0:CAP] = slot_rows[:, o * CAP : (o + 1) * CAP]
    req_recv[0] = req_send[n]
    loads[6].wait()
    edge_recv[f] = edge_feat[:, pl.ds(pl.multiple_of(f * EV, EV), EV)]

    loads[0].wait()
    loads[1].wait()
    mem_t[0:MEM, :] = memory[...]
    stamp = last_update[...].astype(F32)
    high = jnp.floor(stamp * (1.0 / 128.0))
    mem_t[MEM : MEM + 1, :] = high
    mem_t[MEM + 1 : MEM + 2, :] = stamp - high * 128.0
    mem_t[MEM + 2 : 256, :] = jnp.zeros((256 - MEM - 2, ROWS), F32)
    for b in range(4):
        memb[b * 256 : (b + 1) * 256, :] = mem_t[:, b * 256 : (b + 1) * 256].T.astype(BF16)

    pl.semaphore_wait(barrier, len(near_by))

    for t, dx, i in everyone:
        if dx == 0:
            to = peer(t, i, 0)
            send(
                req_send.at[to[0]],
                req_recv.at[t * 32 + i],
                send_sem.at[0],
                recv_req.at[2 + t],
                to,
            )
    for dx in range(1, 4):
        to = peer(0, 0, dx)
        send(
            edge_feat.at[:, pl.ds(pl.multiple_of(to[1] * EV, EV), EV)],
            edge_recv.at[f],
            send_sem.at[1],
            recv_x.at[0],
            to,
        )

    loads[16].wait()
    r640 = iota((640, 700), 0)
    c640 = iota((640, 700), 1)
    place = one_hot(
        ((r640 < MEM) & (c640 == r640 + MEM))
        | ((r640 >= 256) & (r640 < 256 + TIME) & (c640 == r640 - 256 + 2 * MEM))
        | ((r640 >= 384) & (c640 == r640 - 384 + 2 * MEM + TIME))
    )
    rows43 = iota((128, UNITS), 0)
    cols43 = iota((128, UNITS), 1)
    wide = mm(one_hot(rows43 == cols43), w_input[0].astype(BF16))
    wide += mm(one_hot(rows43 == cols43 + UNITS), w_input[1].astype(BF16))
    wide += mm(one_hot(rows43 == cols43 + 2 * UNITS), w_input[2].astype(BF16))
    w_mine[...] = mm_nt(place, wide.astype(BF16)).astype(BF16)
    last = mm(one_hot(iota((8, UNITS), 1) == UNITS - 1), w_input[2].astype(BF16))
    wx_mine[...] = mm_nt(last.astype(BF16), place)[0:1, :]
    for dx in range(1, 4):
        to = peer(0, 0, 4 - dx)
        for rows in (slice(0, 176), slice(256, 368), slice(384, 640)):
            send(w_mine.at[rows], w_all.at[dx, rows], send_sem.at[2], recv_x.at[1], to)
        send(wx_mine, wx_all.at[dx], send_sem.at[3], recv_x.at[2], to)
    w_all[0] = w_mine[...]
    wx_all[0] = wx_mine[...]

    for t in range(4):
        first = 1 if t == 0 else 0
        wait_bytes(req_recv.at[t * 32 + first : t * 32 + 8], recv_req.at[2 + t])
    small[...] = jnp.zeros(small.shape, F32)
    for t in range(4):
        small[8 * t : 8 * t + 8, :] = req_recv[t * 32 : t * 32 + 8].reshape(8, 128).astype(F32)
    asked = small[...].T.astype(I32)
    row_lane = iota((CAP, ROWS), 1)
    for t in (2, 1, 3, 0):
        mask = jnp.concatenate(
            [
                one_hot(asked[0:CAP, 8 * t + i : 8 * t + i + 1] == row_lane)
                for i in range(8)
            ],
            axis=0,
        )
        rows = mm(mask, memb[...]).astype(BF16)
        for i in range(8):
            if t == 0 and i == 0:
                fetched[n] = rows[0:CAP, :]
            else:
                row_send[t * 8 + i] = rows[i * CAP : (i + 1) * CAP, :]
        for i in (4, 2, 6, 0, 5, 3, 7, 1):
            if t == 0 and i == 0:
                continue
            send(
                row_send.at[t * 8 + i],
                fetched.at[n],
                send_sem.at[4],
                recv_rows,
                peer((4 - t) % 4, (4 - i // 2) % 4 * 2 + i % 2, 0),
            )

    wait_bytes(edge_recv.at[0:3], recv_x.at[0])
    for t, dx, i in everyone:
        if dx != 0:
            to = peer(t, i, dx)
            send(
                req_send.at[to[0]],
                req_recv.at[t * 32 + dx * 8 + i],
                send_sem.at[0],
                recv_req.at[1],
                to,
            )

    for i in (2, 3, 5, 7, 8, 9, 10, 11, 12, 13, 14, 15, 17, 18):
        loads[i].wait()
    vec[...] = jnp.zeros(vec.shape, F32)
    vec[0:1, 0:TIME] = frequency[...]
    vec[1:2, 0:TIME] = phase_shift[...]
    vec[2:3, 0:EMB] = b_merge[...]
    vec[3:4, 0:EMB] = b_out[...]
    vec[4:8, 0:UNITS] = gru_bias[...]
    freq = vec[0:1, 0:128]
    phase = vec[1:2, 0:128]

    wide_t[...] = jnp.zeros(wide_t.shape, F32)
    wide_t[0 : K + 2, :] = slot_ref[...].astype(F32)
    wide_t[16 : 16 + K, :] = nbr_gap[...].astype(F32)
    wide_t[32:33, :] = ev_time[...].astype(F32)
    cols[...] = wide_t[...].T
    end_cols[:, 0:EV] = slot_ref[0:1, :]
    end_cols[:, EV : 2 * EV] = slot_ref[1:2, :]

    for k in range(K):
        times[k] = cosine(cols[:, 16 + k : 17 + k] * freq + phase).astype(BF16).astype(F32)

    slot_lane = iota((128, SLOTS), 1)

    def mark(b, carry):
        rows = pl.ds(pl.multiple_of(b * 128, 128), 128)
        picks = cols[rows, :].astype(I32)
        for k in range(K):
            hot[b, k * 128 : (k + 1) * 128, :] = one_hot(picks[:, 2 + k : 3 + k] == slot_lane)
        for e in range(2):
            ends[e, rows, :] = one_hot(picks[:, e : e + 1] == slot_lane)
        return carry

    lax.fori_loop(0, 4, mark, 0)

    r272 = iota((384, ATT), 0)
    c272 = iota((384, ATT), 1)
    place = one_hot(
        ((c272 < MEM) & (r272 == c272)) | ((c272 >= MEM) & (r272 == c272 + (256 - MEM)))
    )
    wkv[...] = jnp.zeros(wkv.shape, BF16)
    wkv[:, 0:ATT] = mm(place, w_key[...]).astype(BF16)
    wkv[:, 384 : 384 + ATT] = mm(place, w_value[...]).astype(BF16)
    wq[...] = jnp.zeros(wq.shape, BF16)
    wq[:, 0:ATT] = mm(place, w_query[...]).astype(BF16)
    r444 = iota((640, ATT + MEM), 0)
    c444 = iota((640, ATT + MEM), 1)
    place = one_hot(
        ((c444 < ATT) & (r444 == c444)) | ((c444 >= ATT) & (r444 == c444 + (384 - ATT)))
    )
    wm[...] = mm_nt(place, w_merge[...]).astype(BF16)

    widen = one_hot(iota((CAP, UNITS), 0) == iota((CAP, UNITS), 1))
    mem_b = memory[...].astype(BF16)
    gates = (
        w_input[0, :, 0:MEM] + w_hidden[0],
        w_input[1, :, 0:MEM] + w_hidden[1],
        w_input[2, :, 0:MEM],
        w_hidden[2],
    )
    for g, w in enumerate(gates):
        zed[g] = mm(mm(widen, w.astype(BF16)).astype(BF16), mem_b)
    own[...] = jnp.dot(
        jnp.where(
            (iota((CAP, MEM), 1) == iota((CAP, MEM), 0) + f * UNITS)
            & (iota((CAP, MEM), 0) < UNITS),
            1.0,
            0.0,
        ),
        memory[...],
        preferred_element_type=F32,
        precision=lax.Precision.HIGHEST,
    )

    edges = edge_recv[...].reshape(256, EV).astype(F32).T.astype(BF16)
    for e in range(2):
        msg[e * EV : (e + 1) * EV, 384:640] = edges
    ext_send[...] = jnp.zeros(ext_send.shape, F32)

    wait_bytes(req_recv.at[0:96], recv_req.at[1])
    for t in range(4):
        small[...] = jnp.zeros(small.shape, F32)
        small[0:32, :] = req_recv[t * 32 : t * 32 + 32].reshape(32, 128).astype(F32)
        asked_by[t] = small[...].T

    def claim(t, carry):
        for i in range(32):
            claims[t, i * CAP : (i + 1) * CAP, :] = one_hot(
                asked_by[t, 0:CAP, i : i + 1].astype(I32) == row_lane
            )
        return carry

    lax.fori_loop(0, 4, claim, 0)

    wait_bytes(fetched.at[0:31], recv_rows)
    table = fetched.reshape(SLOTS, 256)
    for e in range(2):
        src[e] = mm(ends[e], table[...])
    lane = iota((EV, 256), 1)
    counted = (lane == MEM + 2) | (lane == MEM + 3)
    for e in range(2):
        msg[e * EV : (e + 1) * EV, 0:256] = jnp.where(counted, 1.0, src[1 - e]).astype(BF16)
        stamp = src[e, :, MEM : MEM + 1] * 128.0 + src[e, :, MEM + 1 : MEM + 2]
        gap = cols[:, 32:33] - stamp
        msg[e * EV : (e + 1) * EV, 256:384] = cosine(gap * freq + phase).astype(BF16)

    wait_bytes(w_all.at[0:3, 0:544], recv_x.at[1])
    wait_bytes(wx_all.at[0:3], recv_x.at[2])
    rows4 = jnp.concatenate([wx_all[dx] for dx in range(4)] + [jnp.zeros((4, 640), F32)], axis=0)
    row = iota((8, 640), 0)
    counts = (row >= 4) & (row < 6) & (iota((8, 640), 1) == row + (MEM + 2 - 4))
    w_ext[...] = jnp.where(counts, 1.0, rows4).astype(BF16)

    lane = iota((384, 256), 1)
    for t in (2, 1, 3, 0):
        mask = jnp.concatenate(
            [
                one_hot(
                    iota((2 * CAP, 2 * EV), 0) + (at_y[dy] + at_z[(t - dy) % 4]) * CAP
                    == end_cols[...]
                )
                for dy in range(4)
            ],
            axis=0,
        )
        total = mm(mask, msg[...])
        first = total[:, 0:256]
        high = jnp.floor(first * (1.0 / 128.0))
        first = jnp.where(
            lane == MEM + 2, first - high * 128.0, jnp.where(lane == MEM + 3, high, first)
        )
        sums = jnp.concatenate([first, total[:, 256:640]], axis=1).astype(BF16)
        for pair in (1, 0):
            w_pair = jnp.concatenate([w_all[2 * pair], w_all[2 * pair + 1]], axis=1)
            out = mm(sums, w_pair).astype(BF16)
            for half in range(2):
                main_send[t, 2 * pair + half] = out[:, half * 128 : (half + 1) * 128].reshape(
                    8, CAP, 128
                )
            for i in (4, 2, 6, 0, 5, 3, 7, 1):
                for dx in (2 * pair, 2 * pair + 1):
                    if t == 0 and dx == 0 and i == 0:
                        continue
                    send(
                        main_send.at[t, dx, i // 2 * 2 + at_c[i % 2]],
                        main_recv.at[t, dx * 8 + i],
                        send_sem.at[5],
                        recv_main.at[t],
                        peer(t, i, dx),
                    )
        ext_tmp[0:8, :] = mm_nt(w_ext[...], sums)
        ext_tmp[8:9, :] = ext_tmp[4:5, :] + ext_tmp[5:6, :] * 128.0
        for j in range(8):
            count_row = ext_tmp[8:9, j * CAP : (j + 1) * CAP]
            for dx in range(4):
                ext_send[t, dx, j, :, 0:CAP] = ext_tmp[dx : dx + 1, j * CAP : (j + 1) * CAP]
                ext_send[t, dx, j, :, 64 : 64 + CAP] = count_row
        for i in (4, 2, 6, 0, 5, 3, 7, 1):
            for dx in (2, 3, 1, 0):
                if t == 0 and dx == 0 and i == 0:
                    continue
                send(
                    ext_send.at[t, dx, i // 2 * 2 + at_c[i % 2]],
                    ext_recv.at[t, dx * 8 + i],
                    send_sem.at[6],
                    recv_ext.at[t],
                    peer(t, i, dx),
                )
    main_recv[0, 0] = main_send[0, 0, at_c[0]]
    ext_recv[0, 0] = ext_send[0, 0, at_c[0]]

    still = jnp.broadcast_to(cosine(phase), (EV, 128)).astype(BF16)
    query[...] = (
        mm(src[0].astype(BF16), wq[0:256, :]) + mm(still, wq[256:384, :])
    ) * (1.0 / math.sqrt(HEAD))
    head_of = iota((EV, 384), 1) < HEAD
    for h in range(2):
        part = query[...]
        part = jnp.where(head_of, part, 0.0) if h == 0 else jnp.where(head_of, 0.0, part)
        coarse = part.astype(BF16)
        fine = (part - coarse.astype(F32)).astype(BF16)
        qk[h] = mm_nt(coarse, wkv[:, 0:384]) + mm_nt(fine, wkv[:, 0:384])

    def attend(b, carry):
        at = pl.multiple_of(b * 128, 128)
        near[...] = mm(hot[b], table[...]).reshape(K, 128, 256)

        def group(g, inner):
            r = pl.multiple_of(g * 16, 16)
            rows = pl.ds(at + r, 16)
            q0, q1 = qk[0, rows, :], qk[1, rows, :]
            s0, s1 = [], []
            for k in range(K):
                x, t = near[k, pl.ds(r, 16), :], times[k, rows, :]
                u0 = x * q0[:, 0:256]
                u1 = x * q1[:, 0:256]
                u0 = u0[:, 0:128] + u0[:, 128:256] + t * q0[:, 256:384]
                u1 = u1[:, 0:128] + u1[:, 128:256] + t * q1[:, 256:384]
                s0.append(jnp.sum(u0, axis=1, keepdims=True))
                s1.append(jnp.sum(u1, axis=1, keepdims=True))
            m0 = functools.reduce(jnp.maximum, s0)
            m1 = functools.reduce(jnp.maximum, s1)
            p0 = [jnp.exp(s - m0) for s in s0]
            p1 = [jnp.exp(s - m1) for s in s1]
            n0 = 1.0 / sum(p0)
            n1 = 1.0 / sum(p1)
            a0 = a1 = jnp.zeros((16, 256), F32)
            c0 = c1 = jnp.zeros((16, 128), F32)
            for k in range(K):
                x, t = near[k, pl.ds(r, 16), :], times[k, rows, :]
                a0 += p0[k] * x
                a1 += p1[k] * x
                c0 += p0[k] * t
                c1 += p1[k] * t
            mix[0, rows, 0:256] = a0 * n0
            mix[1, rows, 0:256] = a1 * n1
            mix[0, rows, 256:384] = c0 * n0
            mix[1, rows, 256:384] = c1 * n1
            return inner

        lax.fori_loop(0, 8, group, 0, unroll=2)
        return carry

    lax.fori_loop(0, 4, attend, 0)
    halves = []
    for h in range(2):
        part = mix[h]
        coarse = part.astype(BF16)
        fine = (part - coarse.astype(F32)).astype(BF16)
        halves.append(mm(coarse, wkv[:, 384:768]) + mm(fine, wkv[:, 384:768]))
    attended = jnp.where(head_of, halves[0], halves[1]).astype(BF16)
    hidden = mm(attended, wm[0:384, :]) + mm(src[0].astype(BF16), wm[384:640, :])
    hidden = jnp.maximum(hidden + vec[2:3, 0:EMB], 0.0).astype(BF16)
    embedding[...] = (mm(hidden, w_out[...]) + vec[3:4, 0:EMB]).T

    for t in (2, 1, 3, 0):
        first = 1 if t == 0 else 0
        wait_bytes(main_recv.at[t, first:32], recv_main.at[t])
        wait_bytes(ext_recv.at[t, first:32], recv_ext.at[t])
        for i in range(32):
            side[0:1, i * CAP : (i + 1) * CAP] = ext_recv[t, i, :, 0:CAP]
            side[1:2, i * CAP : (i + 1) * CAP] = ext_recv[t, i, :, 64 : 64 + CAP]
        count = side[1:2, :]
        high = jnp.floor(count * (1.0 / 128.0))
        row = iota((16, SLOTS), 0)
        rest = jnp.where(
            row == 0,
            side[0:1, :],
            jnp.where(row == 1, count - high * 128.0, jnp.where(row == 2, high, 0.0)),
        )
        left = jnp.concatenate(
            [main_recv[t].reshape(SLOTS, 128).T, rest.astype(BF16)], axis=0
        )
        total = mm(left, claims[t])
        if t == 2:
            acc[...] = total
        else:
            acc[...] += total

    small[...] = jnp.zeros(small.shape, F32)
    small[0:4, :] = vec[4:8, 0:128]
    bias = small[...].T
    b0, b1, b2, b3 = (bias[0:UNITS, g : g + 1] for g in range(4))
    heard = acc[129:130, :] + acc[130:131, :] * 128.0
    share = 1.0 / jnp.maximum(heard, 1.0)
    reset = jax.nn.sigmoid(acc[0:UNITS, :] * share + zed[0, 0:UNITS, :] + b0)
    update = jax.nn.sigmoid(acc[UNITS : 2 * UNITS, :] * share + zed[1, 0:UNITS, :] + b1)
    cand = jnp.tanh(
        acc[2 * UNITS : 3 * UNITS, :] * share
        + zed[2, 0:UNITS, :]
        + b2
        + reset * (zed[3, 0:UNITS, :] + b3)
    )
    mine = own[0:UNITS, :]
    fresh = (1.0 - update) * cand + update * mine
    new_memory[...] = jnp.where(heard > 0.0, fresh, mine)

    wait_bytes(req_recv.at[0:127], send_sem.at[0])
    wait_bytes(edge_recv.at[0:3], send_sem.at[1])
    wait_bytes(w_all.at[0:3, 0:544], send_sem.at[2])
    wait_bytes(wx_all.at[0:3], send_sem.at[3])
    wait_bytes(row_send.at[0:31], send_sem.at[4])
    wait_bytes(main_recv.at[0:3], send_sem.at[5])
    wait_bytes(main_recv.at[3, 0:31], send_sem.at[5])
    wait_bytes(ext_recv.at[0:3], send_sem.at[6])
    wait_bytes(ext_recv.at[3, 0:31], send_sem.at[6])


def step(
    memory,
    last_update,
    ev_time,
    nbr_gap,
    slot_rows,
    slot_ref,
    edge_feat,
    frequency,
    phase_shift,
    w_query,
    w_key,
    w_value,
    w_merge,
    b_merge,
    w_out,
    b_out,
    w_input,
    w_hidden,
    gru_bias,
):
    args = (
        memory.T,
        last_update.reshape(1, ROWS),
        ev_time.reshape(1, EV),
        nbr_gap.T,
        slot_rows,
        slot_ref.T,
        edge_feat.T,
        frequency.reshape(1, TIME),
        phase_shift.reshape(1, TIME),
        w_query,
        w_key,
        w_value,
        w_merge.T,
        b_merge.reshape(1, EMB),
        w_out,
        b_out.reshape(1, EMB),
        jnp.swapaxes(w_input, 1, 2),
        jnp.swapaxes(w_hidden, 1, 2),
        gru_bias,
    )
    vmem = pl.BlockSpec(memory_space=pltpu.VMEM)
    V, D = pltpu.VMEM, pltpu.SemaphoreType.DMA
    embedding, new_memory = pl.pallas_call(
        kernel,
        out_shape=(
            jax.ShapeDtypeStruct((EMB, EV), F32),
            jax.ShapeDtypeStruct((UNITS, ROWS), F32),
        ),
        in_specs=[pl.BlockSpec(memory_space=pl.ANY)] * len(args),
        out_specs=(vmem, vmem),
        scratch_shapes=[
            V((32, 1, 128), I32),
            V((128, 1, 128), I32),
            V((32, CAP, 256), BF16),
            V((32, CAP, 256), BF16),
            V((4, 64, EV), BF16),
            V((640, 128), BF16),
            V((1, 640), F32),
            V((4, 640, 128), BF16),
            V((4, 1, 640), F32),
            V((4, 4, 8, CAP, 128), BF16),
            V((4, 32, CAP, 128), BF16),
            V((4, 4, 8, 1, 128), F32),
            V((4, 32, 1, 128), F32),
            V((8, 256), F32),
            V((256, ROWS), F32),
            V((ROWS, 256), BF16),
            V((128, EV), F32),
            V((EV, 128), F32),
            V((128, 128), F32),
            V((K, EV, 128), F32),
            V((384, 768), BF16),
            V((384, 384), BF16),
            V((640, EMB), BF16),
            V((8, 640), BF16),
            V((4, CAP, ROWS), F32),
            V((CAP, ROWS), F32),
            V((1, 2 * EV), I32),
            V((2, EV, SLOTS), BF16),
            V((2, EV, 256), F32),
            V((2 * EV, 640), BF16),
            V((16, 384), F32),
            V((EV, 384), F32),
            V((4, K * 128, SLOTS), BF16),
            V((K, 128, 256), F32),
            V((2, EV, 384), F32),
            V((4, SLOTS, ROWS), BF16),
            V((4, 128, 128), F32),
            V((2, EV, 384), F32),
            V((8, SLOTS), F32),
            V((144, ROWS), F32),
            D((7,)),
            D((6,)),
            D,
            D((3,)),
            D((4,)),
            D((4,)),
            D((19,)),
        ]
        + [V(a.shape, a.dtype) for a in args],
        compiler_params=pltpu.CompilerParams(
            collective_id=0, has_side_effects=True, vmem_limit_bytes=60 * 1024 * 1024
        ),
    )(*args)
    return embedding.T.astype(BF16), new_memory.T


def solution(mesh):
    return jax.shard_map(
        step,
        mesh=mesh,
        in_specs=(
            P("node", None),
            P("node"),
            P(("node", "feat")),
            P(("node", "feat"), None),
            P(("node", "feat"), None),
            P(("node", "feat"), None),
            P("node", "feat"),
            P(),
            P(),
            P(),
            P(),
            P(),
            P(),
            P(),
            P(),
            P(),
            P(None, None, "feat"),
            P(None, None, "feat"),
            P(None, "feat"),
        ),
        out_specs=(P(("node", "feat"), None), P("node", "feat")),
        check_vma=False,
    )
```

```python
import functools
import math

import jax
import jax.numpy as jnp
from jax import lax
from jax.experimental import pallas as pl
from jax.experimental.pallas import tpu as pltpu
from jax.sharding import PartitionSpec as P

F32, BF16, I32 = jnp.float32, jnp.bfloat16, jnp.int32
MESH = pl.DeviceIdType.MESH
COS = (
    0.9999999998851011,
    -0.49999999850736465,
    0.041666663483369594,
    -0.0013888863001969808,
    2.4800551963260593e-05,
    -2.7534774132807624e-07,
    2.060335926598073e-09,
    -9.721760760713551e-12,
)
TURN_HI = 6.28125
TURN_LO = 2.0 * math.pi - TURN_HI

MEM, TIME, ATT, EMB, UNITS = 172, 100, 272, 172, 43
CAP, K, EV, ROWS, SLOTS = 48, 10, 512, 1024, 1536
HEAD = ATT // 2


def cosine(x):
    turns = jnp.floor(x * (0.5 / math.pi) + 0.5)
    r = (x - turns * TURN_HI) - turns * TURN_LO
    u = r * r
    total = jnp.full_like(u, COS[-1])
    for c in COS[-2::-1]:
        total = total * u + c
    return total


def mm(a, b):
    return jnp.dot(a, b, preferred_element_type=F32)


def mm_nt(a, b):
    return lax.dot_general(a, b, (((1,), (1,)), ((), ())), preferred_element_type=F32)


def iota(shape, dim):
    return lax.broadcasted_iota(I32, shape, dim)


def one_hot(mask):
    return jnp.where(mask, 1.0, 0.0).astype(BF16)


def kernel(*refs):
    given, refs = refs[:19], refs[19:]
    loaded, refs = refs[-19:], refs[:-19]
    (
        embedding,
        new_memory,
        req_send,
        req_recv,
        row_send,
        fetched,
        edge_recv,
        w_mine,
        wx_mine,
        w_all,
        wx_all,
        main_send,
        main_recv,
        ext_send,
        ext_recv,
        vec,
        mem_t,
        memb,
        wide_t,
        cols,
        small,
        times,
        wkv,
        wq,
        wm,
        w_ext,
        zed,
        own,
        end_cols,
        ends,
        src,
        msg,
        ext_tmp,
        query,
        hot,
        near,
        qk,
        claims,
        asked_by,
        bias,
        mix,
        side,
        acc,
        send_sem,
        recv_req,
        recv_rows,
        recv_x,
        recv_main,
        recv_ext,
        in_sem,
    ) = refs
    (
        memory,
        last_update,
        ev_time,
        nbr_gap,
        slot_rows,
        slot_ref,
        edge_feat,
        frequency,
        phase_shift,
        w_query,
        w_key,
        w_value,
        w_merge,
        b_merge,
        w_out,
        b_out,
        w_input,
        w_hidden,
        gru_bias,
    ) = loaded
    loads = [
        pltpu.make_async_copy(a, b, in_sem.at[i]) for i, (a, b) in enumerate(zip(given, loaded))
    ]
    n = lax.axis_index("node")
    f = lax.axis_index("feat")
    y, z, c = n // 8, (n // 2) % 4, n % 2
    at_y = [((y + d) % 4) * 8 for d in range(4)]
    at_z = [((z + d) % 4) * 2 for d in range(4)]
    at_c = [(c + d) % 2 for d in range(2)]
    at_f = [(f + d) % 4 for d in range(4)]
    def peer(t, i, dx):
        return at_y[i // 2] + at_z[(t - i // 2) % 4] + at_c[i % 2], at_f[dx]

    def send(src_ref, dst_ref, s_sem, r_sem, to):
        pltpu.make_async_remote_copy(
            src_ref=src_ref,
            dst_ref=dst_ref,
            send_sem=s_sem,
            recv_sem=r_sem,
            device_id=to,
            device_id_type=MESH,
        ).start()

    def wait_bytes(ref, sem):
        pltpu.make_async_copy(ref, ref, sem).wait()

    everyone = [(t, dx, i) for t in range(4) for dx in range(4) for i in range(8)][1:]

    for dx in range(4):
        w_all[dx, 176:256, :] = jnp.zeros((80, 128), BF16)
        w_all[dx, 368:384, :] = jnp.zeros((16, 128), BF16)

    barrier = pltpu.get_barrier_semaphore()
    near_by = [(t, dx, i) for t, dx, i in everyone if dx == 0 or (t == 0 and i == 0)]
    for t, dx, i in near_by:
        pl.semaphore_signal(
            barrier, inc=1, device_id=peer(t, i, dx), device_id_type=MESH
        )
    for first in (4, 0, 1, 6):
        loads[first].start()
    for i in range(19):
        if i not in (4, 0, 1, 6):
            loads[i].start()

    req_send[...] = jnp.full(req_send.shape, -1, I32)
    loads[4].wait()
    for o in range(32):
        req_send[o, :, 0:CAP] = slot_rows[:, o * CAP : (o + 1) * CAP]
    req_recv[0] = req_send[n]
    loads[6].wait()
    edge_recv[f] = edge_feat[:, pl.ds(pl.multiple_of(f * EV, EV), EV)]

    loads[0].wait()
    loads[1].wait()
    mem_t[0:MEM, :] = memory[...]
    stamp = last_update[...].astype(F32)
    high = jnp.floor(stamp * (1.0 / 128.0))
    mem_t[MEM : MEM + 1, :] = high
    mem_t[MEM + 1 : MEM + 2, :] = stamp - high * 128.0
    mem_t[MEM + 2 : 256, :] = jnp.zeros((256 - MEM - 2, ROWS), F32)
    for b in range(4):
        memb[b * 256 : (b + 1) * 256, :] = mem_t[:, b * 256 : (b + 1) * 256].T.astype(BF16)

    pl.semaphore_wait(barrier, len(near_by))

    for t, dx, i in everyone:
        if dx == 0:
            to = peer(t, i, 0)
            send(
                req_send.at[to[0]],
                req_recv.at[t * 32 + i],
                send_sem.at[0],
                recv_req.at[2 + t],
                to,
            )
    for dx in range(1, 4):
        to = peer(0, 0, dx)
        send(
            edge_feat.at[:, pl.ds(pl.multiple_of(to[1] * EV, EV), EV)],
            edge_recv.at[f],
            send_sem.at[1],
            recv_x.at[0],
            to,
        )

    loads[16].wait()
    r640 = iota((640, 700), 0)
    c640 = iota((640, 700), 1)
    place = one_hot(
        ((r640 < MEM) & (c640 == r640 + MEM))
        | ((r640 >= 256) & (r640 < 256 + TIME) & (c640 == r640 - 256 + 2 * MEM))
        | ((r640 >= 384) & (c640 == r640 - 384 + 2 * MEM + TIME))
    )
    rows43 = iota((128, UNITS), 0)
    cols43 = iota((128, UNITS), 1)
    wide = mm(one_hot(rows43 == cols43), w_input[0].astype(BF16))
    wide += mm(one_hot(rows43 == cols43 + UNITS), w_input[1].astype(BF16))
    wide += mm(one_hot(rows43 == cols43 + 2 * UNITS), w_input[2].astype(BF16))
    w_mine[...] = mm_nt(place, wide.astype(BF16)).astype(BF16)
    last = mm(one_hot(iota((8, UNITS), 1) == UNITS - 1), w_input[2].astype(BF16))
    wx_mine[...] = mm_nt(last.astype(BF16), place)[0:1, :]
    for dx in range(1, 4):
        to = peer(0, 0, 4 - dx)
        for rows in (slice(0, 176), slice(256, 368), slice(384, 640)):
            send(w_mine.at[rows], w_all.at[dx, rows], send_sem.at[2], recv_x.at[1], to)
        send(wx_mine, wx_all.at[dx], send_sem.at[3], recv_x.at[2], to)
    w_all[0] = w_mine[...]
    wx_all[0] = wx_mine[...]

    for i in (2, 3, 5, 7, 8, 9, 10, 11, 12, 13, 14, 15, 17, 18):
        loads[i].wait()
    vec[...] = jnp.zeros(vec.shape, F32)
    vec[0:1, 0:TIME] = frequency[...]
    vec[1:2, 0:TIME] = phase_shift[...]
    vec[2:3, 0:EMB] = b_merge[...]
    vec[3:4, 0:EMB] = b_out[...]
    vec[4:8, 0:UNITS] = gru_bias[...]
    freq = vec[0:1, 0:128]
    phase = vec[1:2, 0:128]

    wide_t[...] = jnp.zeros(wide_t.shape, F32)
    wide_t[0 : K + 2, :] = slot_ref[...].astype(F32)
    wide_t[16 : 16 + K, :] = nbr_gap[...].astype(F32)
    wide_t[32:33, :] = ev_time[...].astype(F32)
    cols[...] = wide_t[...].T
    end_cols[:, 0:EV] = slot_ref[0:1, :]
    end_cols[:, EV : 2 * EV] = slot_ref[1:2, :]

    for k in range(K):
        times[k] = cosine(cols[:, 16 + k : 17 + k] * freq + phase).astype(BF16).astype(F32)

    r272 = iota((384, ATT), 0)
    c272 = iota((384, ATT), 1)
    place = one_hot(
        ((c272 < MEM) & (r272 == c272)) | ((c272 >= MEM) & (r272 == c272 + (256 - MEM)))
    )
    wkv[...] = jnp.zeros(wkv.shape, BF16)
    wkv[:, 0:ATT] = mm(place, w_key[...]).astype(BF16)
    wkv[:, 384 : 384 + ATT] = mm(place, w_value[...]).astype(BF16)
    wq[...] = jnp.zeros(wq.shape, BF16)
    wq[:, 0:ATT] = mm(place, w_query[...]).astype(BF16)
    r444 = iota((640, ATT + MEM), 0)
    c444 = iota((640, ATT + MEM), 1)
    place = one_hot(
        ((c444 < ATT) & (r444 == c444)) | ((c444 >= ATT) & (r444 == c444 + (384 - ATT)))
    )
    wm[...] = mm_nt(place, w_merge[...]).astype(BF16)

    widen = one_hot(iota((CAP, UNITS), 0) == iota((CAP, UNITS), 1))
    mem_b = memory[...].astype(BF16)
    gates = (
        w_input[0, :, 0:MEM] + w_hidden[0],
        w_input[1, :, 0:MEM] + w_hidden[1],
        w_input[2, :, 0:MEM],
        w_hidden[2],
    )
    for g, w in enumerate(gates):
        zed[g] = mm(mm(widen, w.astype(BF16)).astype(BF16), mem_b)
    own[...] = jnp.dot(
        jnp.where(
            (iota((CAP, MEM), 1) == iota((CAP, MEM), 0) + f * UNITS)
            & (iota((CAP, MEM), 0) < UNITS),
            1.0,
            0.0,
        ),
        memory[...],
        preferred_element_type=F32,
        precision=lax.Precision.HIGHEST,
    )

    for t in range(4):
        first = 1 if t == 0 else 0
        wait_bytes(req_recv.at[t * 32 + first : t * 32 + 8], recv_req.at[2 + t])
    small[...] = jnp.zeros(small.shape, F32)
    for t in range(4):
        small[8 * t : 8 * t + 8, :] = req_recv[t * 32 : t * 32 + 8].reshape(8, 128).astype(F32)
    asked = small[...].T.astype(I32)
    row_lane = iota((CAP, ROWS), 1)
    for t in (2, 1, 3, 0):
        mask = jnp.concatenate(
            [
                one_hot(asked[0:CAP, 8 * t + i : 8 * t + i + 1] == row_lane)
                for i in range(8)
            ],
            axis=0,
        )
        rows = mm(mask, memb[...]).astype(BF16)
        for i in range(8):
            if t == 0 and i == 0:
                fetched[n] = rows[0:CAP, :]
            else:
                row_send[t * 8 + i] = rows[i * CAP : (i + 1) * CAP, :]
        for i in (4, 2, 6, 0, 5, 3, 7, 1):
            if t == 0 and i == 0:
                continue
            send(
                row_send.at[t * 8 + i],
                fetched.at[n],
                send_sem.at[4],
                recv_rows,
                peer((4 - t) % 4, (4 - i // 2) % 4 * 2 + i % 2, 0),
            )

    wait_bytes(edge_recv.at[0:3], recv_x.at[0])
    for t, dx, i in everyone:
        if dx != 0:
            to = peer(t, i, dx)
            send(
                req_send.at[to[0]],
                req_recv.at[t * 32 + dx * 8 + i],
                send_sem.at[0],
                recv_req.at[1],
                to,
            )

    slot_lane = iota((128, SLOTS), 1)

    def mark(b, carry):
        rows = pl.ds(pl.multiple_of(b * 128, 128), 128)
        picks = cols[rows, :].astype(I32)
        for k in range(K):
            hot[b, k * 128 : (k + 1) * 128, :] = one_hot(picks[:, 2 + k : 3 + k] == slot_lane)
        for e in range(2):
            ends[e, rows, :] = one_hot(picks[:, e : e + 1] == slot_lane)
        return carry

    lax.fori_loop(0, 4, mark, 0)

    edges = edge_recv[...].reshape(256, EV).astype(F32).T.astype(BF16)
    for e in range(2):
        msg[e * EV : (e + 1) * EV, 384:640] = edges
    ext_send[...] = jnp.zeros(ext_send.shape, F32)

    wait_bytes(req_recv.at[0:96], recv_req.at[1])
    small[...] = jnp.zeros(small.shape, F32)
    small[0:4, :] = vec[4:8, 0:128]
    bias[...] = small[...].T
    for t in range(4):
        small[...] = jnp.zeros(small.shape, F32)
        small[0:32, :] = req_recv[t * 32 : t * 32 + 32].reshape(32, 128).astype(F32)
        asked_by[t] = small[...].T

    def claim(t, carry):
        for i in range(32):
            claims[t, i * CAP : (i + 1) * CAP, :] = one_hot(
                asked_by[t, 0:CAP, i : i + 1].astype(I32) == row_lane
            )
        return carry

    lax.fori_loop(0, 4, claim, 0)

    wait_bytes(fetched.at[0:31], recv_rows)
    table = fetched.reshape(SLOTS, 256)
    for e in range(2):
        src[e] = mm(ends[e], table[...])
    lane = iota((EV, 256), 1)
    counted = (lane == MEM + 2) | (lane == MEM + 3)
    for e in range(2):
        msg[e * EV : (e + 1) * EV, 0:256] = jnp.where(counted, 1.0, src[1 - e]).astype(BF16)
        stamp = src[e, :, MEM : MEM + 1] * 128.0 + src[e, :, MEM + 1 : MEM + 2]
        gap = cols[:, 32:33] - stamp
        msg[e * EV : (e + 1) * EV, 256:384] = cosine(gap * freq + phase).astype(BF16)

    wait_bytes(w_all.at[0:3, 0:544], recv_x.at[1])
    wait_bytes(wx_all.at[0:3], recv_x.at[2])
    rows4 = jnp.concatenate([wx_all[dx] for dx in range(4)] + [jnp.zeros((4, 640), F32)], axis=0)
    row = iota((8, 640), 0)
    counts = (row >= 4) & (row < 6) & (iota((8, 640), 1) == row + (MEM + 2 - 4))
    w_ext[...] = jnp.where(counts, 1.0, rows4).astype(BF16)

    lane = iota((384, 256), 1)
    for t in (2, 1, 3, 0):
        mask = jnp.concatenate(
            [
                one_hot(
                    iota((2 * CAP, 2 * EV), 0) + (at_y[dy] + at_z[(t - dy) % 4]) * CAP
                    == end_cols[...]
                )
                for dy in range(4)
            ],
            axis=0,
        )
        total = mm(mask, msg[...])
        first = total[:, 0:256]
        high = jnp.floor(first * (1.0 / 128.0))
        first = jnp.where(
            lane == MEM + 2, first - high * 128.0, jnp.where(lane == MEM + 3, high, first)
        )
        sums = jnp.concatenate([first, total[:, 256:640]], axis=1).astype(BF16)
        for pair in range(2):
            w_pair = jnp.concatenate([w_all[2 * pair], w_all[2 * pair + 1]], axis=1)
            out = mm(sums, w_pair).astype(BF16)
            for i in range(2):
                main_send[t, 2 * pair + i] = out[:, i * 128 : (i + 1) * 128].reshape(8, CAP, 128)
        ext_tmp[0:8, :] = mm_nt(w_ext[...], sums)
        ext_tmp[8:9, :] = ext_tmp[4:5, :] + ext_tmp[5:6, :] * 128.0
        for j in range(8):
            count_row = ext_tmp[8:9, j * CAP : (j + 1) * CAP]
            for dx in range(4):
                ext_send[t, dx, j, :, 0:CAP] = ext_tmp[dx : dx + 1, j * CAP : (j + 1) * CAP]
                ext_send[t, dx, j, :, 64 : 64 + CAP] = count_row
        for i in (4, 2, 6, 0, 5, 3, 7, 1):
            for dx in (2, 1, 3, 0):
                if t == 0 and dx == 0 and i == 0:
                    continue
                to = peer(t, i, dx)
                at = i // 2 * 2 + at_c[i % 2]
                send(
                    main_send.at[t, dx, at],
                    main_recv.at[t, dx * 8 + i],
                    send_sem.at[5],
                    recv_main.at[t],
                    to,
                )
                send(
                    ext_send.at[t, dx, at],
                    ext_recv.at[t, dx * 8 + i],
                    send_sem.at[6],
                    recv_ext.at[t],
                    to,
                )
    main_recv[0, 0] = main_send[0, 0, at_c[0]]
    ext_recv[0, 0] = ext_send[0, 0, at_c[0]]

    still = jnp.broadcast_to(cosine(phase), (EV, 128)).astype(BF16)
    query[...] = (
        mm(src[0].astype(BF16), wq[0:256, :]) + mm(still, wq[256:384, :])
    ) * (1.0 / math.sqrt(HEAD))
    head_of = iota((EV, 384), 1) < HEAD
    for h in range(2):
        part = query[...]
        part = jnp.where(head_of, part, 0.0) if h == 0 else jnp.where(head_of, 0.0, part)
        coarse = part.astype(BF16)
        fine = (part - coarse.astype(F32)).astype(BF16)
        qk[h] = mm_nt(coarse, wkv[:, 0:384]) + mm_nt(fine, wkv[:, 0:384])

    def attend(b, carry):
        at = pl.multiple_of(b * 128, 128)
        near[...] = mm(hot[b], table[...]).reshape(K, 128, 256)

        def group(g, inner):
            r = pl.multiple_of(g * 16, 16)
            rows = pl.ds(at + r, 16)
            q0, q1 = qk[0, rows, :], qk[1, rows, :]
            s0, s1 = [], []
            for k in range(K):
                x, t = near[k, pl.ds(r, 16), :], times[k, rows, :]
                u0 = x * q0[:, 0:256]
                u1 = x * q1[:, 0:256]
                u0 = u0[:, 0:128] + u0[:, 128:256] + t * q0[:, 256:384]
                u1 = u1[:, 0:128] + u1[:, 128:256] + t * q1[:, 256:384]
                s0.append(jnp.sum(u0, axis=1, keepdims=True))
                s1.append(jnp.sum(u1, axis=1, keepdims=True))
            m0 = functools.reduce(jnp.maximum, s0)
            m1 = functools.reduce(jnp.maximum, s1)
            p0 = [jnp.exp(s - m0) for s in s0]
            p1 = [jnp.exp(s - m1) for s in s1]
            n0 = 1.0 / sum(p0)
            n1 = 1.0 / sum(p1)
            a0 = a1 = jnp.zeros((16, 256), F32)
            c0 = c1 = jnp.zeros((16, 128), F32)
            for k in range(K):
                x, t = near[k, pl.ds(r, 16), :], times[k, rows, :]
                a0 += p0[k] * x
                a1 += p1[k] * x
                c0 += p0[k] * t
                c1 += p1[k] * t
            mix[0, rows, 0:256] = a0 * n0
            mix[1, rows, 0:256] = a1 * n1
            mix[0, rows, 256:384] = c0 * n0
            mix[1, rows, 256:384] = c1 * n1
            return inner

        lax.fori_loop(0, 8, group, 0, unroll=4)
        return carry

    lax.fori_loop(0, 4, attend, 0)
    halves = []
    for h in range(2):
        part = mix[h]
        coarse = part.astype(BF16)
        fine = (part - coarse.astype(F32)).astype(BF16)
        halves.append(mm(coarse, wkv[:, 384:768]) + mm(fine, wkv[:, 384:768]))
    attended = jnp.where(head_of, halves[0], halves[1]).astype(BF16)
    hidden = mm(attended, wm[0:384, :]) + mm(src[0].astype(BF16), wm[384:640, :])
    hidden = jnp.maximum(hidden + vec[2:3, 0:EMB], 0.0).astype(BF16)
    embedding[...] = (mm(hidden, w_out[...]) + vec[3:4, 0:EMB]).T.astype(BF16)

    for t in (2, 1, 3, 0):
        first = 1 if t == 0 else 0
        wait_bytes(main_recv.at[t, first:32], recv_main.at[t])
        wait_bytes(ext_recv.at[t, first:32], recv_ext.at[t])
        for i in range(32):
            side[0:1, i * CAP : (i + 1) * CAP] = ext_recv[t, i, :, 0:CAP]
            side[1:2, i * CAP : (i + 1) * CAP] = ext_recv[t, i, :, 64 : 64 + CAP]
        count = side[1:2, :]
        high = jnp.floor(count * (1.0 / 128.0))
        row = iota((16, SLOTS), 0)
        rest = jnp.where(
            row == 0,
            side[0:1, :],
            jnp.where(row == 1, count - high * 128.0, jnp.where(row == 2, high, 0.0)),
        )
        left = jnp.concatenate(
            [main_recv[t].reshape(SLOTS, 128).T, rest.astype(BF16)], axis=0
        )
        total = mm(left, claims[t])
        if t == 2:
            acc[...] = total
        else:
            acc[...] += total

    b0, b1, b2, b3 = (bias[0:UNITS, g : g + 1] for g in range(4))
    heard = acc[129:130, :] + acc[130:131, :] * 128.0
    share = 1.0 / jnp.maximum(heard, 1.0)
    reset = jax.nn.sigmoid(acc[0:UNITS, :] * share + zed[0, 0:UNITS, :] + b0)
    update = jax.nn.sigmoid(acc[UNITS : 2 * UNITS, :] * share + zed[1, 0:UNITS, :] + b1)
    cand = jnp.tanh(
        acc[2 * UNITS : 3 * UNITS, :] * share
        + zed[2, 0:UNITS, :]
        + b2
        + reset * (zed[3, 0:UNITS, :] + b3)
    )
    mine = own[0:UNITS, :]
    fresh = (1.0 - update) * cand + update * mine
    new_memory[...] = jnp.where(heard > 0.0, fresh, mine)

    wait_bytes(req_recv.at[0:127], send_sem.at[0])
    wait_bytes(edge_recv.at[0:3], send_sem.at[1])
    wait_bytes(w_all.at[0:3, 0:544], send_sem.at[2])
    wait_bytes(wx_all.at[0:3], send_sem.at[3])
    wait_bytes(row_send.at[0:31], send_sem.at[4])
    wait_bytes(main_recv.at[0:3], send_sem.at[5])
    wait_bytes(main_recv.at[3, 0:31], send_sem.at[5])
    wait_bytes(ext_recv.at[0:3], send_sem.at[6])
    wait_bytes(ext_recv.at[3, 0:31], send_sem.at[6])


def step(
    memory,
    last_update,
    ev_time,
    nbr_gap,
    slot_rows,
    slot_ref,
    edge_feat,
    frequency,
    phase_shift,
    w_query,
    w_key,
    w_value,
    w_merge,
    b_merge,
    w_out,
    b_out,
    w_input,
    w_hidden,
    gru_bias,
):
    args = (
        memory.T,
        last_update.reshape(1, ROWS),
        ev_time.reshape(1, EV),
        nbr_gap.T,
        slot_rows,
        slot_ref.T,
        edge_feat.T,
        frequency.reshape(1, TIME),
        phase_shift.reshape(1, TIME),
        w_query,
        w_key,
        w_value,
        w_merge.T,
        b_merge.reshape(1, EMB),
        w_out,
        b_out.reshape(1, EMB),
        jnp.swapaxes(w_input, 1, 2),
        jnp.swapaxes(w_hidden, 1, 2),
        gru_bias,
    )
    vmem = pl.BlockSpec(memory_space=pltpu.VMEM)
    V, D = pltpu.VMEM, pltpu.SemaphoreType.DMA
    embedding, new_memory = pl.pallas_call(
        kernel,
        out_shape=(
            jax.ShapeDtypeStruct((EMB, EV), BF16),
            jax.ShapeDtypeStruct((UNITS, ROWS), F32),
        ),
        in_specs=[pl.BlockSpec(memory_space=pl.ANY)] * len(args),
        out_specs=(vmem, vmem),
        scratch_shapes=[
            V((32, 1, 128), I32),
            V((128, 1, 128), I32),
            V((32, CAP, 256), BF16),
            V((32, CAP, 256), BF16),
            V((4, 64, EV), BF16),
            V((640, 128), BF16),
            V((1, 640), F32),
            V((4, 640, 128), BF16),
            V((4, 1, 640), F32),
            V((4, 4, 8, CAP, 128), BF16),
            V((4, 32, CAP, 128), BF16),
            V((4, 4, 8, 1, 128), F32),
            V((4, 32, 1, 128), F32),
            V((8, 256), F32),
            V((256, ROWS), F32),
            V((ROWS, 256), BF16),
            V((128, EV), F32),
            V((EV, 128), F32),
            V((128, 128), F32),
            V((K, EV, 128), F32),
            V((384, 768), BF16),
            V((384, 384), BF16),
            V((640, EMB), BF16),
            V((8, 640), BF16),
            V((4, CAP, ROWS), F32),
            V((CAP, ROWS), F32),
            V((1, 2 * EV), I32),
            V((2, EV, SLOTS), BF16),
            V((2, EV, 256), F32),
            V((2 * EV, 640), BF16),
            V((16, 384), F32),
            V((EV, 384), F32),
            V((4, K * 128, SLOTS), BF16),
            V((K, 128, 256), F32),
            V((2, EV, 384), F32),
            V((4, SLOTS, ROWS), BF16),
            V((4, 128, 128), F32),
            V((128, 128), F32),
            V((2, EV, 384), F32),
            V((8, SLOTS), F32),
            V((144, ROWS), F32),
            D((7,)),
            D((6,)),
            D,
            D((3,)),
            D((4,)),
            D((4,)),
            D((19,)),
        ]
        + [V(a.shape, a.dtype) for a in args],
        compiler_params=pltpu.CompilerParams(
            collective_id=0, has_side_effects=True, vmem_limit_bytes=60 * 1024 * 1024
        ),
    )(*args)
    return embedding.T, new_memory.T


def solution(mesh):
    return jax.shard_map(
        step,
        mesh=mesh,
        in_specs=(
            P("node", None),
            P("node"),
            P(("node", "feat")),
            P(("node", "feat"), None),
            P(("node", "feat"), None),
            P(("node", "feat"), None),
            P("node", "feat"),
            P(),
            P(),
            P(),
            P(),
            P(),
            P(),
            P(),
            P(),
            P(),
            P(None, None, "feat"),
            P(None, None, "feat"),
            P(None, "feat"),
        ),
        out_specs=(P(("node", "feat"), None), P("node", "feat")),
        check_vma=False,
    )
```

```python
import functools
import math

import jax
import jax.numpy as jnp
from jax import lax
from jax.experimental import pallas as pl
from jax.experimental.pallas import tpu as pltpu
from jax.sharding import PartitionSpec as P

F32, BF16, I32 = jnp.float32, jnp.bfloat16, jnp.int32
MESH = pl.DeviceIdType.MESH
COS = (
    0.9999999998851011,
    -0.49999999850736465,
    0.041666663483369594,
    -0.0013888863001969808,
    2.4800551963260593e-05,
    -2.7534774132807624e-07,
    2.060335926598073e-09,
    -9.721760760713551e-12,
)
TURN_HI = 6.28125
TURN_LO = 2.0 * math.pi - TURN_HI

MEM, TIME, ATT, EMB, UNITS = 172, 100, 272, 172, 43
CAP, K, EV, ROWS, SLOTS = 48, 10, 512, 1024, 1536
HEAD = ATT // 2


def cosine(x):
    turns = jnp.floor(x * (0.5 / math.pi) + 0.5)
    r = (x - turns * TURN_HI) - turns * TURN_LO
    u = r * r
    total = jnp.full_like(u, COS[-1])
    for c in COS[-2::-1]:
        total = total * u + c
    return total


def mm(a, b):
    return jnp.dot(a, b, preferred_element_type=F32)


def mm_nt(a, b):
    return lax.dot_general(a, b, (((1,), (1,)), ((), ())), preferred_element_type=F32)


def iota(shape, dim):
    return lax.broadcasted_iota(I32, shape, dim)


def one_hot(mask):
    return jnp.where(mask, 1.0, 0.0).astype(BF16)


def kernel(*refs):
    given, refs = refs[:19], refs[19:]
    loaded, refs = refs[-19:], refs[:-19]
    (
        embedding,
        new_memory,
        req_send,
        req_recv,
        row_send,
        fetched,
        edge_recv,
        w_mine,
        wx_mine,
        w_all,
        wx_all,
        main_send,
        main_recv,
        ext_send,
        ext_recv,
        vec,
        mem_t,
        memb,
        wide_t,
        cols,
        small,
        times,
        wkv,
        wq,
        wm,
        w_ext,
        zed,
        own,
        end_cols,
        ends,
        src,
        msg,
        ext_tmp,
        query,
        hot,
        near,
        qk,
        claims,
        asked_by,
        bias,
        mix,
        side,
        acc,
        send_sem,
        recv_req,
        recv_rows,
        recv_x,
        recv_main,
        recv_ext,
        in_sem,
    ) = refs
    (
        memory,
        last_update,
        ev_time,
        nbr_gap,
        slot_rows,
        slot_ref,
        edge_feat,
        frequency,
        phase_shift,
        w_query,
        w_key,
        w_value,
        w_merge,
        b_merge,
        w_out,
        b_out,
        w_input,
        w_hidden,
        gru_bias,
    ) = loaded
    loads = [
        pltpu.make_async_copy(a, b, in_sem.at[i]) for i, (a, b) in enumerate(zip(given, loaded))
    ]
    n = lax.axis_index("node")
    f = lax.axis_index("feat")
    y, z, c = n // 8, (n // 2) % 4, n % 2
    at_y = [((y + d) % 4) * 8 for d in range(4)]
    at_z = [((z + d) % 4) * 2 for d in range(4)]
    at_c = [(c + d) % 2 for d in range(2)]
    at_f = [(f + d) % 4 for d in range(4)]
    def peer(t, i, dx):
        return at_y[i // 2] + at_z[(t - i // 2) % 4] + at_c[i % 2], at_f[dx]

    def send(src_ref, dst_ref, s_sem, r_sem, to):
        pltpu.make_async_remote_copy(
            src_ref=src_ref,
            dst_ref=dst_ref,
            send_sem=s_sem,
            recv_sem=r_sem,
            device_id=to,
            device_id_type=MESH,
        ).start()

    def wait_bytes(ref, sem):
        pltpu.make_async_copy(ref, ref, sem).wait()

    everyone = [(t, dx, i) for t in range(4) for dx in range(4) for i in range(8)][1:]

    def hops(pair):
        t, dx, i = pair
        return sum(min(d, 4 - d) for d in (i // 2, (t - i // 2) % 4, dx))

    everyone.sort(key=hops, reverse=True)

    for dx in range(4):
        w_all[dx, 176:256, :] = jnp.zeros((80, 128), BF16)
        w_all[dx, 368:384, :] = jnp.zeros((16, 128), BF16)

    barrier = pltpu.get_barrier_semaphore()
    near_by = [(t, dx, i) for t, dx, i in everyone if dx == 0 or (t == 0 and i == 0)]
    for t, dx, i in near_by:
        pl.semaphore_signal(
            barrier, inc=1, device_id=peer(t, i, dx), device_id_type=MESH
        )
    for first in (4, 0, 1, 6):
        loads[first].start()
    for i in range(19):
        if i not in (4, 0, 1, 6):
            loads[i].start()

    req_send[...] = jnp.full(req_send.shape, -1, I32)
    loads[4].wait()
    for o in range(32):
        req_send[o, :, 0:CAP] = slot_rows[:, o * CAP : (o + 1) * CAP]
    req_recv[0] = req_send[n]
    loads[6].wait()
    edge_recv[f] = edge_feat[:, pl.ds(pl.multiple_of(f * EV, EV), EV)]

    loads[0].wait()
    loads[1].wait()
    mem_t[0:MEM, :] = memory[...]
    stamp = last_update[...].astype(F32)
    high = jnp.floor(stamp * (1.0 / 128.0))
    mem_t[MEM : MEM + 1, :] = high
    mem_t[MEM + 1 : MEM + 2, :] = stamp - high * 128.0
    mem_t[MEM + 2 : 256, :] = jnp.zeros((256 - MEM - 2, ROWS), F32)
    for b in range(4):
        memb[b * 256 : (b + 1) * 256, :] = mem_t[:, b * 256 : (b + 1) * 256].T.astype(BF16)

    pl.semaphore_wait(barrier, len(near_by))

    for t, dx, i in everyone:
        if dx == 0:
            to = peer(t, i, 0)
            send(
                req_send.at[to[0]],
                req_recv.at[t * 32 + i],
                send_sem.at[0],
                recv_req.at[2 + t],
                to,
            )
    for dx in range(1, 4):
        to = peer(0, 0, dx)
        send(
            edge_feat.at[:, pl.ds(pl.multiple_of(to[1] * EV, EV), EV)],
            edge_recv.at[f],
            send_sem.at[1],
            recv_x.at[0],
            to,
        )

    loads[16].wait()
    r640 = iota((640, 700), 0)
    c640 = iota((640, 700), 1)
    place = one_hot(
        ((r640 < MEM) & (c640 == r640 + MEM))
        | ((r640 >= 256) & (r640 < 256 + TIME) & (c640 == r640 - 256 + 2 * MEM))
        | ((r640 >= 384) & (c640 == r640 - 384 + 2 * MEM + TIME))
    )
    rows43 = iota((128, UNITS), 0)
    cols43 = iota((128, UNITS), 1)
    wide = mm(one_hot(rows43 == cols43), w_input[0].astype(BF16))
    wide += mm(one_hot(rows43 == cols43 + UNITS), w_input[1].astype(BF16))
    wide += mm(one_hot(rows43 == cols43 + 2 * UNITS), w_input[2].astype(BF16))
    w_mine[...] = mm_nt(place, wide.astype(BF16)).astype(BF16)
    last = mm(one_hot(iota((8, UNITS), 1) == UNITS - 1), w_input[2].astype(BF16))
    wx_mine[...] = mm_nt(last.astype(BF16), place)[0:1, :]
    for dx in range(1, 4):
        to = peer(0, 0, 4 - dx)
        for rows in (slice(0, 176), slice(256, 368), slice(384, 640)):
            send(w_mine.at[rows], w_all.at[dx, rows], send_sem.at[2], recv_x.at[1], to)
        send(wx_mine, wx_all.at[dx], send_sem.at[3], recv_x.at[2], to)
    w_all[0] = w_mine[...]
    wx_all[0] = wx_mine[...]

    for i in (2, 3, 5, 7, 8, 9, 10, 11, 12, 13, 14, 15, 17, 18):
        loads[i].wait()
    vec[...] = jnp.zeros(vec.shape, F32)
    vec[0:1, 0:TIME] = frequency[...]
    vec[1:2, 0:TIME] = phase_shift[...]
    vec[2:3, 0:EMB] = b_merge[...]
    vec[3:4, 0:EMB] = b_out[...]
    vec[4:8, 0:UNITS] = gru_bias[...]
    freq = vec[0:1, 0:128]
    phase = vec[1:2, 0:128]

    wide_t[...] = jnp.zeros(wide_t.shape, F32)
    wide_t[0 : K + 2, :] = slot_ref[...].astype(F32)
    wide_t[16 : 16 + K, :] = nbr_gap[...].astype(F32)
    wide_t[32:33, :] = ev_time[...].astype(F32)
    cols[...] = wide_t[...].T
    end_cols[:, 0:EV] = slot_ref[0:1, :]
    end_cols[:, EV : 2 * EV] = slot_ref[1:2, :]

    for k in range(K):
        times[k] = cosine(cols[:, 16 + k : 17 + k] * freq + phase).astype(BF16).astype(F32)

    r272 = iota((384, ATT), 0)
    c272 = iota((384, ATT), 1)
    place = one_hot(
        ((c272 < MEM) & (r272 == c272)) | ((c272 >= MEM) & (r272 == c272 + (256 - MEM)))
    )
    wkv[...] = jnp.zeros(wkv.shape, BF16)
    wkv[:, 0:ATT] = mm(place, w_key[...]).astype(BF16)
    wkv[:, 384 : 384 + ATT] = mm(place, w_value[...]).astype(BF16)
    wq[...] = jnp.zeros(wq.shape, BF16)
    wq[:, 0:ATT] = mm(place, w_query[...]).astype(BF16)
    r444 = iota((640, ATT + MEM), 0)
    c444 = iota((640, ATT + MEM), 1)
    place = one_hot(
        ((c444 < ATT) & (r444 == c444)) | ((c444 >= ATT) & (r444 == c444 + (384 - ATT)))
    )
    wm[...] = mm_nt(place, w_merge[...]).astype(BF16)

    widen = one_hot(iota((CAP, UNITS), 0) == iota((CAP, UNITS), 1))
    mem_b = memory[...].astype(BF16)
    gates = (
        w_input[0, :, 0:MEM] + w_hidden[0],
        w_input[1, :, 0:MEM] + w_hidden[1],
        w_input[2, :, 0:MEM],
        w_hidden[2],
    )
    for g, w in enumerate(gates):
        zed[g] = mm(mm(widen, w.astype(BF16)).astype(BF16), mem_b)
    own[...] = jnp.dot(
        jnp.where(
            (iota((CAP, MEM), 1) == iota((CAP, MEM), 0) + f * UNITS)
            & (iota((CAP, MEM), 0) < UNITS),
            1.0,
            0.0,
        ),
        memory[...],
        preferred_element_type=F32,
        precision=lax.Precision.HIGHEST,
    )

    for t in range(4):
        first = 1 if t == 0 else 0
        wait_bytes(req_recv.at[t * 32 + first : t * 32 + 8], recv_req.at[2 + t])
    small[...] = jnp.zeros(small.shape, F32)
    for t in range(4):
        small[8 * t : 8 * t + 8, :] = req_recv[t * 32 : t * 32 + 8].reshape(8, 128).astype(F32)
    asked = small[...].T.astype(I32)
    row_lane = iota((CAP, ROWS), 1)
    for t in (2, 1, 3, 0):
        mask = jnp.concatenate(
            [
                one_hot(asked[0:CAP, 8 * t + i : 8 * t + i + 1] == row_lane)
                for i in range(8)
            ],
            axis=0,
        )
        rows = mm(mask, memb[...]).astype(BF16)
        for i in range(8):
            if t == 0 and i == 0:
                fetched[n] = rows[0:CAP, :]
            else:
                row_send[t * 8 + i] = rows[i * CAP : (i + 1) * CAP, :]
        for i in (4, 2, 6, 0, 5, 3, 7, 1):
            if t == 0 and i == 0:
                continue
            send(
                row_send.at[t * 8 + i],
                fetched.at[n],
                send_sem.at[4],
                recv_rows,
                peer((4 - t) % 4, (4 - i // 2) % 4 * 2 + i % 2, 0),
            )

    wait_bytes(edge_recv.at[0:3], recv_x.at[0])
    for t, dx, i in everyone:
        if dx != 0:
            to = peer(t, i, dx)
            send(
                req_send.at[to[0]],
                req_recv.at[t * 32 + dx * 8 + i],
                send_sem.at[0],
                recv_req.at[1],
                to,
            )

    slot_lane = iota((128, SLOTS), 1)

    def mark(b, carry):
        rows = pl.ds(pl.multiple_of(b * 128, 128), 128)
        picks = cols[rows, :].astype(I32)
        for k in range(K):
            hot[b, k * 128 : (k + 1) * 128, :] = one_hot(picks[:, 2 + k : 3 + k] == slot_lane)
        for e in range(2):
            ends[e, rows, :] = one_hot(picks[:, e : e + 1] == slot_lane)
        return carry

    lax.fori_loop(0, 4, mark, 0)

    edges = edge_recv[...].reshape(256, EV).astype(F32).T.astype(BF16)
    for e in range(2):
        msg[e * EV : (e + 1) * EV, 384:640] = edges
    ext_send[...] = jnp.zeros(ext_send.shape, F32)

    wait_bytes(req_recv.at[0:96], recv_req.at[1])
    small[...] = jnp.zeros(small.shape, F32)
    small[0:4, :] = vec[4:8, 0:128]
    bias[...] = small[...].T
    for t in range(4):
        small[...] = jnp.zeros(small.shape, F32)
        small[0:32, :] = req_recv[t * 32 : t * 32 + 32].reshape(32, 128).astype(F32)
        asked_by[t] = small[...].T

    def claim(t, carry):
        for i in range(32):
            claims[t, i * CAP : (i + 1) * CAP, :] = one_hot(
                asked_by[t, 0:CAP, i : i + 1].astype(I32) == row_lane
            )
        return carry

    lax.fori_loop(0, 4, claim, 0)

    wait_bytes(fetched.at[0:31], recv_rows)
    table = fetched.reshape(SLOTS, 256)
    for e in range(2):
        src[e] = mm(ends[e], table[...])
    lane = iota((EV, 256), 1)
    counted = (lane == MEM + 2) | (lane == MEM + 3)
    for e in range(2):
        msg[e * EV : (e + 1) * EV, 0:256] = jnp.where(counted, 1.0, src[1 - e]).astype(BF16)
        stamp = src[e, :, MEM : MEM + 1] * 128.0 + src[e, :, MEM + 1 : MEM + 2]
        gap = cols[:, 32:33] - stamp
        msg[e * EV : (e + 1) * EV, 256:384] = cosine(gap * freq + phase).astype(BF16)

    wait_bytes(w_all.at[0:3, 0:544], recv_x.at[1])
    wait_bytes(wx_all.at[0:3], recv_x.at[2])
    rows4 = jnp.concatenate([wx_all[dx] for dx in range(4)] + [jnp.zeros((4, 640), F32)], axis=0)
    row = iota((8, 640), 0)
    counts = (row >= 4) & (row < 6) & (iota((8, 640), 1) == row + (MEM + 2 - 4))
    w_ext[...] = jnp.where(counts, 1.0, rows4).astype(BF16)

    lane = iota((384, 256), 1)
    for t in (2, 1, 3, 0):
        mask = jnp.concatenate(
            [
                one_hot(
                    iota((2 * CAP, 2 * EV), 0) + (at_y[dy] + at_z[(t - dy) % 4]) * CAP
                    == end_cols[...]
                )
                for dy in range(4)
            ],
            axis=0,
        )
        total = mm(mask, msg[...])
        first = total[:, 0:256]
        high = jnp.floor(first * (1.0 / 128.0))
        first = jnp.where(
            lane == MEM + 2, first - high * 128.0, jnp.where(lane == MEM + 3, high, first)
        )
        sums = jnp.concatenate([first, total[:, 256:640]], axis=1).astype(BF16)
        for pair in range(2):
            w_pair = jnp.concatenate([w_all[2 * pair], w_all[2 * pair + 1]], axis=1)
            out = mm(sums, w_pair).astype(BF16)
            for i in range(2):
                main_send[t, 2 * pair + i] = out[:, i * 128 : (i + 1) * 128].reshape(8, CAP, 128)
        ext_tmp[0:8, :] = mm_nt(w_ext[...], sums)
        ext_tmp[8:9, :] = ext_tmp[4:5, :] + ext_tmp[5:6, :] * 128.0
        for j in range(8):
            count_row = ext_tmp[8:9, j * CAP : (j + 1) * CAP]
            for dx in range(4):
                ext_send[t, dx, j, :, 0:CAP] = ext_tmp[dx : dx + 1, j * CAP : (j + 1) * CAP]
                ext_send[t, dx, j, :, 64 : 64 + CAP] = count_row
        for i in (4, 2, 6, 0, 5, 3, 7, 1):
            for dx in (2, 1, 3, 0):
                if t == 0 and dx == 0 and i == 0:
                    continue
                to = peer(t, i, dx)
                at = i // 2 * 2 + at_c[i % 2]
                send(
                    main_send.at[t, dx, at],
                    main_recv.at[t, dx * 8 + i],
                    send_sem.at[5],
                    recv_main.at[t],
                    to,
                )
                send(
                    ext_send.at[t, dx, at],
                    ext_recv.at[t, dx * 8 + i],
                    send_sem.at[6],
                    recv_ext.at[t],
                    to,
                )
    main_recv[0, 0] = main_send[0, 0, at_c[0]]
    ext_recv[0, 0] = ext_send[0, 0, at_c[0]]

    still = jnp.broadcast_to(cosine(phase), (EV, 128)).astype(BF16)
    query[...] = (
        mm(src[0].astype(BF16), wq[0:256, :]) + mm(still, wq[256:384, :])
    ) * (1.0 / math.sqrt(HEAD))
    head_of = iota((EV, 384), 1) < HEAD
    for h in range(2):
        part = query[...]
        part = jnp.where(head_of, part, 0.0) if h == 0 else jnp.where(head_of, 0.0, part)
        coarse = part.astype(BF16)
        fine = (part - coarse.astype(F32)).astype(BF16)
        qk[h] = mm_nt(coarse, wkv[:, 0:384]) + mm_nt(fine, wkv[:, 0:384])

    def attend(b, carry):
        at = pl.multiple_of(b * 128, 128)
        near[...] = mm(hot[b], table[...]).reshape(K, 128, 256)

        def group(g, inner):
            r = pl.multiple_of(g * 16, 16)
            rows = pl.ds(at + r, 16)
            q0, q1 = qk[0, rows, :], qk[1, rows, :]
            s0, s1 = [], []
            for k in range(K):
                x, t = near[k, pl.ds(r, 16), :], times[k, rows, :]
                u0 = x * q0[:, 0:256]
                u1 = x * q1[:, 0:256]
                u0 = u0[:, 0:128] + u0[:, 128:256] + t * q0[:, 256:384]
                u1 = u1[:, 0:128] + u1[:, 128:256] + t * q1[:, 256:384]
                s0.append(jnp.sum(u0, axis=1, keepdims=True))
                s1.append(jnp.sum(u1, axis=1, keepdims=True))
            m0 = functools.reduce(jnp.maximum, s0)
            m1 = functools.reduce(jnp.maximum, s1)
            p0 = [jnp.exp(s - m0) for s in s0]
            p1 = [jnp.exp(s - m1) for s in s1]
            n0 = 1.0 / sum(p0)
            n1 = 1.0 / sum(p1)
            a0 = a1 = jnp.zeros((16, 256), F32)
            c0 = c1 = jnp.zeros((16, 128), F32)
            for k in range(K):
                x, t = near[k, pl.ds(r, 16), :], times[k, rows, :]
                a0 += p0[k] * x
                a1 += p1[k] * x
                c0 += p0[k] * t
                c1 += p1[k] * t
            mix[0, rows, 0:256] = a0 * n0
            mix[1, rows, 0:256] = a1 * n1
            mix[0, rows, 256:384] = c0 * n0
            mix[1, rows, 256:384] = c1 * n1
            return inner

        lax.fori_loop(0, 8, group, 0, unroll=4)
        return carry

    lax.fori_loop(0, 4, attend, 0)
    halves = []
    for h in range(2):
        part = mix[h]
        coarse = part.astype(BF16)
        fine = (part - coarse.astype(F32)).astype(BF16)
        halves.append(mm(coarse, wkv[:, 384:768]) + mm(fine, wkv[:, 384:768]))
    attended = jnp.where(head_of, halves[0], halves[1]).astype(BF16)
    hidden = mm(attended, wm[0:384, :]) + mm(src[0].astype(BF16), wm[384:640, :])
    hidden = jnp.maximum(hidden + vec[2:3, 0:EMB], 0.0).astype(BF16)
    embedding[...] = (mm(hidden, w_out[...]) + vec[3:4, 0:EMB]).T.astype(BF16)

    for t in (2, 1, 3, 0):
        first = 1 if t == 0 else 0
        wait_bytes(main_recv.at[t, first:32], recv_main.at[t])
        wait_bytes(ext_recv.at[t, first:32], recv_ext.at[t])
        for i in range(32):
            side[0:1, i * CAP : (i + 1) * CAP] = ext_recv[t, i, :, 0:CAP]
            side[1:2, i * CAP : (i + 1) * CAP] = ext_recv[t, i, :, 64 : 64 + CAP]
        count = side[1:2, :]
        high = jnp.floor(count * (1.0 / 128.0))
        row = iota((16, SLOTS), 0)
        rest = jnp.where(
            row == 0,
            side[0:1, :],
            jnp.where(row == 1, count - high * 128.0, jnp.where(row == 2, high, 0.0)),
        )
        left = jnp.concatenate(
            [main_recv[t].reshape(SLOTS, 128).T, rest.astype(BF16)], axis=0
        )
        total = mm(left, claims[t])
        if t == 2:
            acc[...] = total
        else:
            acc[...] += total

    b0, b1, b2, b3 = (bias[0:UNITS, g : g + 1] for g in range(4))
    heard = acc[129:130, :] + acc[130:131, :] * 128.0
    share = 1.0 / jnp.maximum(heard, 1.0)
    reset = jax.nn.sigmoid(acc[0:UNITS, :] * share + zed[0, 0:UNITS, :] + b0)
    update = jax.nn.sigmoid(acc[UNITS : 2 * UNITS, :] * share + zed[1, 0:UNITS, :] + b1)
    cand = jnp.tanh(
        acc[2 * UNITS : 3 * UNITS, :] * share
        + zed[2, 0:UNITS, :]
        + b2
        + reset * (zed[3, 0:UNITS, :] + b3)
    )
    mine = own[0:UNITS, :]
    fresh = (1.0 - update) * cand + update * mine
    new_memory[...] = jnp.where(heard > 0.0, fresh, mine)

    wait_bytes(req_recv.at[0:127], send_sem.at[0])
    wait_bytes(edge_recv.at[0:3], send_sem.at[1])
    wait_bytes(w_all.at[0:3, 0:544], send_sem.at[2])
    wait_bytes(wx_all.at[0:3], send_sem.at[3])
    wait_bytes(row_send.at[0:31], send_sem.at[4])
    wait_bytes(main_recv.at[0:3], send_sem.at[5])
    wait_bytes(main_recv.at[3, 0:31], send_sem.at[5])
    wait_bytes(ext_recv.at[0:3], send_sem.at[6])
    wait_bytes(ext_recv.at[3, 0:31], send_sem.at[6])


def step(
    memory,
    last_update,
    ev_time,
    nbr_gap,
    slot_rows,
    slot_ref,
    edge_feat,
    frequency,
    phase_shift,
    w_query,
    w_key,
    w_value,
    w_merge,
    b_merge,
    w_out,
    b_out,
    w_input,
    w_hidden,
    gru_bias,
):
    args = (
        memory.T,
        last_update.reshape(1, ROWS),
        ev_time.reshape(1, EV),
        nbr_gap.T,
        slot_rows,
        slot_ref.T,
        edge_feat.T,
        frequency.reshape(1, TIME),
        phase_shift.reshape(1, TIME),
        w_query,
        w_key,
        w_value,
        w_merge.T,
        b_merge.reshape(1, EMB),
        w_out,
        b_out.reshape(1, EMB),
        jnp.swapaxes(w_input, 1, 2),
        jnp.swapaxes(w_hidden, 1, 2),
        gru_bias,
    )
    vmem = pl.BlockSpec(memory_space=pltpu.VMEM)
    V, D = pltpu.VMEM, pltpu.SemaphoreType.DMA
    embedding, new_memory = pl.pallas_call(
        kernel,
        out_shape=(
            jax.ShapeDtypeStruct((EMB, EV), BF16),
            jax.ShapeDtypeStruct((UNITS, ROWS), F32),
        ),
        in_specs=[pl.BlockSpec(memory_space=pl.ANY)] * len(args),
        out_specs=(vmem, vmem),
        scratch_shapes=[
            V((32, 1, 128), I32),
            V((128, 1, 128), I32),
            V((32, CAP, 256), BF16),
            V((32, CAP, 256), BF16),
            V((4, 64, EV), BF16),
            V((640, 128), BF16),
            V((1, 640), F32),
            V((4, 640, 128), BF16),
            V((4, 1, 640), F32),
            V((4, 4, 8, CAP, 128), BF16),
            V((4, 32, CAP, 128), BF16),
            V((4, 4, 8, 1, 128), F32),
            V((4, 32, 1, 128), F32),
            V((8, 256), F32),
            V((256, ROWS), F32),
            V((ROWS, 256), BF16),
            V((128, EV), F32),
            V((EV, 128), F32),
            V((128, 128), F32),
            V((K, EV, 128), F32),
            V((384, 768), BF16),
            V((384, 384), BF16),
            V((640, EMB), BF16),
            V((8, 640), BF16),
            V((4, CAP, ROWS), F32),
            V((CAP, ROWS), F32),
            V((1, 2 * EV), I32),
            V((2, EV, SLOTS), BF16),
            V((2, EV, 256), F32),
            V((2 * EV, 640), BF16),
            V((16, 384), F32),
            V((EV, 384), F32),
            V((4, K * 128, SLOTS), BF16),
            V((K, 128, 256), F32),
            V((2, EV, 384), F32),
            V((4, SLOTS, ROWS), BF16),
            V((4, 128, 128), F32),
            V((128, 128), F32),
            V((2, EV, 384), F32),
            V((8, SLOTS), F32),
            V((144, ROWS), F32),
            D((7,)),
            D((6,)),
            D,
            D((3,)),
            D((4,)),
            D((4,)),
            D((19,)),
        ]
        + [V(a.shape, a.dtype) for a in args],
        compiler_params=pltpu.CompilerParams(
            collective_id=0, has_side_effects=True, vmem_limit_bytes=60 * 1024 * 1024
        ),
    )(*args)
    return embedding.T, new_memory.T


def solution(mesh):
    return jax.shard_map(
        step,
        mesh=mesh,
        in_specs=(
            P("node", None),
            P("node"),
            P(("node", "feat")),
            P(("node", "feat"), None),
            P(("node", "feat"), None),
            P(("node", "feat"), None),
            P("node", "feat"),
            P(),
            P(),
            P(),
            P(),
            P(),
            P(),
            P(),
            P(),
            P(),
            P(None, None, "feat"),
            P(None, None, "feat"),
            P(None, "feat"),
        ),
        out_specs=(P(("node", "feat"), None), P("node", "feat")),
        check_vma=False,
    )
```
